32 devices in a mesh: tp: 8 (over z, y), fsdp: 4 (over x, core).
Axes of the slice: x: 2, y: 2, z: 4, core: 2. Of those that a mesh axis runs over, the one named last changes fastest.
Arguments:
- hidden: bfloat16 [8192, 1024], P('fsdp')
- labels: int32 [8192], P('fsdp')
- tok_mask: float32 [8192], P('fsdp')
- norm_gain: bfloat16 [1024], replicated
- w_head: bfloat16 [1024, 151936], P('fsdp', 'tp')
Outputs:
- output 1: float32 [], replicated
- output 2: bfloat16 [8192, 1024], P('fsdp')
- output 3: bfloat16 [1024, 151936], P('fsdp', 'tp')
- output 4: float32 [1024], replicated
All inputs are finite; a program needn't handle non-finite values.
Results may differ from the reference program's by a relative error of at most 0.0132744.
Values are sent between devices in bfloat16 or wider.
A program may use at most 1 GiB of HBM per device.

```python
import jax
import jax.numpy as jnp
from jax import lax

D = 1024
V = 151936
TOKENS = 8192
FSDP_SHARDS = 4
NORM_EPS = 1e-6
BLOCK_ROWS = min(TOKENS, 256)
NUM_BLOCKS = TOKENS // BLOCK_ROWS


def draw_routing(key_base):
    key_label, key_thresh, key_draws = jax.random.split(key_base, 3)
    labels = jax.random.randint(key_label, (TOKENS,), 0, V, dtype=jnp.int32)
    labels = labels.at[0].set(V - 1).at[1].set(0)
    thresholds = jax.random.randint(key_thresh, (FSDP_SHARDS, 1), 3, 16, dtype=jnp.int32)
    coin_draws = jax.random.randint(key_draws, (FSDP_SHARDS, TOKENS // FSDP_SHARDS), 0, 16, dtype=jnp.int32)
    keep_flags = (coin_draws < thresholds).reshape(TOKENS).at[0].set(True)
    return labels, keep_flags.astype(jnp.float32)


def setup_inputs(seed: int = 0) -> dict:
    key_base = jax.random.key(seed)
    key_route, key_head, key_noise, key_pull, key_gain = jax.random.split(key_base, 5)
    labels, tok_mask = draw_routing(key_route)
    head32 = jax.random.normal(key_head, (D, V), jnp.float32) * D ** -0.5
    label_cols = jnp.take(head32, labels, axis=1).T
    label_dirs = label_cols * lax.rsqrt(jnp.sum(label_cols * label_cols, axis=1, keepdims=True))
    pull_size = jax.random.uniform(key_pull, (TOKENS, 1), jnp.float32, 9.0, 15.0)
    hidden = jax.random.normal(key_noise, (TOKENS, D), jnp.float32) + pull_size * label_dirs
    norm_gain = 1.0 + 0.3 * jax.random.normal(key_gain, (D,), jnp.float32)
    return {'hidden': hidden.astype(jnp.bfloat16), 'labels': labels, 'tok_mask': tok_mask, 'norm_gain': norm_gain.astype(jnp.bfloat16), 'w_head': head32.astype(jnp.bfloat16)}


def norm_apply(hidden_f32, gain_f32):
    inv_rms = lax.rsqrt(jnp.mean(hidden_f32 * hidden_f32, axis=-1, keepdims=True) + NORM_EPS)
    return hidden_f32 * inv_rms * gain_f32


def reference(hidden, labels, tok_mask, norm_gain, w_head):
    normed_out, norm_pullback = jax.vjp(norm_apply, hidden.astype(jnp.float32), norm_gain.astype(jnp.float32))
    z_rows = normed_out.astype(jnp.bfloat16)
    z_blocks = z_rows.reshape(NUM_BLOCKS, BLOCK_ROWS, D)
    label_blocks = labels.reshape(NUM_BLOCKS, BLOCK_ROWS)

    def forward_block(block_in):
        z_blk, label_blk = block_in
        logits = jnp.dot(z_blk, w_head, preferred_element_type=jnp.float32)
        log_norm = jax.nn.logsumexp(logits, axis=1)
        label_logit = jnp.take_along_axis(logits, label_blk[:, None], axis=1)[:, 0]
        return log_norm, label_logit

    log_norm, label_logit = lax.map(forward_block, (z_blocks, label_blocks))
    tok_loss = (log_norm - label_logit).reshape(TOKENS)
    tok_count = jnp.sum(tok_mask)
    mean_loss = jnp.sum(tok_mask * tok_loss) / tok_count
    scale_blocks = (tok_mask / tok_count).reshape(NUM_BLOCKS, BLOCK_ROWS)
    vocab_ids = jnp.arange(V)

    def backward_block(dw_sum, block_in):
        z_blk, label_blk, norm_blk, scale_blk = block_in
        logits = jnp.dot(z_blk, w_head, preferred_element_type=jnp.float32)
        onehot = (vocab_ids[None, :] == label_blk[:, None]).astype(jnp.float32)
        d_logits = ((jnp.exp(logits - norm_blk[:, None]) - onehot) * scale_blk[:, None]).astype(jnp.bfloat16)
        grad_z = jnp.dot(d_logits, w_head.T, preferred_element_type=jnp.float32)
        dw_sum = dw_sum + jnp.dot(z_blk.T, d_logits, preferred_element_type=jnp.float32)
        return dw_sum, grad_z

    dw_sum, grad_z = lax.scan(backward_block, jnp.zeros((D, V), jnp.float32), (z_blocks, label_blocks, log_norm, scale_blocks))
    grad_hid, grad_gain = norm_pullback(grad_z.reshape(TOKENS, D))
    return mean_loss, grad_hid.astype(jnp.bfloat16), dw_sum.astype(jnp.bfloat16), grad_gain
```

```python
import functools

import jax
import jax.numpy as jnp
from jax import lax
from jax.experimental import pallas as pl
from jax.experimental.pallas import tpu as pltpu
from jax.sharding import PartitionSpec as P

NORM_EPS = 1e-6
LOG2E = 1.4426950408889634
NEG = -1e30
CHUNK = 512
TOK = 2048
TOK_DZ = 256
Z_ROWS = 512
AHEAD = 5
VMEM_LIMIT = 63 * 1024 * 1024
MESH = pl.DeviceIdType.MESH
f32, bf16 = jnp.float32, jnp.bfloat16


def dot_nt(a, b):
    return lax.dot_general(a, b, (((1,), (1,)), ((), ())), preferred_element_type=f32)


def dot_tn(a, b):
    return lax.dot_general(a, b, (((0,), (0,)), ((), ())), preferred_element_type=f32)


def dot_nn(a, b):
    return lax.dot_general(a, b, (((1,), (0,)), ((), ())), preferred_element_type=f32)


def cols(k, size):
    return pl.ds(pl.multiple_of(k * size, size), size)


class Sizes:
    def __init__(self, vocab_tp, n_fsdp, chunk):
        self.n = n_fsdp
        self.rows = -(-vocab_tp // (n_fsdp * 16)) * 16
        self.short = n_fsdp * self.rows - vocab_tp
        self.full = self.rows // chunk
        self.rem = self.rows - self.full * chunk
        self.solid = self.rem - self.short
        assert self.rem > self.short and self.rem % 16 == 0 and self.short % 16 == 0


def logits_kernel(sz, chunk, tok, h_hbm, w_hbm, gain, lab, l_hbm, z_hbm, wb_hbm, stat, z, w, lb0, lb1, hb0, hb1, m, s, hit, send, recv, loc, hsem, lsem, osem):
    me = lax.axis_index('fsdp')
    n, width = sz.n, w_hbm.shape[1]
    tokens = h_hbm.shape[0]
    lbufs, hbufs = (lb0, lb1), (hb0, hb1)

    barrier = pltpu.get_barrier_semaphore()
    for k in range(1, n):
        pl.semaphore_signal(barrier, inc=1, device_id={'fsdp': lax.rem(me + k, n)}, device_id_type=MESH)
    pl.semaphore_wait(barrier, n - 1)

    def remote(k, c, row0, rows):
        dest = lax.rem(me + k, n)
        return pltpu.make_async_remote_copy(
            src_ref=w_hbm.at[pl.ds(pl.multiple_of(dest * sz.rows + row0, 16), rows), :],
            dst_ref=w.at[pl.ds(pl.multiple_of(row0, 16), rows), cols(me, width)],
            send_sem=send.at[c, k], recv_sem=recv.at[c, k], device_id={'fsdp': dest}, device_id_type=MESH)

    def arrival(k, c, row0, rows):
        src = lax.rem(me + n - k, n)
        return pltpu.make_async_remote_copy(
            src_ref=w_hbm.at[pl.ds(0, rows), :],
            dst_ref=w.at[pl.ds(pl.multiple_of(row0, 16), rows), cols(src, width)],
            send_sem=send.at[c, k], recv_sem=recv.at[c, k], device_id={'fsdp': src}, device_id_type=MESH)

    def local(c, row0, rows):
        return pltpu.make_async_copy(
            w_hbm.at[pl.ds(pl.multiple_of(me * sz.rows + row0, 16), rows), :],
            w.at[pl.ds(pl.multiple_of(row0, 16), rows), cols(me, width)], loc.at[c])

    row_rem = sz.full * chunk
    row_odd = row_rem + sz.solid

    def issue(c):
        local(c, c * chunk, chunk).start()
        for k in range(1, n):
            remote(k, c, c * chunk, chunk).start()

    def when_not_last(dest, fn):
        if sz.short:
            pl.when(dest != n - 1)(fn)

    def issue_rem():
        local(sz.full, row_rem, sz.solid).start()
        when_not_last(me, lambda: local(sz.full + 1, row_odd, sz.short).start())
        for k in range(1, n):
            remote(k, sz.full, row_rem, sz.solid).start()
            when_not_last(lax.rem(me + k, n), lambda: remote(k, sz.full + 1, row_odd, sz.short).start())

    ahead = min(AHEAD, sz.full)
    for c in range(ahead):
        issue(c)

    if sz.short:
        @pl.when(me == n - 1)
        def _():
            w[row_odd:, :] = jnp.zeros((sz.short, w.shape[1]), bf16)

    z_rows = hb0.shape[0]
    n_z = tokens // z_rows

    def load_h(i, b):
        return pltpu.make_async_copy(h_hbm.at[cols(i, z_rows), :], hbufs[b], hsem.at[b])

    load_h(0, 0).start()
    load_h(1, 1).start()

    def norm(i, _):
        for b in (0, 1):
            k = 2 * i + b
            load_h(k, b).wait()
            h = hbufs[b][...].astype(f32)
            inv = lax.rsqrt(jnp.mean(h * h, axis=-1, keepdims=True) + NORM_EPS)
            z[cols(k, z_rows), :] = (h * inv * gain[...].astype(f32)).astype(bf16)

            @pl.when(k + 2 < n_z)
            def _():
                load_h(k + 2, b).start()
        return 0

    lax.fori_loop(0, n_z // 2, norm, 0)
    z_out = pltpu.make_async_copy(z, z_hbm, osem.at[0])
    z_out.start()

    m[...] = jnp.full(m.shape, NEG, f32)
    s[...] = jnp.zeros(s.shape, f32)
    hit[...] = jnp.zeros(hit.shape, f32)
    n_tok = tokens // tok
    sub = min(256, tok)
    lane = min(128, sub)

    def out_copy(row0, rows, k, b):
        return pltpu.make_async_copy(lbufs[b].at[pl.ds(0, rows), :], l_hbm.at[pl.ds(pl.multiple_of(row0, 16), rows), cols(k, tok)], lsem.at[b])

    def tile(row0, rows, k, b, masked):
        group = min(4, rows // 8)
        sub_rows = lax.broadcasted_iota(jnp.int32, (8, lane), 0)
        for c0 in range(0, tok, sub):
            logits = dot_nt(w[pl.ds(pl.multiple_of(row0, 16), rows), :], z[pl.ds(pl.multiple_of(k * tok + c0, sub), sub), :]) * LOG2E
            if masked:
                ids = lax.broadcasted_iota(jnp.int32, (rows, sub), 0)
                logits = jnp.where(ids < jnp.where(me == n - 1, sz.solid, sz.rem), logits, NEG)
            lbufs[b][0:rows, c0:c0 + sub] = logits
            for c1 in range(0, sub, lane):
                sl = pl.ds(pl.multiple_of(k * tok + c0 + c1, lane), lane)
                big, tot, got = m[:, sl], s[:, sl], hit[:, sl]
                rel = lab[0:1, sl] - row0 - sub_rows
                for g in range(0, rows // 8, group):
                    part = [logits[8 * r:8 * r + 8, c1:c1 + lane] for r in range(g, min(g + group, rows // 8))]
                    new = functools.reduce(jnp.maximum, part, big)
                    tot = tot * jnp.exp2(big - new)
                    for r, x in enumerate(part):
                        tot += jnp.exp2(x - new)
                        got += jnp.where(rel == 8 * (g + r), x, 0.0)
                    big = new
                m[:, sl], s[:, sl], hit[:, sl] = big, tot, got

    def chunk_rows(row0, rows, first, masked):
        def step(i, _):
            for b in (0, 1):
                k = 2 * i + b

                @pl.when(jnp.logical_not(jnp.logical_and(first, i == 0)))
                def _():
                    out_copy(0, chunk if not masked else rows, 0, b).wait()
                tile(row0, rows, k, b, masked)
                out_copy(row0, rows, k, b).start()
            return 0
        lax.fori_loop(0, n_tok // 2, step, 0)

    def full_chunk(c, _):
        local(c, c * chunk, chunk).wait()
        for k in range(1, n):
            arrival(k, c, c * chunk, chunk).wait_recv()

        @pl.when(c + ahead < sz.full)
        def _():
            issue(c + ahead)

        @pl.when(c + ahead == sz.full)
        def _():
            issue_rem()
        chunk_rows(c * chunk, chunk, c == 0, False)
        return 0

    lax.fori_loop(0, sz.full, full_chunk, 0)
    for b in (0, 1):
        out_copy(0, chunk, 0, b).wait()
    local(sz.full, row_rem, sz.solid).wait()
    when_not_last(me, lambda: local(sz.full + 1, row_odd, sz.short).wait())
    for k in range(1, n):
        arrival(k, sz.full, row_rem, sz.solid).wait_recv()
        when_not_last(me, lambda: arrival(k, sz.full + 1, row_odd, sz.short).wait_recv())
    w_out = pltpu.make_async_copy(w, wb_hbm, osem.at[1])
    w_out.start()
    chunk_rows(row_rem, sz.rem, True, True)
    for b in (0, 1):
        out_copy(0, sz.rem, 0, b).wait()

    big = jnp.max(m[...], axis=0, keepdims=True)
    stat[0:1, :] = big
    stat[1:2, :] = jnp.sum(s[...] * jnp.exp2(m[...] - big), axis=0, keepdims=True)
    stat[2:3, :] = jnp.sum(hit[...], axis=0, keepdims=True)
    z_out.wait()
    w_out.wait()

    def drain(c, _):
        for k in range(1, n):
            remote(k, c, c * chunk, chunk).wait_send()
        return 0

    lax.fori_loop(0, sz.full, drain, 0)
    for k in range(1, n):
        remote(k, sz.full, row_rem, sz.solid).wait_send()
        when_not_last(lax.rem(me + k, n), lambda: remote(k, sz.full + 1, row_odd, sz.short).wait_send())


def head_grad_kernel(sz, chunk, tok, z_hbm, l_hbm, st, lab, g_hbm, dw_hbm, z, l0, l1, g0, g1, acc, stage, zsem, lsem, gsem, dsem):
    tokens = z_hbm.shape[0]
    lbufs, gbufs = (l0, l1), (g0, g1)
    n_tok = tokens // tok
    lane = min(128, tok)
    z_in = pltpu.make_async_copy(z_hbm, z, zsem.at[0])
    z_in.start()

    def load(row0, rows, k, b):
        return pltpu.make_async_copy(l_hbm.at[pl.ds(pl.multiple_of(row0, 16), rows), cols(k, tok)], lbufs[b].at[pl.ds(0, rows), :], lsem.at[b])

    def save(row0, rows, k, b):
        return pltpu.make_async_copy(gbufs[b].at[pl.ds(0, rows), :], g_hbm.at[pl.ds(pl.multiple_of(row0, 16), rows), cols(k, tok)], gsem.at[b])

    def put(row0, rows):
        return pltpu.make_async_copy(stage.at[pl.ds(0, rows), :], dw_hbm.at[pl.ds(pl.multiple_of(row0, 16), rows), :], dsem.at[0])

    acc[...] = jnp.zeros(acc.shape, f32)

    def tile(row0, rows, k, b):
        ids = lax.broadcasted_iota(jnp.int32, (rows, lane), 0)
        step = min(256, tok)
        total = None
        for c0 in range(0, tok, step):
            for c1 in range(c0, c0 + step, lane):
                sl = pl.ds(pl.multiple_of(k * tok + c1, lane), lane)
                p = jnp.exp2(lbufs[b][0:rows, c1:c1 + lane] - st[0:1, sl])
                g = jnp.where(ids == lab[0:1, sl] - row0, p - 1.0, p) * st[1:2, sl]
                gbufs[b][0:rows, c1:c1 + lane] = g.astype(bf16)
            d = dot_nn(gbufs[b][0:rows, c0:c0 + step], z[pl.ds(pl.multiple_of(k * tok + c0, step), step), :])
            total = d if total is None else total + d
        acc[0:rows, :] += total

    def chunk_rows(row0, rows, first, next_row0, next_rows, has_next):
        def step(i, _):
            for b in (0, 1):
                k = 2 * i + b
                load(row0, rows, k, b).wait()

                @pl.when(jnp.logical_not(jnp.logical_and(first, i == 0)))
                def _():
                    save(row0, rows, 0, b).wait()
                tile(row0, rows, k, b)
                save(row0, rows, k, b).start()

                @pl.when(k + 2 < n_tok)
                def _():
                    load(row0, rows, k + 2, b).start()
            return 0
        lax.fori_loop(0, n_tok // 2, step, 0)

    for b in (0, 1):
        load(0, chunk, b, b).start()
    z_in.wait()

    def full_chunk(c, _):
        chunk_rows(c * chunk, chunk, c == 0, None, None, None)

        @pl.when(c + 1 < sz.full)
        def _():
            for b in (0, 1):
                load((c + 1) * chunk, chunk, b, b).start()

        @pl.when(c + 1 == sz.full)
        def _():
            for b in (0, 1):
                load(sz.full * chunk, sz.rem, b, b).start()

        @pl.when(c > 0)
        def _():
            put(0, chunk).wait()
        stage[...] = acc[...].astype(bf16)
        acc[...] = jnp.zeros(acc.shape, f32)
        put(c * chunk, chunk).start()
        return 0

    lax.fori_loop(0, sz.full, full_chunk, 0)
    for b in (0, 1):
        save(0, chunk, 0, b).wait()
    put(0, chunk).wait()
    chunk_rows(sz.full * chunk, sz.rem, True, None, None, None)
    for b in (0, 1):
        save(0, sz.rem, 0, b).wait()
    stage[0:sz.rem, :] = acc[0:sz.rem, :].astype(bf16)
    last = put(sz.full * chunk, sz.rem)
    last.start()
    last.wait()


def dz_kernel(tok, w_hbm, g_hbm, o_hbm, w, g0, g1, o0, o1, wsem, gsem, osem):
    gbufs, obufs = (g0, g1), (o0, o1)
    n_tok = g_hbm.shape[1] // tok
    w_in = pltpu.make_async_copy(w_hbm, w, wsem.at[0])
    w_in.start()

    def load(k, b):
        return pltpu.make_async_copy(g_hbm.at[:, cols(k, tok)], gbufs[b], gsem.at[b])

    def put(k, b):
        return pltpu.make_async_copy(obufs[b], o_hbm.at[cols(k, tok), :], osem.at[b])

    for b in (0, 1):
        load(b, b).start()
    w_in.wait()

    def step(i, _):
        for b in (0, 1):
            k = 2 * i + b
            load(k, b).wait()

            @pl.when(i > 0)
            def _():
                put(0, b).wait()
            obufs[b][...] = dot_tn(gbufs[b][...], w[...]).astype(bf16)
            put(k, b).start()

            @pl.when(k + 2 < n_tok)
            def _():
                load(k + 2, b).start()
        return 0

    lax.fori_loop(0, n_tok // 2, step, 0)
    for b in (0, 1):
        put(0, b).wait()


HBM = pl.BlockSpec(memory_space=pl.ANY)
VM = pl.BlockSpec(memory_space=pltpu.VMEM)
DMA = pltpu.SemaphoreType.DMA


def params(**kw):
    return pltpu.CompilerParams(vmem_limit_bytes=VMEM_LIMIT, **kw)


def solution(mesh, chunk=CHUNK, tok=TOK, tok_dz=TOK_DZ, z_rows=Z_ROWS):
    n_fsdp, n_tp = mesh.shape['fsdp'], mesh.shape['tp']
    everyone = ('fsdp', 'tp')
    S = jax.ShapeDtypeStruct

    def per_device(hidden, labels, tok_mask, norm_gain, w_rows):
        fsdp_id, tp_id = lax.axis_index('fsdp'), lax.axis_index('tp')
        d = hidden.shape[1]
        width, vocab_tp = w_rows.shape
        tokens = hidden.shape[0] * n_fsdp
        sz = Sizes(vocab_tp, n_fsdp, chunk)
        rows_own = hidden.shape[0] // n_tp
        hid_own = lax.dynamic_slice_in_dim(hidden, tp_id * rows_own, rows_own, 0)
        hid_all = lax.all_gather(hid_own, everyone, axis=0, tiled=True)
        lab_all = lax.all_gather(labels, 'fsdp', axis=0, tiled=True)
        mask_all = lax.all_gather(tok_mask, 'fsdp', axis=0, tiled=True)
        gain_f32 = norm_gain.astype(f32)
        mine = lab_all // vocab_tp == tp_id
        lab_loc = jnp.where(mine, lab_all - tp_id * vocab_tp - fsdp_id * sz.rows, -1)[None, :]

        logits, z_all, w_blk, stats = pl.pallas_call(
            functools.partial(logits_kernel, sz, chunk, tok),
            out_shape=(S((sz.rows, tokens), f32), S((tokens, d), bf16), S((sz.rows, d), bf16), S((8, tokens), f32)),
            in_specs=[HBM, HBM, VM, VM], out_specs=(HBM, HBM, HBM, VM),
            scratch_shapes=[pltpu.VMEM((tokens, d), bf16), pltpu.VMEM((sz.rows, d), bf16), pltpu.VMEM((chunk, tok), f32), pltpu.VMEM((chunk, tok), f32),
                            pltpu.VMEM((z_rows, d), bf16), pltpu.VMEM((z_rows, d), bf16),
                            pltpu.VMEM((8, tokens), f32), pltpu.VMEM((8, tokens), f32), pltpu.VMEM((8, tokens), f32),
                            DMA((sz.full + 2, n_fsdp)), DMA((sz.full + 2, n_fsdp)), DMA((sz.full + 2,)), DMA((2,)), DMA((2,)), DMA((2,))],
            compiler_params=params(collective_id=0, has_side_effects=True), name='logits',
        )(hid_all, w_rows.T, norm_gain[None, :], lab_loc)

        big = lax.pmax(stats[0], everyone)
        tot = lax.psum(jnp.stack([stats[1] * jnp.exp2(stats[0] - big), stats[2]]), everyone)
        lse = big + jnp.log2(tot[0])
        count = jnp.sum(mask_all)
        mean_loss = jnp.sum(mask_all * (lse - tot[1])) / LOG2E / count
        st = jnp.stack([lse, mask_all / count])

        g_t, dw_t = pl.pallas_call(
            functools.partial(head_grad_kernel, sz, chunk, tok),
            out_shape=(S((sz.rows, tokens), bf16), S((sz.rows, d), bf16)),
            in_specs=[HBM, HBM, VM, VM], out_specs=(HBM, HBM),
            scratch_shapes=[pltpu.VMEM((tokens, d), bf16), pltpu.VMEM((chunk, tok), f32), pltpu.VMEM((chunk, tok), f32), pltpu.VMEM((chunk, tok), bf16), pltpu.VMEM((chunk, tok), bf16),
                            pltpu.VMEM((chunk, d), f32), pltpu.VMEM((chunk, d), bf16), DMA((1,)), DMA((2,)), DMA((2,)), DMA((1,))],
            compiler_params=params(), name='head_grad',
        )(z_all, logits, st, lab_loc)

        grad_part = pl.pallas_call(
            functools.partial(dz_kernel, tok_dz),
            out_shape=S((tokens, d), bf16), in_specs=[HBM, HBM], out_specs=HBM,
            scratch_shapes=[pltpu.VMEM((sz.rows, d), bf16), pltpu.VMEM((sz.rows, tok_dz), bf16), pltpu.VMEM((sz.rows, tok_dz), bf16),
                            pltpu.VMEM((tok_dz, d), bf16), pltpu.VMEM((tok_dz, d), bf16), DMA((1,)), DMA((2,)), DMA((2,))],
            compiler_params=params(), name='dz',
        )(w_blk, g_t)

        grad_z = lax.psum_scatter(grad_part, 'fsdp', scatter_dimension=0, tiled=True)
        grad_z = lax.psum_scatter(grad_z, 'tp', scatter_dimension=0, tiled=True).astype(f32)
        hid_f32 = hid_own.astype(f32)
        inv_rms = lax.rsqrt(jnp.mean(hid_f32 * hid_f32, axis=-1, keepdims=True) + NORM_EPS)
        normed = hid_f32 * inv_rms
        d_normed = grad_z * gain_f32
        grad_hid = inv_rms * (d_normed - normed * jnp.mean(d_normed * normed, axis=-1, keepdims=True))
        grad_hidden = lax.all_gather(grad_hid.astype(bf16), 'tp', axis=0, tiled=True)
        grad_gain = lax.psum(jnp.sum(grad_z * normed, axis=0), everyone)
        grad_head = lax.all_to_all(dw_t, 'fsdp', split_axis=1, concat_axis=0, tiled=True)
        return mean_loss, grad_hidden, grad_head[:vocab_tp].T, grad_gain

    return jax.shard_map(per_device, mesh=mesh, in_specs=(P('fsdp', None), P('fsdp'), P('fsdp'), P(), P('fsdp', 'tp')), out_specs=(P(), P('fsdp', None), P('fsdp', 'tp'), P()), check_vma=False)
```

```python
import functools

import jax
import jax.numpy as jnp
from jax import lax
from jax.experimental import pallas as pl
from jax.experimental.pallas import tpu as pltpu
from jax.sharding import PartitionSpec as P

NORM_EPS = 1e-6
LOG2E = 1.4426950408889634
NEG = -1e30
CHUNK = 512
TOK = 2048
EARLY = 6
Z_ROWS = 512
AHEAD = 5
VMEM_LIMIT = 67_043_328
MESH = pl.DeviceIdType.MESH
f32, bf16 = jnp.float32, jnp.bfloat16


def dot_nt(a, b):
    return lax.dot_general(a, b, (((1,), (1,)), ((), ())), preferred_element_type=f32)


def dot_tn(a, b):
    return lax.dot_general(a, b, (((0,), (0,)), ((), ())), preferred_element_type=f32)


def dot_nn(a, b):
    return lax.dot_general(a, b, (((1,), (0,)), ((), ())), preferred_element_type=f32)


def cols(k, size):
    return pl.ds(pl.multiple_of(k * size, size), size)


class Sizes:
    def __init__(self, vocab_tp, n_fsdp, chunk):
        self.n = n_fsdp
        self.rows = -(-vocab_tp // (n_fsdp * 16)) * 16
        self.short = n_fsdp * self.rows - vocab_tp
        self.full = self.rows // chunk
        self.rem = self.rows - self.full * chunk
        self.solid = self.rem - self.short
        assert self.rem > self.short and self.rem % 16 == 0 and self.short % 16 == 0


class Place:
    def __init__(self, n_fsdp, n_tp):
        self.n_fsdp, self.n_tp, self.n_all = n_fsdp, n_tp, n_fsdp * n_tp
        self.f, self.tp = lax.axis_index('fsdp'), lax.axis_index('tp')
        self.x, self.c = self.f // 2, lax.rem(self.f, 2)
        self.n_z = n_tp // 2
        self.z, self.y = self.tp // 2, lax.rem(self.tp, 2)
        self.index = self.tp * n_fsdp + self.f

    def other(self, k):
        i = lax.rem(self.index + k, self.n_all)
        return i // self.n_fsdp, lax.rem(i, self.n_fsdp)


def dev(tp, f):
    return {'tp': tp, 'fsdp': f}


def rcopy(src, dst, ssem, rsem, to):
    return pltpu.make_async_remote_copy(src_ref=src, dst_ref=dst, send_sem=ssem, recv_sem=rsem, device_id=to, device_id_type=MESH)


def enter(at):
    barrier = pltpu.get_barrier_semaphore()

    def tell(k, _):
        tp, f = at.other(k)
        pl.semaphore_signal(barrier, inc=1, device_id=dev(tp, f), device_id_type=MESH)
        return 0

    lax.fori_loop(1, at.n_all, tell, 0)
    pl.semaphore_wait(barrier, at.n_all - 1)


def logits_kernel(sz, n_tp, chunk, tok, h_hbm, w_hbm, gain, lab, scale, l_hbm, z_hbm, wb_hbm, st_out, z, w, lb0, lb1, hb0, hb1, m, s, hit, st_loc, got, res, st, send, recv, loc, hsem, lsem, osem, ssend, srecv, rsend, rrecv):
    at = Place(sz.n, n_tp)
    me = at.f
    n, width = sz.n, w_hbm.shape[1]
    tokens = h_hbm.shape[0]
    lbufs, hbufs = (lb0, lb1), (hb0, hb1)

    enter(at)

    def remote(k, c, row0, rows):
        dest = lax.rem(me + k, n)
        return pltpu.make_async_remote_copy(
            src_ref=w_hbm.at[pl.ds(pl.multiple_of(dest * sz.rows + row0, 16), rows), :],
            dst_ref=w.at[pl.ds(pl.multiple_of(row0, 16), rows), cols(me, width)],
            send_sem=send.at[c, k], recv_sem=recv.at[c, k], device_id={'fsdp': dest}, device_id_type=MESH)

    def arrival(k, c, row0, rows):
        src = lax.rem(me + n - k, n)
        return pltpu.make_async_remote_copy(
            src_ref=w_hbm.at[pl.ds(0, rows), :],
            dst_ref=w.at[pl.ds(pl.multiple_of(row0, 16), rows), cols(src, width)],
            send_sem=send.at[c, k], recv_sem=recv.at[c, k], device_id={'fsdp': src}, device_id_type=MESH)

    def local(c, row0, rows):
        return pltpu.make_async_copy(
            w_hbm.at[pl.ds(pl.multiple_of(me * sz.rows + row0, 16), rows), :],
            w.at[pl.ds(pl.multiple_of(row0, 16), rows), cols(me, width)], loc.at[c])

    row_rem = sz.full * chunk
    row_odd = row_rem + sz.solid

    def issue(c):
        local(c, c * chunk, chunk).start()
        for k in range(1, n):
            remote(k, c, c * chunk, chunk).start()

    def when_not_last(dest, fn):
        if sz.short:
            pl.when(dest != n - 1)(fn)

    def issue_rem():
        local(sz.full, row_rem, sz.solid).start()
        when_not_last(me, lambda: local(sz.full + 1, row_odd, sz.short).start())
        for k in range(1, n):
            remote(k, sz.full, row_rem, sz.solid).start()
            when_not_last(lax.rem(me + k, n), lambda: remote(k, sz.full + 1, row_odd, sz.short).start())

    ahead = min(AHEAD, sz.full)
    for c in range(ahead):
        issue(c)

    if sz.short:
        @pl.when(me == n - 1)
        def _():
            w[row_odd:, :] = jnp.zeros((sz.short, w.shape[1]), bf16)

    z_rows = hb0.shape[0]
    n_z = tokens // z_rows

    def load_h(i, b):
        return pltpu.make_async_copy(h_hbm.at[cols(i, z_rows), :], hbufs[b], hsem.at[b])

    load_h(0, 0).start()
    load_h(1, 1).start()

    def norm(i, _):
        for b in (0, 1):
            k = 2 * i + b
            load_h(k, b).wait()
            h = hbufs[b][...].astype(f32)
            inv = lax.rsqrt(jnp.mean(h * h, axis=-1, keepdims=True) + NORM_EPS)
            z[cols(k, z_rows), :] = (h * inv * gain[...].astype(f32)).astype(bf16)

            @pl.when(k + 2 < n_z)
            def _():
                load_h(k + 2, b).start()
        return 0

    lax.fori_loop(0, n_z // 2, norm, 0)
    z_out = pltpu.make_async_copy(z, z_hbm, osem.at[0])
    z_out.start()

    m[...] = jnp.full(m.shape, NEG, f32)
    s[...] = jnp.zeros(s.shape, f32)
    hit[...] = jnp.zeros(hit.shape, f32)
    n_tok = tokens // tok
    sub = min(256, tok)
    lane = min(128, sub)

    def out_copy(row0, rows, k, b):
        return pltpu.make_async_copy(lbufs[b].at[pl.ds(0, rows), :], l_hbm.at[pl.ds(pl.multiple_of(row0, 16), rows), cols(k, tok)], lsem.at[b])

    def tile(row0, rows, k, b, masked):
        group = min(4, rows // 8)
        sub_rows = lax.broadcasted_iota(jnp.int32, (8, lane), 0)
        for c0 in range(0, tok, sub):
            logits = dot_nt(w[pl.ds(pl.multiple_of(row0, 16), rows), :], z[pl.ds(pl.multiple_of(k * tok + c0, sub), sub), :]) * LOG2E
            if masked:
                ids = lax.broadcasted_iota(jnp.int32, (rows, sub), 0)
                logits = jnp.where(ids < jnp.where(me == n - 1, sz.solid, sz.rem), logits, NEG)
            lbufs[b][0:rows, c0:c0 + sub] = logits
            for c1 in range(0, sub, lane):
                sl = pl.ds(pl.multiple_of(k * tok + c0 + c1, lane), lane)
                big, tot, got = m[:, sl], s[:, sl], hit[:, sl]
                rel = lab[0:1, sl] - row0 - sub_rows
                for g in range(0, rows // 8, group):
                    part = [logits[8 * r:8 * r + 8, c1:c1 + lane] for r in range(g, min(g + group, rows // 8))]
                    new = functools.reduce(jnp.maximum, part, big)
                    tot = tot * jnp.exp2(big - new)
                    for r, x in enumerate(part):
                        tot += jnp.exp2(x - new)
                        got += jnp.where(rel == 8 * (g + r), x, 0.0)
                    big = new
                m[:, sl], s[:, sl], hit[:, sl] = big, tot, got

    def chunk_rows(row0, rows, first, masked):
        def step(i, _):
            for b in (0, 1):
                k = 2 * i + b

                @pl.when(jnp.logical_not(jnp.logical_and(first, i == 0)))
                def _():
                    out_copy(0, chunk if not masked else rows, 0, b).wait()
                tile(row0, rows, k, b, masked)
                out_copy(row0, rows, k, b).start()
            return 0
        lax.fori_loop(0, n_tok // 2, step, 0)

    def full_chunk(c, _):
        local(c, c * chunk, chunk).wait()
        for k in range(1, n):
            arrival(k, c, c * chunk, chunk).wait_recv()

        @pl.when(c + ahead < sz.full)
        def _():
            issue(c + ahead)

        @pl.when(c + ahead == sz.full)
        def _():
            issue_rem()
        chunk_rows(c * chunk, chunk, c == 0, False)
        return 0

    lax.fori_loop(0, sz.full, full_chunk, 0)
    for b in (0, 1):
        out_copy(0, chunk, 0, b).wait()
    local(sz.full, row_rem, sz.solid).wait()
    when_not_last(me, lambda: local(sz.full + 1, row_odd, sz.short).wait())
    for k in range(1, n):
        arrival(k, sz.full, row_rem, sz.solid).wait_recv()
        when_not_last(me, lambda: arrival(k, sz.full + 1, row_odd, sz.short).wait_recv())
    w_out = pltpu.make_async_copy(w, wb_hbm, osem.at[1])
    w_out.start()
    chunk_rows(row_rem, sz.rem, True, True)
    for b in (0, 1):
        out_copy(0, sz.rem, 0, b).wait()

    big = jnp.max(m[...], axis=0, keepdims=True)
    st_loc[0:1, :] = big
    st_loc[1:2, :] = jnp.sum(s[...] * jnp.exp2(m[...] - big), axis=0, keepdims=True)
    st_loc[2:3, :] = jnp.sum(hit[...], axis=0, keepdims=True)
    st_loc[3:8, :] = jnp.zeros((5, tokens), f32)

    own = tokens // at.n_all

    def block(tp, f):
        return pl.ds(pl.multiple_of((f * at.n_tp + tp) * own, own), own)

    mine = block(at.tp, at.f)

    def ask(k):
        tp, f = at.other(k)
        return rcopy(st_loc.at[:, block(tp, f)], got.at[k], ssend.at[k], srecv.at[k], dev(tp, f))

    def answer(k):
        tp, f = at.other(k)
        return rcopy(res, st.at[:, mine], rsend.at[k], rrecv.at[k], dev(tp, f))

    def answered(k):
        tp, f = at.other(at.n_all - k)
        return rcopy(res, st.at[:, block(tp, f)], rsend.at[k], rrecv.at[k], dev(tp, f))

    def every(fn):
        def go(k, _):
            fn(k)
            return 0
        lax.fori_loop(1, at.n_all, go, 0)

    every(lambda k: ask(k).start())
    got[0] = st_loc[:, mine]
    every(lambda k: ask(k).wait_recv())
    tops = got[:, 0:1, :]
    top = jnp.max(tops, axis=0)
    lse = top + jnp.log2(jnp.sum(got[:, 1:2, :] * jnp.exp2(tops - top[None]), axis=0))
    sc = scale[0:1, mine]
    res[0:1, :] = lse - jnp.log2(sc)
    res[1:2, :] = sc
    res[2:3, :] = (lse - jnp.sum(got[:, 2:3, :], axis=0)) * (sc * (1.0 / LOG2E))
    res[3:8, :] = jnp.zeros((5, own), f32)
    every(lambda k: answer(k).start())
    st[:, mine] = res[...]
    every(lambda k: answered(k).wait_recv())
    st_out[...] = st[...]
    every(lambda k: ask(k).wait_send())
    every(lambda k: answer(k).wait_send())
    z_out.wait()
    w_out.wait()

    def drain(c, _):
        for k in range(1, n):
            remote(k, c, c * chunk, chunk).wait_send()
        return 0

    lax.fori_loop(0, sz.full, drain, 0)
    for k in range(1, n):
        remote(k, sz.full, row_rem, sz.solid).wait_send()
        when_not_last(lax.rem(me + k, n), lambda: remote(k, sz.full + 1, row_odd, sz.short).wait_send())


def grad_kernel(sz, n_tp, chunk, early, tok, tok_own, half, z_hbm, w_hbm, l_hbm, st, lab, hid, gain, g_hbm, dw_hbm, gh_hbm, gg_out,
                z, w, l0, l1, g0, g1, q0, q1, acc, stage, acc_own, stage_own, sib_out, sib_in, pair_sum, y_out, y_in, part, z_out, z_in, z_own, x_out, x_in, gh, gg, gg_in,
                zsem, wsem, lsem, gsem, qsem, bsem, ssem, dw_send, dw_recv, own_sem, sib_s, sib_r, y_s, y_r, zz_s, zz_r, x_s, x_r, ag_s, ag_r, fw_s, fw_r, gh_sem, gain_s, gain_r):
    at = Place(sz.n, n_tp)
    me, n = at.f, sz.n
    tokens, width = z.shape[0], dw_hbm.shape[1]
    per_f, per_tp = tokens // n, tokens // at.n_all
    n_z, groups = at.n_z, 2 * at.n_z
    rounds = per_tp // half
    lbufs, gbufs, qbufs = (l0, l1), (g0, g1), (q0, q1)
    lane = min(128, tok)
    row_rem, row_low = sz.full * chunk, early * chunk
    low = [(j, chunk) for j in range(sz.full - early)] + [(sz.full - early, sz.rem)]
    far, sib = 1 - at.x, at.x * 2 + 1 - at.c
    sibling, y_peer, x_peer = dev(at.tp, sib), dev(at.z * 2 + 1 - at.y, at.f), dev(at.tp, far * 2 + at.c)

    z_load = pltpu.make_async_copy(z_hbm, z, zsem.at[0])
    w_load = pltpu.make_async_copy(w_hbm, w, wsem.at[0])
    z_load.start()
    w_load.start()

    def rows_at(row0, rows):
        return pl.ds(pl.multiple_of(row0, 16), rows)

    def gradient(x, top, sc, rel):
        rows = x.shape[0]
        p = jnp.exp2(x - top).reshape(rows // 8, 8, x.shape[1])
        ids = lax.broadcasted_iota(jnp.int32, p.shape, 0) * 8
        return jnp.where(ids == rel[None], p - sc[None], p).reshape(x.shape).astype(bf16)

    def token_row(sl, row0):
        size = sl.size
        return st[0:1, sl], st[1:2, sl], lab[0:1, sl] - row0 - lax.broadcasted_iota(jnp.int32, (8, size), 0)

    def load_l(row0, rows, k, b):
        return pltpu.make_async_copy(l_hbm.at[rows_at(row0, rows), cols(k, tok)], lbufs[b].at[pl.ds(0, rows), :], lsem.at[b])

    def load_g(row0, rows, k, b):
        return pltpu.make_async_copy(g_hbm.at[rows_at(row0, rows), cols(k, tok)], gbufs[b].at[pl.ds(0, rows), :], gsem.at[b])

    def save_g(row0, rows, k, b):
        return pltpu.make_async_copy(gbufs[b].at[pl.ds(0, rows), :], g_hbm.at[rows_at(row0, rows), cols(k, tok)], gsem.at[b])

    n_tok = tokens // tok
    step = min(256, tok)
    n_far = 2 * width

    def tile(row0, rows, k, b, fresh):
        total = None
        for c0 in range(0, tok, step):
            if fresh:
                for c1 in range(c0, c0 + step, lane):
                    top, sc, rel = token_row(pl.ds(pl.multiple_of(k * tok + c1, lane), lane), row0)
                    gbufs[b][0:rows, c1:c1 + lane] = gradient(lbufs[b][0:rows, c1:c1 + lane], top, sc, rel)
            lhs = gbufs[b][0:rows, c0:c0 + step]
            rhs = pl.ds(pl.multiple_of(k * tok + c0, step), step)
            d = (dot_nn(lhs, z[rhs, cols(far, n_far)]), dot_nn(lhs, z[rhs, cols(sib, width)]))
            total = d if total is None else (total[0] + d[0], total[1] + d[1])
        acc[0:rows, 0:n_far] += total[0]
        acc[0:rows, n_far:] += total[1]

    def sends(slot, row0, rows):
        out = []
        for i, f in enumerate((far * 2, far * 2 + 1, sib)):
            k = lax.rem(f + n - me, n)
            out.append(rcopy(stage.at[slot, pl.ds(0, rows), i * width:(i + 1) * width], dw_hbm.at[rows_at(me * sz.rows + row0, rows), :],
                             dw_send.at[slot, i], dw_recv.at[k], dev(at.tp, f)))
        return out

    def ship(c, row0, rows):
        slot = lax.rem(c, 2)

        @pl.when(c >= 2)
        def _():
            for cp in sends(slot, 0, chunk):
                cp.wait_send()
        stage[slot, 0:rows, :] = acc[0:rows, :].astype(bf16)
        acc[...] = jnp.zeros(acc.shape, f32)
        for cp in sends(slot, row0, rows):
            cp.start()

    enter(at)
    acc[...] = jnp.zeros(acc.shape, f32)
    for b in (0, 1):
        load_l(0, chunk, b, b).start()
    z_load.wait()

    def early_chunk(c, _):
        def pair(i, _):
            for b in (0, 1):
                k = 2 * i + b
                load_l(0, chunk, 0, b).wait()

                @pl.when(jnp.logical_not(jnp.logical_and(c == 0, i == 0)))
                def _():
                    save_g(0, chunk, 0, b).wait()
                tile(c * chunk, chunk, k, b, True)
                save_g(c * chunk, chunk, k, b).start()
                wrap = k + 2 >= n_tok
                c2 = jnp.where(wrap, c + 1, c)

                @pl.when(c2 < early)
                def _():
                    load_l(c2 * chunk, chunk, jnp.where(wrap, k + 2 - n_tok, k + 2), b).start()
            return 0
        lax.fori_loop(0, n_tok // 2, pair, 0)
        ship(c, c * chunk, chunk)
        return 0

    lax.fori_loop(0, early, early_chunk, 0)
    for b in (0, 1):
        save_g(0, chunk, 0, b).wait()
    w_load.wait()

    def group_of(q):
        r, g = q // groups, lax.rem(q, groups)
        xi, jj = g // n_z, lax.rem(g, n_z)
        return r, xi, jj, jnp.where(xi == 0, far, at.x), lax.rem(at.z + jj + 1, n_z)

    def pieces(q, own):
        r, _, _, xb, zb = group_of(q)
        cb = at.c if own else 1 - at.c
        return [pl.multiple_of((xb * 2 + cb) * per_f + (zb * 2 + yb) * per_tp + r * half, half) for yb in (1 - at.y, at.y)]

    def block_loads(q, b):
        out = []
        for i, t0 in enumerate(pieces(q, b == 1)):
            dst = pl.ds(i * half, half)
            out.append(pltpu.make_async_copy(g_hbm.at[pl.ds(0, row_low), pl.ds(t0, half)], qbufs[b].at[pl.ds(0, row_low), dst], qsem.at[b, i]))
            for j, rows in low:
                out.append(pltpu.make_async_copy(l_hbm.at[pl.ds(row_low + j * chunk, rows), pl.ds(t0, half)],
                                                 lbufs[b].at[pl.ds(0, rows), pl.ds((2 * j + i) * half, half)], bsem.at[b, 2 * j + i]))
        return out

    def block_saves(q, b):
        return [pltpu.make_async_copy(qbufs[b].at[pl.ds(row_low, sz.rows - row_low), pl.ds(i * half, half)],
                                      g_hbm.at[pl.ds(row_low, sz.rows - row_low), pl.ds(t0, half)], ssem.at[b, i]) for i, t0 in enumerate(pieces(q, b == 1))]

    def block_dot(q, b):
        for i, t0 in enumerate(pieces(q, b == 1)):
            for j, rows in low:
                row0 = row_low + j * chunk
                top, sc, rel = token_row(pl.ds(t0, half), row0)
                qbufs[b][row0:row0 + rows, i * half:(i + 1) * half] = gradient(lbufs[b][0:rows, (2 * j + i) * half:(2 * j + i + 1) * half], top, sc, rel)
        return dot_tn(qbufs[b][...], w[...])

    def to_sib(q):
        slot = lax.rem(q, 2)
        return rcopy(sib_out.at[slot], sib_in.at[slot], sib_s.at[slot], sib_r.at[slot], sibling)

    def to_y(q):
        slot, land = lax.rem(q, 2), lax.rem(q, y_in.shape[0])
        return rcopy(y_out.at[slot], y_in.at[land], y_s.at[slot], y_r.at[land], y_peer)

    def to_z(q):
        r, xi, jj, _, zb = group_of(q)
        return rcopy(z_out.at[jj], z_in.at[r, xi, jj], zz_s.at[jj], zz_r.at[r, xi, jj], dev(zb * 2 + at.y, at.f))

    def to_x(r):
        return rcopy(x_out, x_in.at[r], x_s.at[0], x_r.at[r], x_peer)

    def z_stage(q):
        _, xi, jj, _, _ = group_of(q)
        to_y(q).wait_recv()
        val = part[lax.rem(q, part.shape[0])] + y_in[lax.rem(q, y_in.shape[0])].astype(f32)

        @pl.when(jj == n_z - 1)
        def _():
            z_own[xi] = val

        @pl.when(jj < n_z - 1)
        def _():
            @pl.when(q >= n_z)
            def _():
                to_z(q - n_z).wait_send()
            z_out[jj] = val.astype(bf16)
            to_z(q).start()

    def z_sum(r, xi):
        val = z_own[xi]
        for jj in range(n_z - 1):
            rcopy(z_out.at[0], z_in.at[r, xi, jj], zz_s.at[jj], zz_r.at[r, xi, jj], sibling).wait_recv()
            val = val + z_in[r, xi, jj].astype(f32)
        return val

    def x_stage(r):
        @pl.when(r > 0)
        def _():
            to_x(0).wait_send()
        x_out[...] = z_sum(r, 0)
        to_x(r).start()

    def home(tp, r):
        return gh_hbm.at[pl.ds(pl.multiple_of(tp * per_tp + r * half, half), half), :]

    def gathers(r):
        out = [rcopy(gh.at[r], home(at.tp, r), ag_s.at[r, n_z - 1], fw_r.at[r, at.z], y_peer)]
        for jj in range(n_z - 1):
            to = lax.rem(at.z + jj + 1, n_z)
            out.append(rcopy(gh.at[r], home(at.tp, r), ag_s.at[r, jj], ag_r.at[r, jj], dev(to * 2 + at.y, at.f)))
        return out

    def keep(r):
        return pltpu.make_async_copy(gh.at[r], home(at.tp, r), gh_sem.at[r])

    def from_z(jj):
        return lax.rem(at.z + n_z - jj - 1, n_z)

    def arrived(r, jj):
        return rcopy(gh.at[r], home(from_z(jj) * 2 + at.y, r), ag_s.at[r, jj], ag_r.at[r, jj], sibling)

    def onward(r, jj):
        here = home(from_z(jj) * 2 + at.y, r)
        return rcopy(here, here, fw_s.at[r, jj], fw_r.at[r, from_z(jj)], y_peer)

    def final(r):
        to_x(r).wait_recv()
        dz = z_sum(r, 1) + x_in[r]
        h = hid[pl.ds(pl.multiple_of(r * half, half), half), :].astype(f32)
        inv = lax.rsqrt(jnp.mean(h * h, axis=-1, keepdims=True) + NORM_EPS)
        normed = h * inv
        a = dz * gain[...].astype(f32)
        gh[r] = (inv * (a - normed * jnp.mean(a * normed, axis=-1, keepdims=True))).astype(bf16)
        gg[...] += jnp.sum(dz * normed, axis=0, keepdims=True)
        keep(r).start()
        for cp in gathers(r):
            cp.start()

    def forwards(r):
        for jj in range(n_z - 1):
            arrived(r, jj).wait_recv()
            onward(r, jj).start()

    gg[...] = jnp.zeros(gg.shape, f32)
    last = rounds * groups
    x_at, final_at, forward_at = n_z + 2, groups + 2, groups + 6
    for b in (0, 1):
        for cp in block_loads(0, b):
            cp.start()

    def event(q, first, fn):
        @pl.when(jnp.logical_and(q >= first, jnp.logical_and(lax.rem(q + groups - first, groups) == 0, q < first + last)))
        def _():
            fn((q - first) // groups)

    def events(q):
        @pl.when(jnp.logical_and(q >= 2, q < last + 2))
        def _():
            z_stage(q - 2)
        event(q, x_at, x_stage)
        event(q, final_at, final)
        event(q, forward_at, forwards)

    def dz_group(q, _):
        for b in (0, 1):
            for cp in block_loads(q, b):
                cp.wait()

            @pl.when(q > 0)
            def _():
                for cp in block_saves(q - 1, b):
                    cp.wait()
            slot = lax.rem(q, 2)
            if b == 0:
                @pl.when(q >= 2)
                def _():
                    to_sib(q - 2).wait_send()
                sib_out[slot] = block_dot(q, b).astype(bf16)
                to_sib(q).start()
            else:
                @pl.when(q >= 2)
                def _():
                    to_y(q - 2).wait_send()
                pair_sum[...] = block_dot(q, b)
                to_sib(q).wait_recv()
                val = pair_sum[...] + sib_in[slot].astype(f32)
                y_out[slot] = val[0:half].astype(bf16)
                part[lax.rem(q, part.shape[0])] = val[half:]
                to_y(q).start()
            for cp in block_saves(q, b):
                cp.start()

            @pl.when(q + 1 < last)
            def _():
                for cp in block_loads(q + 1, b):
                    cp.start()
        events(q)
        return 0

    lax.fori_loop(0, last, dz_group, 0)
    for b in (0, 1):
        for cp in block_saves(last - 1, b):
            cp.wait()

    def stored(lo, tile_fn, after):
        for b in (0, 1):
            load_g(lo * chunk, chunk, b, b).start()

        def one(c, _):
            def pair(i, _):
                for b in (0, 1):
                    k = 2 * i + b
                    load_g(0, chunk, 0, b).wait()
                    tile_fn(c * chunk, chunk, k, b)
                    wrap = k + 2 >= n_tok
                    c2, k2 = jnp.where(wrap, c + 1, c), jnp.where(wrap, k + 2 - n_tok, k + 2)

                    @pl.when(c2 < sz.full)
                    def _():
                        load_g(c2 * chunk, chunk, k2, b).start()

                    @pl.when(c2 == sz.full)
                    def _():
                        load_g(row_rem, sz.rem, k2, b).start()
                return 0
            lax.fori_loop(0, n_tok // 2, pair, 0)
            after(c, c * chunk, chunk)
            return 0
        lax.fori_loop(lo, sz.full, one, 0)

        def pair(i, _):
            for b in (0, 1):
                k = 2 * i + b
                load_g(row_rem, sz.rem, 0, b).wait()
                tile_fn(row_rem, sz.rem, k, b)

                @pl.when(k + 2 < n_tok)
                def _():
                    load_g(row_rem, sz.rem, k + 2, b).start()
            return 0
        lax.fori_loop(0, n_tok // 2, pair, 0)
        after(sz.full, row_rem, sz.rem)

    def ship_and_sum(c, row0, rows):
        ship(c, row0, rows)
        if rows == chunk:
            e = last + 2 * (c - early)

            @pl.when(e < last + 4)
            def _():
                events(e)
                events(e + 1)

    stored(early, lambda row0, rows, k, b: tile(row0, rows, k, b, False), ship_and_sum)

    def tell_gain(k):
        tp, f = at.other(k)
        return rcopy(gg, gg_in.at[at.index], gain_s.at[k], gain_r.at[k], dev(tp, f))

    def heard_gain(k):
        i = lax.rem(at.index + at.n_all - k, at.n_all)
        return rcopy(gg, gg_in.at[i], gain_s.at[k], gain_r.at[k], sibling)

    def every(fn):
        def go(k, _):
            fn(k)
            return 0
        lax.fori_loop(1, at.n_all, go, 0)

    every(lambda k: tell_gain(k).start())
    gg_in[at.index] = gg[...]

    def tile_own(row0, rows, k, b):
        acc_own[0:rows, :] += dot_nn(gbufs[b][0:rows, :], z[cols(k, tok), cols(me, width)])

    def put_own(slot, row0, rows):
        return pltpu.make_async_copy(stage_own.at[slot, pl.ds(0, rows), :], dw_hbm.at[rows_at(me * sz.rows + row0, rows), :], own_sem.at[slot])

    def ship_own(c, row0, rows):
        slot = lax.rem(c, 2)

        @pl.when(c >= 2)
        def _():
            put_own(slot, 0, chunk).wait()
        stage_own[slot, 0:rows, :] = acc_own[0:rows, :].astype(bf16)
        acc_own[...] = jnp.zeros(acc_own.shape, f32)
        put_own(slot, row0, rows).start()
        if rows == chunk:
            @pl.when(c == min(6, sz.full - 1))
            def _():
                forwards(rounds - 1)

    acc_own[...] = jnp.zeros(acc_own.shape, f32)
    stored(0, tile_own, ship_own)

    every(lambda k: heard_gain(k).wait_recv())
    gg_out[...] = jnp.sum(gg_in[...], axis=0)
    every(lambda k: tell_gain(k).wait_send())
    put_own((sz.full - 1) % 2, 0, chunk).wait()
    put_own(sz.full % 2, 0, sz.rem).wait()
    for slot, rows in (((sz.full - 1) % 2, chunk), (sz.full % 2, sz.rem)):
        for cp in sends(slot, 0, rows):
            cp.wait_send()
    for q in (last - 2, last - 1):
        to_sib(q).wait_send()
        to_y(q).wait_send()
    for q in range(last - n_z, last - 1):
        to_z(q).wait_send()
    to_x(rounds - 1).wait_send()
    for r in range(rounds):
        keep(r).wait()
        for cp in gathers(r):
            cp.wait_send()
        for jj in range(n_z - 1):
            onward(r, jj).wait_send()
        for zf in range(n_z):
            rcopy(gh.at[r], home(zf * 2 + 1 - at.y, r), ag_s.at[r, 0], fw_r.at[r, zf], y_peer).wait_recv()
    for k in range(1, n):
        src = lax.rem(me + n - k, n)
        rcopy(dw_hbm.at[pl.ds(0, sz.rows), :], dw_hbm.at[rows_at(src * sz.rows, sz.rows), :], dw_send.at[0, 0], dw_recv.at[k], sibling).wait_recv()


HBM = pl.BlockSpec(memory_space=pl.ANY)
VM = pl.BlockSpec(memory_space=pltpu.VMEM)
DMA = pltpu.SemaphoreType.DMA


def params(**kw):
    return pltpu.CompilerParams(vmem_limit_bytes=VMEM_LIMIT, **kw)


def solution(mesh, chunk=CHUNK, tok=TOK, early=EARLY, z_rows=Z_ROWS):
    n_fsdp, n_tp = mesh.shape['fsdp'], mesh.shape['tp']
    n_all, n_z = n_fsdp * n_tp, n_tp // 2
    everyone = ('fsdp', 'tp')
    S = jax.ShapeDtypeStruct

    def per_device(hidden, labels, tok_mask, norm_gain, w_rows):
        fsdp_id, tp_id = lax.axis_index('fsdp'), lax.axis_index('tp')
        d = hidden.shape[1]
        width, vocab_tp = w_rows.shape
        tokens = hidden.shape[0] * n_fsdp
        sz = Sizes(vocab_tp, n_fsdp, chunk)
        own = hidden.shape[0] // n_tp
        half = own // 2
        rounds = 2
        hid_own = lax.dynamic_slice_in_dim(hidden, tp_id * own, own, 0)
        hid_all = lax.all_gather(hid_own, everyone, axis=0, tiled=True)
        lab_all = lax.all_gather(labels, 'fsdp', axis=0, tiled=True)
        mask_all = lax.all_gather(tok_mask, 'fsdp', axis=0, tiled=True)
        scale = (mask_all / jnp.sum(mask_all))[None, :]
        mine = lab_all // vocab_tp == tp_id
        lab_loc = jnp.where(mine, lab_all - tp_id * vocab_tp - fsdp_id * sz.rows, -1)[None, :]
        V = pltpu.VMEM

        logits, z_all, w_blk, st = pl.pallas_call(
            functools.partial(logits_kernel, sz, n_tp, chunk, tok),
            out_shape=(S((sz.rows, tokens), f32), S((tokens, d), bf16), S((sz.rows, d), bf16), S((8, tokens), f32)),
            in_specs=[HBM, HBM, VM, VM, VM], out_specs=(HBM, HBM, HBM, VM),
            scratch_shapes=[V((tokens, d), bf16), V((sz.rows, d), bf16), V((chunk, tok), f32), V((chunk, tok), f32),
                            V((z_rows, d), bf16), V((z_rows, d), bf16),
                            V((8, tokens), f32), V((8, tokens), f32), V((8, tokens), f32),
                            V((8, tokens), f32), V((n_all, 8, own), f32), V((8, own), f32), V((8, tokens), f32),
                            DMA((sz.full + 2, n_fsdp)), DMA((sz.full + 2, n_fsdp)), DMA((sz.full + 2,)), DMA((2,)), DMA((2,)), DMA((2,)),
                            DMA((n_all,)), DMA((n_all,)), DMA((n_all,)), DMA((n_all,))],
            compiler_params=params(collective_id=0, has_side_effects=True), name='logits',
        )(hid_all, w_rows.T, norm_gain[None, :], lab_loc, scale)

        mean_loss = jnp.sum(st[2])
        n_low = sz.full - early + 1

        _, dw_t, grad_hidden, gain_sum = pl.pallas_call(
            functools.partial(grad_kernel, sz, n_tp, chunk, early, tok, tok, half),
            out_shape=(S((sz.rows, tokens), bf16), S((n_fsdp * sz.rows, width), bf16), S(hidden.shape, bf16), S((1, d), f32)),
            in_specs=[HBM, HBM, HBM, VM, VM, VM, VM], out_specs=(HBM, HBM, HBM, VM),
            scratch_shapes=[V((tokens, d), bf16), V((sz.rows, d), bf16), V((chunk, tok), f32), V((chunk, tok), f32), V((chunk, tok), bf16), V((chunk, tok), bf16),
                            V((sz.rows, 2 * half), bf16), V((sz.rows, 2 * half), bf16),
                            V((chunk, 3 * width), f32), V((2, chunk, 3 * width), bf16), V((chunk, width), f32), V((2, chunk, width), bf16),
                            V((2, 2 * half, d), bf16), V((2, 2 * half, d), bf16), V((2 * half, d), f32), V((2, half, d), bf16), V((8, half, d), bf16), V((3, half, d), f32),
                            V((n_z - 1, half, d), bf16), V((rounds, 2, n_z - 1, half, d), bf16), V((2, half, d), f32), V((half, d), f32), V((rounds, half, d), f32),
                            V((rounds, half, d), bf16), V((1, d), f32), V((n_all, 1, d), f32),
                            DMA((1,)), DMA((1,)), DMA((2,)), DMA((2,)), DMA((2, 2)), DMA((2, 2 * n_low)), DMA((2, 2)),
                            DMA((2, 3)), DMA((n_fsdp,)), DMA((2,)), DMA((2,)), DMA((2,)), DMA((2,)), DMA((8,)),
                            DMA((n_z - 1,)), DMA((rounds, 2, n_z - 1)), DMA((1,)), DMA((rounds,)),
                            DMA((rounds, n_z)), DMA((rounds, n_z)), DMA((rounds, n_z)), DMA((rounds, n_z)), DMA((rounds,)), DMA((n_all,)), DMA((n_all,))],
            compiler_params=params(collective_id=1, has_side_effects=True), name='grads',
        )(z_all, w_blk, logits, st, lab_loc, hid_own, norm_gain[None, :])
        return mean_loss, grad_hidden, dw_t[:vocab_tp].T, gain_sum[0]

    return jax.shard_map(per_device, mesh=mesh, in_specs=(P('fsdp', None), P('fsdp'), P('fsdp'), P(), P('fsdp', 'tp')), out_specs=(P(), P('fsdp', None), P('fsdp', 'tp'), P()), check_vma=False)
```

```python
import functools

import jax
import jax.numpy as jnp
from jax import lax
from jax.experimental import pallas as pl
from jax.experimental.pallas import tpu as pltpu
from jax.sharding import PartitionSpec as P

NORM_EPS = 1e-6
LOG2E = 1.4426950408889634
NEG = -1e30
CHUNK = 512
TOK = 2048
EARLY = 4
Z_ROWS = 512
AHEAD = 5
VMEM_LIMIT = 67_043_328
MESH = pl.DeviceIdType.MESH
scope = jax.named_scope
f32, bf16 = jnp.float32, jnp.bfloat16


def dot_nt(a, b):
    return lax.dot_general(a, b, (((1,), (1,)), ((), ())), preferred_element_type=f32)


def dot_tn(a, b):
    return lax.dot_general(a, b, (((0,), (0,)), ((), ())), preferred_element_type=f32)


def dot_nn(a, b):
    return lax.dot_general(a, b, (((1,), (0,)), ((), ())), preferred_element_type=f32)


def cols(k, size):
    return pl.ds(pl.multiple_of(k * size, size), size)


class Sizes:
    def __init__(self, vocab_tp, n_fsdp, chunk):
        self.n = n_fsdp
        self.rows = -(-vocab_tp // (n_fsdp * 16)) * 16
        self.short = n_fsdp * self.rows - vocab_tp
        self.full = self.rows // chunk
        self.rem = self.rows - self.full * chunk
        self.solid = self.rem - self.short
        assert self.rem > self.short and self.rem % 16 == 0 and self.short % 16 == 0


class Place:
    def __init__(self, n_fsdp, n_tp):
        self.n_fsdp, self.n_tp, self.n_all = n_fsdp, n_tp, n_fsdp * n_tp
        self.f, self.tp = lax.axis_index('fsdp'), lax.axis_index('tp')
        self.x, self.c = self.f // 2, lax.rem(self.f, 2)
        self.n_z = n_tp // 2
        self.z, self.y = self.tp // 2, lax.rem(self.tp, 2)
        self.index = self.tp * n_fsdp + self.f

    def other(self, k):
        i = lax.rem(self.index + k, self.n_all)
        return i // self.n_fsdp, lax.rem(i, self.n_fsdp)


def dev(tp, f):
    return {'tp': tp, 'fsdp': f}


def rcopy(src, dst, ssem, rsem, to):
    return pltpu.make_async_remote_copy(src_ref=src, dst_ref=dst, send_sem=ssem, recv_sem=rsem, device_id=to, device_id_type=MESH)


def enter(at):
    barrier = pltpu.get_barrier_semaphore()

    def tell(k, _):
        tp, f = at.other(k)
        pl.semaphore_signal(barrier, inc=1, device_id=dev(tp, f), device_id_type=MESH)
        return 0

    lax.fori_loop(1, at.n_all, tell, 0)
    pl.semaphore_wait(barrier, at.n_all - 1)


def logits_kernel(sz, n_tp, chunk, tok, h_hbm, w_hbm, gain, lab, scale, l_hbm, z_hbm, wb_hbm, st_out, hit_out, z, w, lb0, lb1, hb0, hb1, m, s, hit, st_loc, got, res, st, send, recv, loc, hsem, lsem, osem, ssend, srecv, rsend, rrecv):
    at = Place(sz.n, n_tp)
    me = at.f
    n, width = sz.n, w_hbm.shape[1]
    tokens = h_hbm.shape[0]
    lbufs, hbufs = (lb0, lb1), (hb0, hb1)

    with scope('enter'):
        enter(at)

    def remote(k, c, row0, rows):
        dest = lax.rem(me + k, n)
        return pltpu.make_async_remote_copy(
            src_ref=w_hbm.at[pl.ds(pl.multiple_of(dest * sz.rows + row0, 16), rows), :],
            dst_ref=w.at[pl.ds(pl.multiple_of(row0, 16), rows), cols(me, width)],
            send_sem=send.at[c, k], recv_sem=recv.at[c, k], device_id={'fsdp': dest}, device_id_type=MESH)

    def arrival(k, c, row0, rows):
        src = lax.rem(me + n - k, n)
        return pltpu.make_async_remote_copy(
            src_ref=w_hbm.at[pl.ds(0, rows), :],
            dst_ref=w.at[pl.ds(pl.multiple_of(row0, 16), rows), cols(src, width)],
            send_sem=send.at[c, k], recv_sem=recv.at[c, k], device_id={'fsdp': src}, device_id_type=MESH)

    def local(c, row0, rows):
        return pltpu.make_async_copy(
            w_hbm.at[pl.ds(pl.multiple_of(me * sz.rows + row0, 16), rows), :],
            w.at[pl.ds(pl.multiple_of(row0, 16), rows), cols(me, width)], loc.at[c])

    row_rem = sz.full * chunk
    row_odd = row_rem + sz.solid

    def issue(c):
        local(c, c * chunk, chunk).start()
        for k in range(1, n):
            remote(k, c, c * chunk, chunk).start()

    def when_not_last(dest, fn):
        if sz.short:
            pl.when(dest != n - 1)(fn)

    def issue_rem():
        local(sz.full, row_rem, sz.solid).start()
        when_not_last(me, lambda: local(sz.full + 1, row_odd, sz.short).start())
        for k in range(1, n):
            remote(k, sz.full, row_rem, sz.solid).start()
            when_not_last(lax.rem(me + k, n), lambda: remote(k, sz.full + 1, row_odd, sz.short).start())

    ahead = min(AHEAD, sz.full)
    for c in range(ahead):
        issue(c)

    if sz.short:
        @pl.when(me == n - 1)
        def _():
            w[row_odd:, :] = jnp.zeros((sz.short, w.shape[1]), bf16)

    z_rows = hb0.shape[0]
    n_z = tokens // z_rows

    def load_h(i, b):
        return pltpu.make_async_copy(h_hbm.at[cols(i, z_rows), :], hbufs[b], hsem.at[b])

    load_h(0, 0).start()
    load_h(1, 1).start()

    def norm(i, _):
        for b in (0, 1):
            k = 2 * i + b
            load_h(k, b).wait()
            h = hbufs[b][...].astype(f32)
            inv = lax.rsqrt(jnp.mean(h * h, axis=-1, keepdims=True) + NORM_EPS)
            z[cols(k, z_rows), :] = (h * inv * gain[...].astype(f32)).astype(bf16)

            @pl.when(k + 2 < n_z)
            def _():
                load_h(k + 2, b).start()
        return 0

    with scope('norm'):
        lax.fori_loop(0, n_z // 2, norm, 0)
    z_out = pltpu.make_async_copy(z, z_hbm, osem.at[0])
    z_out.start()

    m[...] = jnp.full(m.shape, NEG, f32)
    s[...] = jnp.zeros(s.shape, f32)
    hit[...] = jnp.zeros(hit.shape, f32)
    n_tok = tokens // tok
    sub = min(256, tok)
    lane = min(128, sub)

    def out_copy(row0, rows, k, b):
        return pltpu.make_async_copy(lbufs[b].at[pl.ds(0, rows), :], l_hbm.at[pl.ds(pl.multiple_of(row0, 16), rows), cols(k, tok)], lsem.at[b])

    def tile(row0, rows, k, b, masked):
        group = min(4, rows // 8)
        sub_rows = lax.broadcasted_iota(jnp.int32, (8, lane), 0)
        for c0 in range(0, tok, sub):
            logits = dot_nt(w[pl.ds(pl.multiple_of(row0, 16), rows), :], z[pl.ds(pl.multiple_of(k * tok + c0, sub), sub), :]) * LOG2E
            if masked:
                ids = lax.broadcasted_iota(jnp.int32, (rows, sub), 0)
                logits = jnp.where(ids < jnp.where(me == n - 1, sz.solid, sz.rem), logits, NEG)
            lbufs[b][0:rows, c0:c0 + sub] = logits
            for c1 in range(0, sub, lane):
                sl = pl.ds(pl.multiple_of(k * tok + c0 + c1, lane), lane)
                big, tot, got = m[:, sl], s[:, sl], hit[:, sl]
                rel = lab[0:1, sl] - row0 - sub_rows
                for g in range(0, rows // 8, group):
                    part = [logits[8 * r:8 * r + 8, c1:c1 + lane] for r in range(g, min(g + group, rows // 8))]
                    new = functools.reduce(jnp.maximum, part, big)
                    tot = tot * jnp.exp2(big - new)
                    for r, x in enumerate(part):
                        tot += jnp.exp2(x - new)
                        got += jnp.where(rel == 8 * (g + r), x, 0.0)
                    big = new
                m[:, sl], s[:, sl], hit[:, sl] = big, tot, got

    def chunk_rows(row0, rows, first, masked):
        def step(i, _):
            for b in (0, 1):
                k = 2 * i + b

                with scope('l_wait'):
                    @pl.when(jnp.logical_not(jnp.logical_and(first, i == 0)))
                    def _():
                        out_copy(0, chunk if not masked else rows, 0, b).wait()
                with scope('l_tile'):
                    tile(row0, rows, k, b, masked)
                out_copy(row0, rows, k, b).start()
            return 0
        lax.fori_loop(0, n_tok // 2, step, 0)

    def full_chunk(c, _):
        with scope('w_wait'):
            local(c, c * chunk, chunk).wait()
            for k in range(1, n):
                arrival(k, c, c * chunk, chunk).wait_recv()

        @pl.when(c + ahead < sz.full)
        def _():
            issue(c + ahead)

        @pl.when(c + ahead == sz.full)
        def _():
            issue_rem()
        chunk_rows(c * chunk, chunk, c == 0, False)
        return 0

    lax.fori_loop(0, sz.full, full_chunk, 0)
    for b in (0, 1):
        out_copy(0, chunk, 0, b).wait()
    local(sz.full, row_rem, sz.solid).wait()
    when_not_last(me, lambda: local(sz.full + 1, row_odd, sz.short).wait())
    for k in range(1, n):
        arrival(k, sz.full, row_rem, sz.solid).wait_recv()
        when_not_last(me, lambda: arrival(k, sz.full + 1, row_odd, sz.short).wait_recv())
    w_out = pltpu.make_async_copy(w, wb_hbm, osem.at[1])
    w_out.start()
    chunk_rows(row_rem, sz.rem, True, True)
    for b in (0, 1):
        out_copy(0, sz.rem, 0, b).wait()

    big = jnp.max(m[...], axis=0, keepdims=True)
    st_loc[0:1, :] = big
    st_loc[1:2, :] = jnp.sum(s[...] * jnp.exp2(m[...] - big), axis=0, keepdims=True)

    own = tokens // at.n_all

    def block(tp, f):
        return pl.ds(pl.multiple_of((f * at.n_tp + tp) * own, own), own)

    mine = block(at.tp, at.f)

    def ask(k):
        tp, f = at.other(k)
        return rcopy(st_loc.at[:, block(tp, f)], got.at[k], ssend.at[k], srecv.at[k], dev(tp, f))

    def answer(k):
        tp, f = at.other(k)
        return rcopy(res, st.at[:, mine], rsend.at[k], rrecv.at[k], dev(tp, f))

    def answered(k):
        tp, f = at.other(at.n_all - k)
        return rcopy(res, st.at[:, block(tp, f)], rsend.at[k], rrecv.at[k], dev(tp, f))

    def every(fn):
        def go(k, _):
            fn(k)
            return 0
        lax.fori_loop(1, at.n_all, go, 0)

    every(lambda k: ask(k).start())
    got[0] = st_loc[:, mine]
    with scope('ask_wait'):
        every(lambda k: ask(k).wait_recv())
    tops = got[:, 0:1, :]
    top = jnp.max(tops, axis=0)
    res[...] = top + jnp.log2(jnp.sum(got[:, 1:2, :] * jnp.exp2(tops - top[None]), axis=0))
    every(lambda k: answer(k).start())
    st[:, mine] = res[...]
    loss_part = jnp.sum(hit[...] * scale[...], axis=0, keepdims=True)
    hit_out[...] = jnp.broadcast_to(jnp.sum(loss_part, axis=1, keepdims=True), hit_out.shape)
    with scope('answer_wait'):
        every(lambda k: answered(k).wait_recv())
    st_out[0:1, :] = st[...] - jnp.log2(scale[...])
    st_out[1:2, :] = scale[...]
    st_out[2:3, :] = st[...]
    st_out[3:8, :] = jnp.zeros((5, tokens), f32)
    scope_tail = scope('l_tail')
    scope_tail.__enter__()
    every(lambda k: ask(k).wait_send())
    every(lambda k: answer(k).wait_send())
    z_out.wait()
    w_out.wait()

    def drain(c, _):
        for k in range(1, n):
            remote(k, c, c * chunk, chunk).wait_send()
        return 0

    lax.fori_loop(0, sz.full, drain, 0)
    for k in range(1, n):
        remote(k, sz.full, row_rem, sz.solid).wait_send()
        when_not_last(lax.rem(me + k, n), lambda: remote(k, sz.full + 1, row_odd, sz.short).wait_send())
    scope_tail.__exit__(None, None, None)


def grad_kernel(sz, n_tp, chunk, early, tok, tok_own, half, z_hbm, w_hbm, l_hbm, st, lab, hid, gain, hit_sum, g_hbm, dw_hbm, gh_hbm, gg_out, ds_hbm,
                z, w, l0, l1, g0, g1, q0, q1, acc, stage, acc_own, stage_own, sib_out, sib_in, pair_sum, y_out, y_in, part, z_out, z_in, z_own, x_out, x_in, gh, gg, gg_in,
                zsem, wsem, lsem, gsem, qsem, bsem, ssem, dw_copy, dw_send, dw_recv, own_sem, sib_s, sib_r, y_s, y_r, zz_s, zz_r, x_s, x_r, ag_s, ag_r, fw_s, fw_r, gh_sem, gain_s, gain_r):
    at = Place(sz.n, n_tp)
    me, n = at.f, sz.n
    tokens, width = z.shape[0], dw_hbm.shape[1]
    per_f, per_tp = tokens // n, tokens // at.n_all
    n_z, groups = at.n_z, 2 * at.n_z
    rounds = per_tp // half
    lbufs, gbufs, qbufs = (l0, l1), (g0, g1), (q0, q1)
    lane = min(128, tok)
    row_rem, row_low = sz.full * chunk, early * chunk
    low = [(j, chunk) for j in range(sz.full - early)] + [(sz.full - early, sz.rem)]
    far, sib = 1 - at.x, at.x * 2 + 1 - at.c
    sibling, y_peer, x_peer = dev(at.tp, sib), dev(at.z * 2 + 1 - at.y, at.f), dev(at.tp, far * 2 + at.c)

    n_far = 2 * width
    z_loads = [pltpu.make_async_copy(z_hbm.at[:, src], z.at[:, dst], zsem.at[i]) for i, (src, dst) in enumerate((
        (cols(far, n_far), pl.ds(0, n_far)), (cols(sib, width), pl.ds(n_far, width)), (cols(me, width), pl.ds(n_far + width, width))))]
    w_load = pltpu.make_async_copy(w_hbm, w, wsem.at[0])
    for cp in z_loads:
        cp.start()
    w_load.start()

    def rows_at(row0, rows):
        return pl.ds(pl.multiple_of(row0, 16), rows)

    def gradient(x, top, sc, rel):
        rows = x.shape[0]
        p = jnp.exp2(x - top).reshape(rows // 8, 8, x.shape[1])
        ids = lax.broadcasted_iota(jnp.int32, p.shape, 0) * 8
        return jnp.where(ids == rel[None], p - sc[None], p).reshape(x.shape).astype(bf16)

    def token_row(sl, row0):
        size = sl.size
        return st[0:1, sl], st[1:2, sl], lab[0:1, sl] - row0 - lax.broadcasted_iota(jnp.int32, (8, size), 0)

    def load_l(row0, rows, k, b):
        return pltpu.make_async_copy(l_hbm.at[rows_at(row0, rows), cols(k, tok)], lbufs[b].at[pl.ds(0, rows), :], lsem.at[b])

    def load_g(row0, rows, k, b):
        return pltpu.make_async_copy(g_hbm.at[rows_at(row0, rows), cols(k, tok)], gbufs[b].at[pl.ds(0, rows), :], gsem.at[b])

    def save_g(row0, rows, k, b):
        return pltpu.make_async_copy(gbufs[b].at[pl.ds(0, rows), :], g_hbm.at[rows_at(row0, rows), cols(k, tok)], gsem.at[b])

    n_tok = tokens // tok
    step = min(256, tok)

    def tile(row0, rows, k, b, fresh):
        mid = rows // 32 * 16
        parts = ((0, rows, 0, n_far), (0, mid, n_far, n_far + width), (mid, rows, n_far, n_far + width))
        total = None
        for c0 in range(0, tok, step):
            if fresh:
                for c1 in range(c0, c0 + step, lane):
                    top, sc, rel = token_row(pl.ds(pl.multiple_of(k * tok + c1, lane), lane), row0)
                    gbufs[b][0:rows, c1:c1 + lane] = gradient(lbufs[b][0:rows, c1:c1 + lane], top, sc, rel)
            rhs = pl.ds(pl.multiple_of(k * tok + c0, step), step)
            d = [dot_nn(gbufs[b][r0:r1, c0:c0 + step], z[rhs, v0:v1]) for r0, r1, v0, v1 in parts]
            total = d if total is None else [p + q for p, q in zip(total, d)]
        for (r0, r1, v0, v1), val in zip(parts, total):
            acc[r0:r1, v0:v1] += val

    def aside(c, rows):
        slot = lax.rem(c, 2)
        return pltpu.make_async_copy(stage.at[slot, pl.ds(0, rows), :], ds_hbm.at[rows_at(c * chunk, rows), :], dw_copy.at[slot])

    def sends(c, rows):
        out = []
        for i, f in enumerate((far * 2, far * 2 + 1, sib)):
            out.append(rcopy(ds_hbm.at[rows_at(c * chunk, rows), i * width:(i + 1) * width], dw_hbm.at[rows_at(me * sz.rows + c * chunk, rows), :],
                             dw_send.at[c, i], dw_recv.at[lax.rem(f + n - me, n)], dev(at.tp, f)))
        return out

    def ship(c, rows):
        stage[lax.rem(c, 2), 0:rows, :] = acc[0:rows, :].astype(bf16)
        acc[...] = jnp.zeros(acc.shape, f32)
        aside(c, rows).start()

    def flush(c, rows):
        aside(c, rows).wait()
        for cp in sends(c, rows):
            cp.start()

    with scope('enter'):
        enter(at)
    acc[...] = jnp.zeros(acc.shape, f32)
    for b in (0, 1):
        load_l(0, chunk, b, b).start()
    with scope('zload'):
        for cp in z_loads:
            cp.wait()

    def early_chunk(c, _):
        def pair(i, _):
            for b in (0, 1):
                k = 2 * i + b
                with scope('b1_wait'):
                    load_l(0, chunk, 0, b).wait()

                    @pl.when(jnp.logical_not(jnp.logical_and(c == 0, i == 0)))
                    def _():
                        save_g(0, chunk, 0, b).wait()
                with scope('b1_tile'):
                    tile(c * chunk, chunk, k, b, True)
                save_g(c * chunk, chunk, k, b).start()
                wrap = k + 2 >= n_tok
                c2 = jnp.where(wrap, c + 1, c)

                @pl.when(c2 < early)
                def _():
                    load_l(c2 * chunk, chunk, jnp.where(wrap, k + 2 - n_tok, k + 2), b).start()

            @pl.when(jnp.logical_and(i == 0, c > 0))
            def _():
                flush(c - 1, chunk)
            return 0
        lax.fori_loop(0, n_tok // 2, pair, 0)
        with scope('ship'):
            ship(c, chunk)
        return 0

    lax.fori_loop(0, early, early_chunk, 0)
    for b in (0, 1):
        save_g(0, chunk, 0, b).wait()
    w_load.wait()

    def group_of(q):
        r, g = q // groups, lax.rem(q, groups)
        xi, jj = g // n_z, lax.rem(g, n_z)
        return r, xi, jj, jnp.where(xi == 0, far, at.x), lax.rem(at.z + jj + 1, n_z)

    def pieces(q, own):
        r, _, _, xb, zb = group_of(q)
        cb = at.c if own else 1 - at.c
        return [pl.multiple_of((xb * 2 + cb) * per_f + (zb * 2 + yb) * per_tp + r * half, half) for yb in (1 - at.y, at.y)]

    def block_loads(q, b):
        out = []
        for i, t0 in enumerate(pieces(q, b == 1)):
            dst = pl.ds(i * half, half)
            out.append(pltpu.make_async_copy(g_hbm.at[pl.ds(0, row_low), pl.ds(t0, half)], qbufs[b].at[pl.ds(0, row_low), dst], qsem.at[b, i]))
            for j, rows in low:
                out.append(pltpu.make_async_copy(l_hbm.at[pl.ds(row_low + j * chunk, rows), pl.ds(t0, half)],
                                                 lbufs[b].at[pl.ds(0, rows), pl.ds((2 * j + i) * half, half)], bsem.at[b, 2 * j + i]))
        return out

    def block_saves(q, b):
        return [pltpu.make_async_copy(qbufs[b].at[pl.ds(row_low, sz.rows - row_low), pl.ds(i * half, half)],
                                      g_hbm.at[pl.ds(row_low, sz.rows - row_low), pl.ds(t0, half)], ssem.at[b, i]) for i, t0 in enumerate(pieces(q, b == 1))]

    def block_dot(q, b):
        for i, t0 in enumerate(pieces(q, b == 1)):
            for j, rows in low:
                row0 = row_low + j * chunk
                top, sc, rel = token_row(pl.ds(t0, half), row0)
                qbufs[b][row0:row0 + rows, i * half:(i + 1) * half] = gradient(lbufs[b][0:rows, (2 * j + i) * half:(2 * j + i + 1) * half], top, sc, rel)
        return dot_tn(qbufs[b][...], w[...])

    def to_sib(q):
        slot = lax.rem(q, 2)
        return rcopy(sib_out.at[slot], sib_in.at[slot], sib_s.at[slot], sib_r.at[slot], sibling)

    def to_y(q):
        slot, land = lax.rem(q, 2), lax.rem(q, y_in.shape[0])
        return rcopy(y_out.at[slot], y_in.at[land], y_s.at[slot], y_r.at[land], y_peer)

    def to_z(q):
        r, xi, jj, _, zb = group_of(q)
        return rcopy(z_out.at[jj], z_in.at[r, xi, jj], zz_s.at[jj], zz_r.at[r, xi, jj], dev(zb * 2 + at.y, at.f))

    def to_x(r):
        return rcopy(x_out, x_in.at[r], x_s.at[0], x_r.at[r], x_peer)

    def z_stage(q):
        _, xi, jj, _, _ = group_of(q)
        with scope('y_wait'):
            to_y(q).wait_recv()
        val = part[lax.rem(q, part.shape[0])] + y_in[lax.rem(q, y_in.shape[0])].astype(f32)

        @pl.when(jj == n_z - 1)
        def _():
            z_own[xi] = val

        @pl.when(jj < n_z - 1)
        def _():
            @pl.when(q >= n_z)
            def _():
                to_z(q - n_z).wait_send()
            z_out[jj] = val.astype(bf16)
            to_z(q).start()

    def z_sum(r, xi):
        val = z_own[xi]
        for jj in range(n_z - 1):
            rcopy(z_out.at[0], z_in.at[r, xi, jj], zz_s.at[jj], zz_r.at[r, xi, jj], sibling).wait_recv()
            val = val + z_in[r, xi, jj].astype(f32)
        return val

    def x_stage(r):
        @pl.when(r > 0)
        def _():
            to_x(0).wait_send()
        with scope('x_stage'):
            x_out[...] = z_sum(r, 0).astype(bf16)
        to_x(r).start()

    def home(tp, r):
        return gh_hbm.at[pl.ds(pl.multiple_of(tp * per_tp + r * half, half), half), :]

    def gathers(r):
        out = [rcopy(gh.at[r], home(at.tp, r), ag_s.at[r, n_z - 1], fw_r.at[r, at.z], y_peer)]
        for jj in range(n_z - 1):
            to = lax.rem(at.z + jj + 1, n_z)
            out.append(rcopy(gh.at[r], home(at.tp, r), ag_s.at[r, jj], ag_r.at[r, jj], dev(to * 2 + at.y, at.f)))
        return out

    def keep(r):
        return pltpu.make_async_copy(gh.at[r], home(at.tp, r), gh_sem.at[r])

    def from_z(jj):
        return lax.rem(at.z + n_z - jj - 1, n_z)

    def arrived(r, jj):
        return rcopy(gh.at[r], home(from_z(jj) * 2 + at.y, r), ag_s.at[r, jj], ag_r.at[r, jj], sibling)

    def onward(r, jj):
        here = home(from_z(jj) * 2 + at.y, r)
        return rcopy(here, here, fw_s.at[r, jj], fw_r.at[r, from_z(jj)], y_peer)

    def final(r):
        with scope('final_wait'):
            to_x(r).wait_recv()
            dz = z_sum(r, 1) + x_in[r].astype(f32)
        h = hid[pl.ds(pl.multiple_of(r * half, half), half), :].astype(f32)
        inv = lax.rsqrt(jnp.mean(h * h, axis=-1, keepdims=True) + NORM_EPS)
        normed = h * inv
        a = dz * gain[...].astype(f32)
        gh[r] = (inv * (a - normed * jnp.mean(a * normed, axis=-1, keepdims=True))).astype(bf16)
        gg[0:1, 0:gain.shape[1]] += jnp.sum(dz * normed, axis=0, keepdims=True)
        keep(r).start()

    def gather_start(r):
        for cp in gathers(r):
            cp.start()

    def forwards(r):
        for jj in range(n_z - 1):
            with scope('fw_wait'):
                arrived(r, jj).wait_recv()
            onward(r, jj).start()

    gg[...] = jnp.zeros(gg.shape, f32)
    gg[0:1, gain.shape[1]:] = hit_sum[...]
    last = rounds * groups
    for b in (0, 1):
        for cp in block_loads(0, b):
            cp.start()

    def dz_group(q, _):
        for b in (0, 1):
            with scope('a_wait'):
                for cp in block_loads(q, b):
                    cp.wait()

                @pl.when(q > 0)
                def _():
                    for cp in block_saves(q - 1, b):
                        cp.wait()
            slot = lax.rem(q, 2)
            if b == 0:
                @pl.when(q >= 2)
                def _():
                    to_sib(q - 2).wait_send()
                with scope('a_dot0'):
                    sib_out[slot] = block_dot(q, b).astype(bf16)
                to_sib(q).start()
            else:
                @pl.when(q >= 2)
                def _():
                    to_y(q - 2).wait_send()
                with scope('a_dot1'):
                    pair_sum[...] = block_dot(q, b)
                with scope('sib_wait'):
                    to_sib(q).wait_recv()
                val = pair_sum[...] + sib_in[slot].astype(f32)
                y_out[slot] = val[0:half].astype(bf16)
                part[lax.rem(q, part.shape[0])] = val[half:]
                to_y(q).start()
            for cp in block_saves(q, b):
                cp.start()

            @pl.when(q + 1 < last)
            def _():
                for cp in block_loads(q + 1, b):
                    cp.start()

        @pl.when(q == 0)
        def _():
            flush(early - 1, chunk)

        @pl.when(q >= 2)
        def _():
            z_stage(q - 2)

        @pl.when(q == groups + 2)
        def _():
            x_stage(0)

        @pl.when(q == last - 2)
        def _():
            final(0)
        return 0

    lax.fori_loop(0, last, dz_group, 0)
    x_stage(1)
    gather_start(0)
    for b in (0, 1):
        for cp in block_saves(last - 1, b):
            cp.wait()

    def stored(lo, name, tile_fn, after, mid):
        for b in (0, 1):
            load_g(lo * chunk, chunk, b, b).start()

        def one(c, _):
            def pair(i, _):
                for b in (0, 1):
                    k = 2 * i + b
                    with scope(name + '_wait'):
                        load_g(0, chunk, 0, b).wait()
                    with scope(name + '_tile'):
                        tile_fn(c * chunk, chunk, k, b)
                    wrap = k + 2 >= n_tok
                    c2, k2 = jnp.where(wrap, c + 1, c), jnp.where(wrap, k + 2 - n_tok, k + 2)

                    @pl.when(c2 < sz.full)
                    def _():
                        load_g(c2 * chunk, chunk, k2, b).start()

                    @pl.when(c2 == sz.full)
                    def _():
                        load_g(row_rem, sz.rem, k2, b).start()

                @pl.when(i == 0)
                def _():
                    mid(c)
                return 0
            lax.fori_loop(0, n_tok // 2, pair, 0)
            after(c, chunk)
            return 0
        lax.fori_loop(lo, sz.full, one, 0)

        def pair(i, _):
            for b in (0, 1):
                k = 2 * i + b
                load_g(row_rem, sz.rem, 0, b).wait()
                tile_fn(row_rem, sz.rem, k, b)

                @pl.when(k + 2 < n_tok)
                def _():
                    load_g(row_rem, sz.rem, k + 2, b).start()

            @pl.when(i == 0)
            def _():
                mid(sz.full)
            return 0
        lax.fori_loop(0, n_tok // 2, pair, 0)
        after(sz.full, sz.rem)

    late = min(3, sz.full - early - 1)

    def ship_and_sum(c, rows):
        ship(c, rows)
        if rows == chunk:
            @pl.when(c == early)
            def _():
                z_stage(last - 2)
                z_stage(last - 1)

            @pl.when(c == early + min(2, late))
            def _():
                final(1)
                gather_start(1)

            @pl.when(c == early + late)
            def _():
                forwards(0)

    def flush_before(c):
        @pl.when(c > early)
        def _():
            flush(c - 1, chunk)

    stored(early, 'b2', lambda row0, rows, k, b: tile(row0, rows, k, b, False), ship_and_sum, flush_before)

    def tell_gain(k):
        tp, f = at.other(k)
        return rcopy(gg, gg_in.at[at.index], gain_s.at[k], gain_r.at[k], dev(tp, f))

    def heard_gain(k):
        i = lax.rem(at.index + at.n_all - k, at.n_all)
        return rcopy(gg, gg_in.at[i], gain_s.at[k], gain_r.at[k], sibling)

    def every(fn):
        def go(k, _):
            fn(k)
            return 0
        lax.fori_loop(1, at.n_all, go, 0)

    every(lambda k: tell_gain(k).start())
    gg_in[at.index] = gg[...]

    def tile_own(row0, rows, k, b):
        mid = rows // 32 * 16
        for r0, r1 in ((0, mid), (mid, rows)):
            acc_own[r0:r1, :] += dot_nn(gbufs[b][r0:r1, :], z[cols(k, tok), n_far + width:])

    def put_own(slot, row0, rows):
        return pltpu.make_async_copy(stage_own.at[slot, pl.ds(0, rows), :], dw_hbm.at[rows_at(me * sz.rows + row0, rows), :], own_sem.at[slot])

    def ship_own(c, rows):
        slot = lax.rem(c, 2)

        @pl.when(c >= 2)
        def _():
            put_own(slot, 0, chunk).wait()
        stage_own[slot, 0:rows, :] = acc_own[0:rows, :].astype(bf16)
        acc_own[...] = jnp.zeros(acc_own.shape, f32)
        put_own(slot, c * chunk, rows).start()
        if rows == chunk:
            @pl.when(c == min(5, sz.full - 1))
            def _():
                forwards(rounds - 1)

    acc_own[...] = jnp.zeros(acc_own.shape, f32)

    def flush_last(c):
        @pl.when(c == 0)
        def _():
            flush(sz.full, sz.rem)

    stored(0, 'own', tile_own, ship_own, flush_last)

    with scope('t_gain'):
        every(lambda k: heard_gain(k).wait_recv())
    total = jnp.sum(gg_in[...], axis=0)
    lse_sum = jnp.sum(st[2:3, :] * st[1:2, :], axis=1, keepdims=True)
    gg_out[0:1, 0:gain.shape[1]] = total[0:1, 0:gain.shape[1]]
    gg_out[0:1, gain.shape[1]:] = (lse_sum - total[0:1, gain.shape[1]:]) * (1.0 / LOG2E)
    every(lambda k: tell_gain(k).wait_send())
    put_own((sz.full - 1) % 2, 0, chunk).wait()
    put_own(sz.full % 2, 0, sz.rem).wait()
    with scope('t_send'):
        def sent(c, _):
            for cp in sends(c, chunk):
                cp.wait_send()
            return 0
        lax.fori_loop(0, sz.full, sent, 0)
        for cp in sends(sz.full, sz.rem):
            cp.wait_send()
    for q in (last - 2, last - 1):
        to_sib(q).wait_send()
        to_y(q).wait_send()
    for q in range(last - n_z, last - 1):
        to_z(q).wait_send()
    to_x(rounds - 1).wait_send()
    for r in range(rounds):
      with scope(f't_gather{r}'):
        keep(r).wait()
        for cp in gathers(r):
            cp.wait_send()
        for jj in range(n_z - 1):
            onward(r, jj).wait_send()
        for zf in range(n_z):
            rcopy(gh.at[r], home(zf * 2 + 1 - at.y, r), ag_s.at[r, 0], fw_r.at[r, zf], y_peer).wait_recv()
    for k in range(1, n):
      with scope(f't_dw{k}'):
        src = lax.rem(me + n - k, n)
        rcopy(dw_hbm.at[pl.ds(0, sz.rows), :], dw_hbm.at[rows_at(src * sz.rows, sz.rows), :], dw_send.at[0, 0], dw_recv.at[k], sibling).wait_recv()


HBM = pl.BlockSpec(memory_space=pl.ANY)
VM = pl.BlockSpec(memory_space=pltpu.VMEM)
DMA = pltpu.SemaphoreType.DMA


def params(**kw):
    return pltpu.CompilerParams(vmem_limit_bytes=VMEM_LIMIT, **kw)


def solution(mesh, chunk=CHUNK, tok=TOK, early=EARLY, z_rows=Z_ROWS):
    n_fsdp, n_tp = mesh.shape['fsdp'], mesh.shape['tp']
    n_all, n_z = n_fsdp * n_tp, n_tp // 2
    everyone = ('fsdp', 'tp')
    S = jax.ShapeDtypeStruct

    def per_device(hidden, labels, tok_mask, norm_gain, w_rows):
        fsdp_id, tp_id = lax.axis_index('fsdp'), lax.axis_index('tp')
        d = hidden.shape[1]
        width, vocab_tp = w_rows.shape
        tokens = hidden.shape[0] * n_fsdp
        sz = Sizes(vocab_tp, n_fsdp, chunk)
        own = hidden.shape[0] // n_tp
        half = own // 2
        rounds = 2
        hid_own = lax.dynamic_slice_in_dim(hidden, tp_id * own, own, 0)
        hid_all = lax.all_gather(hid_own, everyone, axis=0, tiled=True)
        lab_all = lax.all_gather(labels, 'fsdp', axis=0, tiled=True)
        mask_all = lax.all_gather(tok_mask, 'fsdp', axis=0, tiled=True)
        scale = (mask_all / jnp.sum(mask_all))[None, :]
        mine = lab_all // vocab_tp == tp_id
        lab_loc = jnp.where(mine, lab_all - tp_id * vocab_tp - fsdp_id * sz.rows, -1)[None, :]
        V = pltpu.VMEM

        logits, z_all, w_blk, st, hit_sum = pl.pallas_call(
            functools.partial(logits_kernel, sz, n_tp, chunk, tok),
            out_shape=(S((sz.rows, tokens), f32), S((tokens, d), bf16), S((sz.rows, d), bf16), S((8, tokens), f32), S((1, 128), f32)),
            in_specs=[HBM, HBM, VM, VM, VM], out_specs=(HBM, HBM, HBM, VM, VM),
            scratch_shapes=[V((tokens, d), bf16), V((sz.rows, d), bf16), V((chunk, tok), f32), V((chunk, tok), f32),
                            V((z_rows, d), bf16), V((z_rows, d), bf16),
                            V((8, tokens), f32), V((8, tokens), f32), V((8, tokens), f32),
                            V((2, tokens), f32), V((n_all, 2, own), f32), V((1, own), f32), V((1, tokens), f32),
                            DMA((sz.full + 2, n_fsdp)), DMA((sz.full + 2, n_fsdp)), DMA((sz.full + 2,)), DMA((2,)), DMA((2,)), DMA((2,)),
                            DMA((n_all,)), DMA((n_all,)), DMA((n_all,)), DMA((n_all,))],
            compiler_params=params(collective_id=0, has_side_effects=True), name='logits',
        )(hid_all, w_rows.T, norm_gain[None, :], lab_loc, scale)

        n_low = sz.full - early + 1

        _, dw_t, grad_hidden, gain_sum, _ = pl.pallas_call(
            functools.partial(grad_kernel, sz, n_tp, chunk, early, tok, tok, half),
            out_shape=(S((sz.rows, tokens), bf16), S((n_fsdp * sz.rows, width), bf16), S(hidden.shape, bf16), S((1, d + 128), f32), S(((sz.full + 1) * chunk, 3 * width), bf16)),
            in_specs=[HBM, HBM, HBM, VM, VM, VM, VM, VM], out_specs=(HBM, HBM, HBM, VM, HBM),
            scratch_shapes=[V((tokens, d), bf16), V((sz.rows, d), bf16), V((chunk, tok), f32), V((chunk, tok), f32), V((chunk, tok), bf16), V((chunk, tok), bf16),
                            V((sz.rows, 2 * half), bf16), V((sz.rows, 2 * half), bf16),
                            V((chunk, 3 * width), f32), V((2, chunk, 3 * width), bf16), V((chunk, width), f32), V((2, chunk, width), bf16),
                            V((2, 2 * half, d), bf16), V((2, 2 * half, d), bf16), V((2 * half, d), f32), V((2, half, d), bf16), V((8, half, d), bf16), V((3, half, d), f32),
                            V((n_z - 1, half, d), bf16), V((rounds, 2, n_z - 1, half, d), bf16), V((2, half, d), f32), V((half, d), bf16), V((rounds, half, d), bf16),
                            V((rounds, half, d), bf16), V((1, d + 128), f32), V((n_all, 1, d + 128), f32),
                            DMA((3,)), DMA((1,)), DMA((2,)), DMA((2,)), DMA((2, 2)), DMA((2, 2 * n_low)), DMA((2, 2)),
                            DMA((2,)), DMA((sz.full + 1, 3)), DMA((n_fsdp,)), DMA((2,)), DMA((2,)), DMA((2,)), DMA((2,)), DMA((8,)),
                            DMA((n_z - 1,)), DMA((rounds, 2, n_z - 1)), DMA((1,)), DMA((rounds,)),
                            DMA((rounds, n_z)), DMA((rounds, n_z)), DMA((rounds, n_z)), DMA((rounds, n_z)), DMA((rounds,)), DMA((n_all,)), DMA((n_all,))],
            compiler_params=params(collective_id=1, has_side_effects=True), name='grads',
        )(z_all, w_blk, logits, st, lab_loc, hid_own, norm_gain[None, :], hit_sum)
        return gain_sum[0, d], grad_hidden, dw_t[:vocab_tp].T, gain_sum[0, :d]

    return jax.shard_map(per_device, mesh=mesh, in_specs=(P('fsdp', None), P('fsdp'), P('fsdp'), P(), P('fsdp', 'tp')), out_specs=(P(), P('fsdp', None), P('fsdp', 'tp'), P()), check_vma=False)
```

```python
import functools

import jax
import jax.numpy as jnp
from jax import lax
from jax.experimental import pallas as pl
from jax.experimental.pallas import tpu as pltpu
from jax.sharding import PartitionSpec as P

NORM_EPS = 1e-6
LOG2E = 1.4426950408889634
NEG = -1e30
CHUNK = 512
TOK = 1024
EARLY = 4
AHEAD = 5
ROUNDS = 2
VMEM_LIMIT = 67_043_328
MESH = pl.DeviceIdType.MESH
scope = jax.named_scope
f32, bf16 = jnp.float32, jnp.bfloat16


def dot_nt(a, b):
    return lax.dot_general(a, b, (((1,), (1,)), ((), ())), preferred_element_type=f32)


def dot_tn(a, b):
    return lax.dot_general(a, b, (((0,), (0,)), ((), ())), preferred_element_type=f32)


def dot_nn(a, b):
    return lax.dot_general(a, b, (((1,), (0,)), ((), ())), preferred_element_type=f32)


def cols(k, size):
    return pl.ds(pl.multiple_of(k * size, size), size)


def rows_at(row0, rows):
    return pl.ds(pl.multiple_of(row0, 16), rows)


class Sizes:
    def __init__(self, vocab_tp, n_fsdp, chunk):
        self.n = n_fsdp
        self.rows = -(-vocab_tp // (n_fsdp * 16)) * 16
        self.short = n_fsdp * self.rows - vocab_tp
        self.full = self.rows // chunk
        self.rem = self.rows - self.full * chunk
        self.solid = self.rem - self.short
        assert self.rem > self.short and self.rem % 16 == 0 and self.short % 16 == 0


class Place:
    def __init__(self, n_fsdp, n_tp):
        self.n_fsdp, self.n_tp, self.n_all = n_fsdp, n_tp, n_fsdp * n_tp
        self.f, self.tp = lax.axis_index('fsdp'), lax.axis_index('tp')
        self.x, self.c = self.f // 2, lax.rem(self.f, 2)
        self.n_z = n_tp // 2
        self.z, self.y = self.tp // 2, lax.rem(self.tp, 2)
        self.index = self.tp * n_fsdp + self.f

    def other(self, k):
        i = lax.rem(self.index + k, self.n_all)
        return i // self.n_fsdp, lax.rem(i, self.n_fsdp)

    def every(self, fn):
        def go(k, _):
            fn(k)
            return 0
        lax.fori_loop(1, self.n_all, go, 0)


def dev(tp, f):
    return {'tp': tp, 'fsdp': f}


def rcopy(src, dst, ssem, rsem, to):
    return pltpu.make_async_remote_copy(src_ref=src, dst_ref=dst, send_sem=ssem, recv_sem=rsem, device_id=to, device_id_type=MESH)


def enter(at):
    barrier = pltpu.get_barrier_semaphore()

    def tell(k):
        tp, f = at.other(k)
        pl.semaphore_signal(barrier, inc=1, device_id=dev(tp, f), device_id_type=MESH)

    at.every(tell)
    pl.semaphore_wait(barrier, at.n_all - 1)


def head_kernel(sz, n_tp, vocab_tp, chunk, tok, early,
                h_hbm, lab_ref, mask_ref, gain, w_hbm,
                dw_hbm, gh_hbm, gg_out, l_hbm, g_hbm, h_all, ds_hbm,
                z, w, l0, l1, l2, l3, g0, g1, g2, g3, q0, q1, m, s, scale, lab, lab_in, mask_in, st_loc, got, res, st, top_row, hit, hid,
                acc, stage, sib_out, sib_in, y_sum, y_out, y_in, part, z_out, z_in, z_own, x_out, x_in, gh, gg, gg_in,
                w_s, w_r, loc, hsem, lsem, gsem, qsem, bsem, vsem, ssend, srecv, rsend, rrecv, tok_s, tok_r, blk, hx_s, hx_r, hz_s, hz_r, hy_s, hy_r, hc_s, hc_r,
                hid_sem, dw_copy, dw_send, dw_recv, own_sem, sib_s, sib_r, y_s, y_r, zz_s, zz_r, x_s, x_r, ag_s, ag_r, fw_s, fw_r, gh_sem, gain_s, gain_r):
    at = Place(sz.n, n_tp)
    me, n, n_z, width = at.f, sz.n, at.n_z, w_hbm.shape[1]
    per_f, d = h_hbm.shape
    tokens, own = per_f * n, per_f // n_tp
    lbufs, gbufs, qbufs, hbufs = (l0, l1, l2, l3), (g0, g1, g2, g3), (q0, q1), (sib_out.at[0], sib_out.at[1])
    far, sib = 1 - at.x, at.x * 2 + 1 - at.c
    through = far * 2 + at.c
    sibling, y_peer, x_peer = dev(at.tp, sib), dev(at.z * 2 + 1 - at.y, me), dev(at.tp, through)
    row_rem = sz.full * chunk
    row_odd = row_rem + sz.solid

    with scope('enter'):
        enter(at)

    def slab(f, tp):
        return pl.ds(pl.multiple_of((f * n_tp + tp) * own, own), own)

    def block(f):
        return pl.ds(pl.multiple_of(f * per_f, per_f), per_f)

    def h_to_x():
        return rcopy(h_hbm.at[pl.ds(pl.multiple_of(at.tp * own, own), own), :], h_all.at[slab(me, at.tp), :], hx_s.at[0], hx_r.at[0], x_peer)

    def h_from_x():
        return rcopy(h_all.at[slab(through, at.tp), :], h_all.at[slab(through, at.tp), :], hx_s.at[0], hx_r.at[0], x_peer)

    def block_out():
        return rcopy(h_hbm, h_all.at[block(me), :], blk.at[0], blk.at[1], sibling)

    def block_in():
        return rcopy(h_hbm, h_all.at[block(sib), :], blk.at[0], blk.at[1], sibling)

    def moved(tp, ssem, rsem, to):
        here = h_all.at[slab(through, tp), :]
        return rcopy(here, here, ssem, rsem, to)

    def z_from(jj):
        return lax.rem(at.z + n_z - jj - 1, n_z)

    def h_to_z(jj):
        return moved(at.tp, hz_s.at[jj], hz_r.at[jj], dev(lax.rem(at.z + jj + 1, n_z) * 2 + at.y, me))

    def h_from_z(jj):
        return moved(z_from(jj) * 2 + at.y, hz_s.at[jj], hz_r.at[jj], sibling)

    def h_to_y(zo):
        return moved(zo * 2 + at.y, hy_s.at[zo], hy_r.at[zo], y_peer)

    def h_from_y(zo):
        return moved(zo * 2 + 1 - at.y, hy_s.at[zo], hy_r.at[zo], y_peer)

    def h_to_core(tp):
        return moved(tp, hc_s.at[tp], hc_r.at[tp], sibling)

    def h_from_core(tp):
        here = h_all.at[slab(far * 2 + 1 - at.c, tp), :]
        return rcopy(here, here, hc_s.at[tp], hc_r.at[tp], sibling)

    def tok_out(k):
        to = dev(at.tp, lax.rem(me + k, n))
        return [rcopy(lab_ref, lab_in.at[me], tok_s.at[0, k], tok_r.at[0, k], to), rcopy(mask_ref, mask_in.at[me], tok_s.at[1, k], tok_r.at[1, k], to)]

    def tok_in(k):
        src = lax.rem(me + n - k, n)
        return [rcopy(lab_ref, lab_in.at[src], tok_s.at[0, k], tok_r.at[0, k], sibling), rcopy(mask_ref, mask_in.at[src], tok_s.at[1, k], tok_r.at[1, k], sibling)]

    h_to_x().start()
    block_out().start()
    for k in range(1, n):
        for cp in tok_out(k):
            cp.start()
    lab_in[me] = lab_ref[...]
    mask_in[me] = mask_ref[...]

    def remote(k, c, row0, rows):
        dest = lax.rem(me + k, n)
        return rcopy(w_hbm.at[rows_at(dest * sz.rows + row0, rows), :], w.at[rows_at(row0, rows), cols(me, width)], w_s.at[c, k], w_r.at[c, k], dev(at.tp, dest))

    def arrival(k, c, row0, rows):
        src = lax.rem(me + n - k, n)
        return rcopy(w_hbm.at[pl.ds(0, rows), :], w.at[rows_at(row0, rows), cols(src, width)], w_s.at[c, k], w_r.at[c, k], sibling)

    def local(c, row0, rows):
        return pltpu.make_async_copy(w_hbm.at[rows_at(me * sz.rows + row0, rows), :], w.at[rows_at(row0, rows), cols(me, width)], loc.at[c])

    def issue(c):
        local(c, c * chunk, chunk).start()
        for k in range(1, n):
            remote(k, c, c * chunk, chunk).start()

    def when_not_last(dest, fn):
        if sz.short:
            pl.when(dest != n - 1)(fn)

    def issue_rem():
        local(sz.full, row_rem, sz.solid).start()
        when_not_last(me, lambda: local(sz.full + 1, row_odd, sz.short).start())
        for k in range(1, n):
            remote(k, sz.full, row_rem, sz.solid).start()
            when_not_last(lax.rem(me + k, n), lambda: remote(k, sz.full + 1, row_odd, sz.short).start())

    ahead = min(AHEAD, sz.full)
    for c in range(ahead):
        issue(c)
    if sz.short:
        @pl.when(me == n - 1)
        def _():
            w[row_odd:, :] = jnp.zeros((sz.short, d), bf16)

    sub = min(256, own)
    slices, per_own = per_f // sub, own // sub
    lane = min(128, sub)

    def place(t, i):
        near = jnp.where(t == 0, me, sib) * per_f + i * sub
        j = i // per_own
        f = jnp.where(j < n_z, through, far * 2 + 1 - at.c)
        y = jnp.where(t == 2, at.y, 1 - at.y)
        away = (f * n_tp + lax.rem(j, n_z) * 2 + y) * own + lax.rem(i, per_own) * sub
        return pl.multiple_of(jnp.where(t < 2, near, away), sub)

    def norm(t):
        def load(i, b):
            if t == 0:
                return pltpu.make_async_copy(h_hbm.at[cols(i, sub), :], hbufs[b], hsem.at[b])
            return pltpu.make_async_copy(h_all.at[pl.ds(place(t, i), sub), :], hbufs[b], hsem.at[b])

        load(0, 0).start()
        load(1, 1).start()

        def pair(i2, _):
            for b in (0, 1):
                i = 2 * i2 + b
                load(i, b).wait()
                h = hbufs[b][...].astype(f32)
                inv = lax.rsqrt(jnp.mean(h * h, axis=-1, keepdims=True) + NORM_EPS)
                z[pl.ds(place(t, i), sub), :] = (h * inv * gain[...].astype(f32)).astype(bf16)

                @pl.when(i + 2 < slices)
                def _():
                    load(i + 2, b).start()
            return 0

        with scope(f'norm{t}'):
            lax.fori_loop(0, slices // 2, pair, 0)

    norm(0)
    with scope('blk_wait'):
        block_in().wait_recv()
    norm(1)
    with scope('x_wait'):
        h_from_x().wait_recv()
    for jj in range(n_z - 1):
        h_to_z(jj).start()
    h_to_y(at.z).start()
    h_to_core(at.tp).start()
    with scope('tok_wait'):
        for k in range(1, n):
            for cp in tok_in(k):
                cp.wait_recv()
    count = jnp.sum(mask_in[...], axis=(0, 2), keepdims=True)[0]
    for f in range(n):
        here = pl.ds(f * per_f, per_f)
        scale[0:1, here] = mask_in[f] / count
        rel = lab_in[f] - at.tp * vocab_tp
        lab[0:1, here] = jnp.where(jnp.logical_and(rel >= 0, rel < vocab_tp), rel - me * sz.rows, -1)

    def spread_z():
        with scope('z_wait'):
            for jj in range(n_z - 1):
                h_from_z(jj).wait_recv()
                h_to_y(z_from(jj)).start()
                h_to_core(z_from(jj) * 2 + at.y).start()

    def spread_y():
        with scope('hy_wait'):
            for k in range(n_z):
                zo = lax.rem(at.z + n_z - k, n_z)
                h_from_y(zo).wait_recv()
                h_to_core(zo * 2 + 1 - at.y).start()

    def far_ready(y):
        with scope('core_wait'):
            for zo in range(n_z):
                h_from_core(zo * 2 + y).wait_recv()

    m[...] = jnp.full(m.shape, NEG, f32)
    s[...] = jnp.zeros(s.shape, f32)
    per_buf = tok // sub
    n_buf = slices // per_buf

    def out_copies(row0, rows, t, b):
        return [pltpu.make_async_copy(lbufs[b * n_buf + i // per_buf].at[pl.ds(0, rows), pl.ds(i % per_buf * sub, sub)],
                                      l_hbm.at[rows_at(row0, rows), pl.ds(place(t, i), sub)], lsem.at[b * n_buf + i // per_buf]) for i in range(slices)]

    def out_done(rows, b):
        for i in range(n_buf):
            pltpu.make_async_copy(lbufs[b * n_buf + i].at[pl.ds(0, rows), :], l_hbm.at[pl.ds(0, rows), pl.ds(0, tok)], lsem.at[b * n_buf + i]).wait()

    def logits_tile(row0, rows, t, b, masked):
        group = min(4, rows // 8)
        for i in range(slices):
            t0 = place(t, i)
            logits = dot_nt(w[rows_at(row0, rows), :], z[pl.ds(t0, sub), :]) * LOG2E
            if masked:
                ids = lax.broadcasted_iota(jnp.int32, (rows, sub), 0)
                logits = jnp.where(ids < jnp.where(me == n - 1, sz.solid, sz.rem), logits, NEG)
            i0 = i % per_buf * sub
            lbufs[b * n_buf + i // per_buf][0:rows, i0:i0 + sub] = logits
            for c1 in range(0, sub, lane):
                sl = pl.ds(pl.multiple_of(t0 + c1, lane), lane)
                big, tot = m[:, sl], s[:, sl]
                for g in range(0, rows // 8, group):
                    piece = [logits[8 * r:8 * r + 8, c1:c1 + lane] for r in range(g, min(g + group, rows // 8))]
                    new = functools.reduce(jnp.maximum, piece, big)
                    tot = tot * jnp.exp2(big - new)
                    for x in piece:
                        tot += jnp.exp2(x - new)
                    big = new
                m[:, sl], s[:, sl] = big, tot

    n_a = min(3, sz.full)
    n_c = min(3, sz.full - n_a)
    k_b, k_c = 2 * n_a, 3 * n_a
    k_d = k_c + 3 * n_c
    k_e = k_d + n_a + n_c

    def item(k):
        u, v = k - k_c, k - k_e
        c = jnp.where(k < k_b, k // 2, jnp.where(k < k_c, k - k_b, jnp.where(k < k_d, n_a + u // 3, jnp.where(k < k_e, k - k_d, n_a + n_c + v // 4))))
        t = jnp.where(k < k_b, lax.rem(k, 2), jnp.where(k < k_c, 2, jnp.where(k < k_d, lax.rem(u, 3), jnp.where(k < k_e, 3, lax.rem(v, 4)))))
        return c, t

    def work(i2, _):
        for b in (0, 1):
            k = 2 * i2 + b
            c, t = item(k)

            @pl.when(t == 0)
            def _():
                with scope('w_wait'):
                    local(c, c * chunk, chunk).wait()
                    for j in range(1, n):
                        arrival(j, c, c * chunk, chunk).wait_recv()

                @pl.when(c + ahead < sz.full)
                def _():
                    issue(c + ahead)

                @pl.when(c + ahead == sz.full)
                def _():
                    issue_rem()

            @pl.when(k == k_b)
            def _():
                spread_z()
                far_ready(at.y)
                norm(2)

            @pl.when(k == max(k_d - 3, k_c))
            def _():
                spread_y()

            @pl.when(k == k_d)
            def _():
                far_ready(1 - at.y)
                norm(3)

            with scope('l_wait'):
                @pl.when(k >= 2)
                def _():
                    out_done(chunk, b)
            with scope('l_tile'):
                logits_tile(c * chunk, chunk, t, b, False)
            for cp in out_copies(c * chunk, chunk, t, b):
                cp.start()
        return 0

    lax.fori_loop(0, sz.full * 2, work, 0)
    with scope('w_wait_rem'):
        local(sz.full, row_rem, sz.solid).wait()
        when_not_last(me, lambda: local(sz.full + 1, row_odd, sz.short).wait())
        for k in range(1, n):
            arrival(k, sz.full, row_rem, sz.solid).wait_recv()
            when_not_last(me, lambda: arrival(k, sz.full + 1, row_odd, sz.short).wait_recv())

    def work_rem(i2, _):
        for b in (0, 1):
            @pl.when(i2 == 0)
            def _():
                out_done(chunk, b)

            @pl.when(i2 > 0)
            def _():
                out_done(sz.rem, b)
            logits_tile(row_rem, sz.rem, 2 * i2 + b, b, True)
            for cp in out_copies(row_rem, sz.rem, 2 * i2 + b, b):
                cp.start()
        return 0

    with scope('l_rem'):
        lax.fori_loop(0, 2, work_rem, 0)

    big = jnp.max(m[...], axis=0, keepdims=True)
    st_loc[0:1, :] = big
    st_loc[1:2, :] = jnp.sum(s[...] * jnp.exp2(m[...] - big), axis=0, keepdims=True)
    mine = slab(at.f, at.tp)

    def ask(k):
        tp, f = at.other(k)
        return rcopy(st_loc.at[:, slab(f, tp)], got.at[k], ssend.at[k], srecv.at[k], dev(tp, f))

    def answer(k):
        tp, f = at.other(k)
        return rcopy(res, st.at[:, mine], rsend.at[k], rrecv.at[k], dev(tp, f))

    def answered(k):
        tp, f = at.other(at.n_all - k)
        return rcopy(res, st.at[:, slab(f, tp)], rsend.at[k], rrecv.at[k], dev(tp, f))

    n_tok = tokens // tok

    def load_l(row0, rows, k, b):
        return pltpu.make_async_copy(l_hbm.at[rows_at(row0, rows), cols(k, tok)], lbufs[b].at[pl.ds(0, rows), :], lsem.at[b])

    def load_g(row0, rows, k, b):
        return pltpu.make_async_copy(g_hbm.at[rows_at(row0, rows), cols(k, tok)], gbufs[b].at[pl.ds(0, rows), :], gsem.at[b])

    def save_g(row0, rows, k, b):
        return pltpu.make_async_copy(gbufs[b].at[pl.ds(0, rows), :], g_hbm.at[rows_at(row0, rows), cols(k, tok)], gsem.at[b])

    at.every(lambda k: ask(k).start())
    got[0] = st_loc[:, mine]
    for b in (0, 1):
        out_done(sz.rem, b)
    for b in range(4):
        load_l(0, chunk, b, b).start()
    h_load = pltpu.make_async_copy(h_hbm.at[pl.ds(pl.multiple_of(at.tp * own, own), own), :], hid, hid_sem.at[0])
    h_load.start()
    acc[...] = jnp.zeros(acc.shape, f32)
    hit[...] = jnp.zeros(hit.shape, f32)
    with scope('ask_wait'):
        at.every(lambda k: ask(k).wait_recv())
    tops = got[:, 0:1, :]
    top = jnp.max(tops, axis=0)
    res[...] = top + jnp.log2(jnp.sum(got[:, 1:2, :] * jnp.exp2(tops - top[None]), axis=0))
    at.every(lambda k: answer(k).start())
    st[:, mine] = res[...]
    with scope('answer_wait'):
        at.every(lambda k: answered(k).wait_recv())
    top_row[...] = st[...] - jnp.log2(scale[...])

    def gradient(x, sl, row0):
        rows = x.shape[0]
        sc = scale[0:1, sl]
        x3 = x.reshape(rows // 8, 8, x.shape[1])
        p = jnp.exp2(x3 - top_row[0:1, sl][None])
        is_label = lax.broadcasted_iota(jnp.int32, p.shape, 0) * 8 == (lab[0:1, sl] - row0 - lax.broadcasted_iota(jnp.int32, (8, x.shape[1]), 0))[None]
        hit[...] += jnp.sum(jnp.where(is_label, x3, 0.0), axis=0) * sc
        return jnp.where(is_label, p - sc[None], p).reshape(x.shape).astype(bf16)

    step = min(256, tok)

    def grad_tile(row0, rows, k, b, fresh):
        total = None
        for c0 in range(0, tok, step):
            if fresh:
                for c1 in range(c0, c0 + step, lane):
                    gbufs[b][0:rows, c1:c1 + lane] = gradient(lbufs[b][0:rows, c1:c1 + lane], pl.ds(pl.multiple_of(k * tok + c1, lane), lane), row0)
            p = dot_nn(gbufs[b][0:rows, c0:c0 + step], z[pl.ds(pl.multiple_of(k * tok + c0, step), step), :])
            total = p if total is None else total + p
        acc[0:rows, :] += total

    def aside(c, rows):
        slot = lax.rem(c, 2)
        return pltpu.make_async_copy(stage.at[slot, pl.ds(0, rows), :], ds_hbm.at[rows_at(c * chunk, rows), :], dw_copy.at[slot])

    def keep_own(c, rows):
        slot = lax.rem(c, 2)
        return pltpu.make_async_copy(stage.at[slot, pl.ds(0, rows), cols(me, width)], dw_hbm.at[rows_at(me * sz.rows + c * chunk, rows), :], own_sem.at[slot])

    def sends(c, rows):
        out = []
        for i, f in enumerate((far * 2, far * 2 + 1, sib)):
            out.append(rcopy(ds_hbm.at[rows_at(c * chunk, rows), cols(f, width)], dw_hbm.at[rows_at(me * sz.rows + c * chunk, rows), :],
                             dw_send.at[c, i], dw_recv.at[lax.rem(f + n - me, n)], dev(at.tp, f)))
        return out

    def ship(c, rows):
        with scope('ship'):
            stage[lax.rem(c, 2), 0:rows, :] = acc[0:rows, :].astype(bf16)
            acc[...] = jnp.zeros(acc.shape, f32)
        aside(c, rows).start()
        keep_own(c, rows).start()

    def flush(c, rows):
        aside(c, rows).wait()
        keep_own(c, rows).wait()
        for cp in sends(c, rows):
            cp.start()

    def early_chunk(c, _):
        def quad(i, _):
            for b in range(4):
                k = 4 * i + b
                with scope('b1_wait'):
                    load_l(0, chunk, 0, b).wait()

                    @pl.when(jnp.logical_not(jnp.logical_and(c == 0, i == 0)))
                    def _():
                        save_g(0, chunk, 0, b).wait()
                with scope('b1_tile'):
                    grad_tile(c * chunk, chunk, k, b, True)
                save_g(c * chunk, chunk, k, b).start()
                wrap = k + 4 >= n_tok
                c2 = jnp.where(wrap, c + 1, c)

                @pl.when(c2 < early)
                def _():
                    load_l(c2 * chunk, chunk, jnp.where(wrap, k + 4 - n_tok, k + 4), b).start()

            @pl.when(jnp.logical_and(i == 0, c > 0))
            def _():
                flush(c - 1, chunk)
            return 0
        lax.fori_loop(0, n_tok // 4, quad, 0)
        ship(c, chunk)
        return 0

    lax.fori_loop(0, early, early_chunk, 0)

    half = own // ROUNDS
    groups = 2 * n_z
    last = ROUNDS * groups
    row_low = early * chunk
    low = [(j, chunk) for j in range(sz.full - early)] + [(sz.full - early, sz.rem)]
    per_l = tok // half

    def group_of(q):
        r, g = q // groups, lax.rem(q, groups)
        xi, jj = g // n_z, lax.rem(g, n_z)
        return r, xi, jj, jnp.where(xi == 0, far, at.x), lax.rem(at.z + jj + 1, n_z)

    def pieces(q, b):
        r, _, _, xb, zb = group_of(q)
        cb = at.c if b == 1 else 1 - at.c
        return [pl.multiple_of((xb * 2 + cb) * per_f + (zb * 2 + yb) * own + r * half, half) for yb in (1 - at.y, at.y)]

    def l_part(b, j, i, rows):
        p = 2 * j + i
        return lbufs[2 * b + p // per_l].at[pl.ds(0, rows), pl.ds(p % per_l * half, half)]

    def block_loads(q, b):
        out = []
        for i, t0 in enumerate(pieces(q, b)):
            out.append(pltpu.make_async_copy(g_hbm.at[pl.ds(0, row_low), pl.ds(t0, half)], qbufs[b].at[pl.ds(0, row_low), pl.ds(i * half, half)], qsem.at[b, i]))
            for j, rows in low:
                out.append(pltpu.make_async_copy(l_hbm.at[pl.ds(row_low + j * chunk, rows), pl.ds(t0, half)], l_part(b, j, i, rows), bsem.at[b, 2 * j + i]))
        return out

    def block_saves(q, b):
        return [pltpu.make_async_copy(qbufs[b].at[pl.ds(row_low, sz.rows - row_low), pl.ds(i * half, half)],
                                      g_hbm.at[pl.ds(row_low, sz.rows - row_low), pl.ds(t0, half)], vsem.at[b, i]) for i, t0 in enumerate(pieces(q, b))]

    def block_dot(q, b):
        for i, t0 in enumerate(pieces(q, b)):
            for j, rows in low:
                row0 = row_low + j * chunk
                qbufs[b][row0:row0 + rows, i * half:(i + 1) * half] = gradient(l_part(b, j, i, rows)[...], pl.ds(t0, half), row0)
        return dot_tn(qbufs[b][...], w[...])

    def to_sib(q):
        slot = lax.rem(q, 2)
        return rcopy(sib_out.at[slot], sib_in.at[slot], sib_s.at[slot], sib_r.at[slot], sibling)

    def to_y(q):
        slot, land = lax.rem(q, 2), lax.rem(q, y_in.shape[0])
        return rcopy(y_out.at[slot], y_in.at[land], y_s.at[slot], y_r.at[land], y_peer)

    def to_z(q):
        r, xi, jj, _, zb = group_of(q)
        return rcopy(z_out.at[jj], z_in.at[r, xi, jj], zz_s.at[jj], zz_r.at[r, xi, jj], dev(zb * 2 + at.y, me))

    def to_x(r):
        return rcopy(x_out, x_in.at[r], x_s.at[0], x_r.at[r], x_peer)

    def z_stage(q):
        _, xi, jj, _, _ = group_of(q)
        with scope('y_wait'):
            to_y(q).wait_recv()
        val = part[lax.rem(q, part.shape[0])] + y_in[lax.rem(q, y_in.shape[0])].astype(f32)

        @pl.when(jj == n_z - 1)
        def _():
            z_own[xi] = val

        @pl.when(jj < n_z - 1)
        def _():
            @pl.when(q >= n_z)
            def _():
                to_z(q - n_z).wait_send()
            z_out[jj] = val.astype(bf16)
            to_z(q).start()

    def z_sum(r, xi):
        val = z_own[xi]
        for jj in range(n_z - 1):
            rcopy(z_out.at[0], z_in.at[r, xi, jj], zz_s.at[jj], zz_r.at[r, xi, jj], sibling).wait_recv()
            val = val + z_in[r, xi, jj].astype(f32)
        return val

    def x_stage(r):
        @pl.when(r > 0)
        def _():
            to_x(0).wait_send()
        with scope('x_stage'):
            x_out[...] = z_sum(r, 0).astype(bf16)
        to_x(r).start()

    def home(tp, r):
        return gh_hbm.at[pl.ds(pl.multiple_of(tp * own + r * half, half), half), :]

    def gathers(r):
        out = [rcopy(gh.at[r], home(at.tp, r), ag_s.at[r, n_z - 1], fw_r.at[r, at.z], y_peer)]
        for jj in range(n_z - 1):
            to = lax.rem(at.z + jj + 1, n_z)
            out.append(rcopy(gh.at[r], home(at.tp, r), ag_s.at[r, jj], ag_r.at[r, jj], dev(to * 2 + at.y, me)))
        return out

    def keep(r):
        return pltpu.make_async_copy(gh.at[r], home(at.tp, r), gh_sem.at[r])

    def arrived(r, jj):
        return rcopy(gh.at[r], home(z_from(jj) * 2 + at.y, r), ag_s.at[r, jj], ag_r.at[r, jj], sibling)

    def onward(r, jj):
        here = home(z_from(jj) * 2 + at.y, r)
        return rcopy(here, here, fw_s.at[r, jj], fw_r.at[r, z_from(jj)], y_peer)

    def final(r):
        with scope('final_wait'):
            to_x(r).wait_recv()
            dz = z_sum(r, 1) + x_in[r].astype(f32)
        h = hid[pl.ds(pl.multiple_of(r * half, half), half), :].astype(f32)
        inv = lax.rsqrt(jnp.mean(h * h, axis=-1, keepdims=True) + NORM_EPS)
        normed = h * inv
        a = dz * gain[...].astype(f32)
        gh[r] = (inv * (a - normed * jnp.mean(a * normed, axis=-1, keepdims=True))).astype(bf16)
        gg[0:1, 0:d] += jnp.sum(dz * normed, axis=0, keepdims=True)
        keep(r).start()
        for cp in gathers(r):
            cp.start()

    def forwards(r):
        for jj in range(n_z - 1):
            with scope('fw_wait'):
                arrived(r, jj).wait_recv()
            onward(r, jj).start()

    for b in range(4):
        save_g(0, chunk, 0, b).wait()
    h_load.wait()
    gg[...] = jnp.zeros(gg.shape, f32)
    for b in (0, 1):
        for cp in block_loads(0, b):
            cp.start()

    def dz_group(q, _):
        for b in (0, 1):
            with scope('a_wait'):
                for cp in block_loads(q, b):
                    cp.wait()

                @pl.when(q > 0)
                def _():
                    for cp in block_saves(q - 1, b):
                        cp.wait()
            slot = lax.rem(q, 2)
            if b == 0:
                @pl.when(q >= 2)
                def _():
                    to_sib(q - 2).wait_send()
                with scope('a_dot0'):
                    sib_out[slot] = block_dot(q, b).astype(bf16)
                to_sib(q).start()
            else:
                @pl.when(q >= 2)
                def _():
                    to_y(q - 2).wait_send()
                with scope('a_dot1'):
                    val = block_dot(q, b)
                    y_sum[...] = val[0:half]
                    part[lax.rem(q, part.shape[0])] = val[half:]
                with scope('sib_wait'):
                    to_sib(q).wait_recv()
                y_out[slot] = (y_sum[...] + sib_in[slot, 0:half].astype(f32)).astype(bf16)
                part[lax.rem(q, part.shape[0])] += sib_in[slot, half:].astype(f32)
                to_y(q).start()
            for cp in block_saves(q, b):
                cp.start()

            @pl.when(q + 1 < last)
            def _():
                for cp in block_loads(q + 1, b):
                    cp.start()

        @pl.when(q == 0)
        def _():
            flush(early - 1, chunk)

        @pl.when(q >= 2)
        def _():
            z_stage(q - 2)

        @pl.when(q == n_z + 3)
        def _():
            x_stage(0)

        @pl.when(q == max(last - 4, n_z + 4))
        def _():
            final(0)
        return 0

    lax.fori_loop(0, last, dz_group, 0)
    x_stage(1)
    z_stage(last - 2)
    for b in (0, 1):
        for cp in block_saves(last - 1, b):
            cp.wait()

    for b in range(4):
        load_g(early * chunk, chunk, b, b).start()

    def late_chunk(c, _):
        def quad(i, _):
            for b in range(4):
                k = 4 * i + b
                with scope('b2_wait'):
                    load_g(0, chunk, 0, b).wait()
                with scope('b2_tile'):
                    grad_tile(c * chunk, chunk, k, b, False)
                wrap = k + 4 >= n_tok
                c2, k2 = jnp.where(wrap, c + 1, c), jnp.where(wrap, k + 4 - n_tok, k + 4)

                @pl.when(c2 < sz.full)
                def _():
                    load_g(c2 * chunk, chunk, k2, b).start()

                @pl.when(c2 == sz.full)
                def _():
                    load_g(row_rem, sz.rem, k2, b).start()

            @pl.when(jnp.logical_and(i == 0, c > early))
            def _():
                flush(c - 1, chunk)
            return 0
        lax.fori_loop(0, n_tok // 4, quad, 0)
        ship(c, chunk)

        @pl.when(c == early)
        def _():
            z_stage(last - 1)

        @pl.when(c == early + 1)
        def _():
            final(1)
            forwards(0)
        return 0

    lax.fori_loop(early, sz.full, late_chunk, 0)

    def tell_gain(k):
        tp, f = at.other(k)
        return rcopy(gg, gg_in.at[at.index], gain_s.at[k], gain_r.at[k], dev(tp, f))

    def heard_gain(k):
        i = lax.rem(at.index + at.n_all - k, at.n_all)
        return rcopy(gg, gg_in.at[i], gain_s.at[k], gain_r.at[k], sibling)

    hits = jnp.sum(jnp.sum(hit[...], axis=0, keepdims=True), axis=1, keepdims=True)
    gg[0:1, d:] = jnp.broadcast_to(hits, (1, gg.shape[1] - d))
    at.every(lambda k: tell_gain(k).start())
    gg_in[at.index] = gg[...]

    def late_rem(i, _):
        for b in range(4):
            with scope('b2_wait'):
                load_g(row_rem, sz.rem, 0, b).wait()
            with scope('b2_rem'):
                grad_tile(row_rem, sz.rem, 4 * i + b, b, False)

            @pl.when(4 * i + b + 4 < n_tok)
            def _():
                load_g(row_rem, sz.rem, 4 * i + b + 4, b).start()

        @pl.when(i == 0)
        def _():
            flush(sz.full - 1, chunk)
        return 0

    lax.fori_loop(0, n_tok // 4, late_rem, 0)
    ship(sz.full, sz.rem)
    flush(sz.full, sz.rem)
    forwards(1)

    with scope('t_gain'):
        at.every(lambda k: heard_gain(k).wait_recv())
    total = jnp.sum(gg_in[...], axis=0)
    gg_out[0:1, 0:d] = total[0:1, 0:d]
    gg_out[0:1, d:] = (jnp.sum(st[...] * scale[...], axis=1, keepdims=True) - total[0:1, d:]) * (1.0 / LOG2E)
    with scope('t_small'):
        at.every(lambda k: ask(k).wait_send())
        at.every(lambda k: answer(k).wait_send())
        at.every(lambda k: tell_gain(k).wait_send())
        for k in range(1, n):
            for cp in tok_out(k):
                cp.wait_send()
        h_to_x().wait_send()
        block_out().wait_send()
        for jj in range(n_z - 1):
            h_to_z(jj).wait_send()
        for zo in range(n_z):
            h_to_y(zo).wait_send()
        for tp in range(n_tp):
            h_to_core(tp).wait_send()

        def w_sent(c, _):
            for k in range(1, n):
                remote(k, c, c * chunk, chunk).wait_send()
            return 0

        lax.fori_loop(0, sz.full, w_sent, 0)
        for k in range(1, n):
            remote(k, sz.full, row_rem, sz.solid).wait_send()
            when_not_last(lax.rem(me + k, n), lambda: remote(k, sz.full + 1, row_odd, sz.short).wait_send())
        for q in (last - 2, last - 1):
            to_sib(q).wait_send()
            to_y(q).wait_send()
        for q in range(last - n_z, last - 1):
            to_z(q).wait_send()
        to_x(1).wait_send()
    with scope('t_send'):
        def sent(c, _):
            for cp in sends(c, chunk):
                cp.wait_send()
            return 0
        lax.fori_loop(0, sz.full, sent, 0)
        for cp in sends(sz.full, sz.rem):
            cp.wait_send()
    for r in range(ROUNDS):
        with scope(f't_gather{r}'):
            keep(r).wait()
            for cp in gathers(r):
                cp.wait_send()
            for jj in range(n_z - 1):
                onward(r, jj).wait_send()
            for zo in range(n_z):
                rcopy(gh.at[r], home(zo * 2 + 1 - at.y, r), ag_s.at[r, 0], fw_r.at[r, zo], y_peer).wait_recv()
    with scope('t_dw'):
        for k in range(1, n):
            src = lax.rem(me + n - k, n)
            rcopy(dw_hbm.at[pl.ds(0, sz.rows), :], dw_hbm.at[rows_at(src * sz.rows, sz.rows), :], dw_send.at[0, 0], dw_recv.at[k], sibling).wait_recv()


HBM = pl.BlockSpec(memory_space=pl.ANY)
VM = pl.BlockSpec(memory_space=pltpu.VMEM)
DMA = pltpu.SemaphoreType.DMA


def solution(mesh, chunk=CHUNK, tok=TOK, early=EARLY):
    n_fsdp, n_tp = mesh.shape['fsdp'], mesh.shape['tp']
    n_all, n_z = n_fsdp * n_tp, n_tp // 2
    S, V = jax.ShapeDtypeStruct, pltpu.VMEM
    i32 = jnp.int32

    def per_device(hidden, labels, tok_mask, norm_gain, w_rows):
        per_f, d = hidden.shape
        width, vocab_tp = w_rows.shape
        tokens, own = per_f * n_fsdp, per_f // n_tp
        half = own // ROUNDS
        sz = Sizes(vocab_tp, n_fsdp, chunk)
        n_low = sz.full - early + 1

        dw_t, grad_hidden, sums, *_ = pl.pallas_call(
            functools.partial(head_kernel, sz, n_tp, vocab_tp, chunk, tok, early),
            out_shape=(S((n_fsdp * sz.rows, width), bf16), S(hidden.shape, bf16), S((1, d + 128), f32),
                       S((sz.rows, tokens), f32), S((sz.rows, tokens), bf16), S((tokens, d), bf16), S(((sz.full + 1) * chunk, d), bf16)),
            in_specs=[HBM, VM, VM, VM, HBM], out_specs=(HBM, HBM, VM, HBM, HBM, HBM, HBM),
            scratch_shapes=[
                V((tokens, d), bf16), V((sz.rows, d), bf16), *[V((chunk, tok), f32)] * 4, *[V((chunk, tok), bf16)] * 4, *[V((sz.rows, 2 * half), bf16)] * 2,
                V((8, tokens), f32), V((8, tokens), f32), V((1, tokens), f32), V((1, tokens), i32), V((n_fsdp, 1, per_f), i32), V((n_fsdp, 1, per_f), f32),
                V((2, tokens), f32), V((n_all, 2, own), f32), V((1, own), f32), V((1, tokens), f32), V((1, tokens), f32), V((8, min(128, half)), f32), V((own, d), bf16),
                V((chunk, d), f32), V((2, chunk, d), bf16), V((2, 2 * half, d), bf16), V((2, 2 * half, d), bf16), V((half, d), f32),
                V((2, half, d), bf16), V((6, half, d), bf16), V((3, half, d), f32), V((n_z - 1, half, d), bf16), V((ROUNDS, 2, n_z - 1, half, d), bf16), V((2, half, d), f32),
                V((half, d), bf16), V((ROUNDS, half, d), bf16), V((ROUNDS, half, d), bf16), V((1, d + 128), f32), V((n_all, 1, d + 128), f32),
                DMA((sz.full + 2, n_fsdp)), DMA((sz.full + 2, n_fsdp)), DMA((sz.full + 2,)), DMA((2,)), DMA((4,)), DMA((4,)), DMA((2, 2)), DMA((2, 2 * n_low)), DMA((2, 2)),
                DMA((n_all,)), DMA((n_all,)), DMA((n_all,)), DMA((n_all,)), DMA((2, n_fsdp)), DMA((2, n_fsdp)), DMA((2,)), DMA((1,)), DMA((1,)),
                DMA((n_z - 1,)), DMA((n_z - 1,)), DMA((n_z,)), DMA((n_z,)), DMA((n_tp,)), DMA((n_tp,)),
                DMA((1,)), DMA((2,)), DMA((sz.full + 1, 3)), DMA((n_fsdp,)), DMA((2,)), DMA((2,)), DMA((2,)), DMA((2,)), DMA((8,)),
                DMA((n_z - 1,)), DMA((ROUNDS, 2, n_z - 1)), DMA((1,)), DMA((ROUNDS,)),
                DMA((ROUNDS, n_z)), DMA((ROUNDS, n_z)), DMA((ROUNDS, n_z)), DMA((ROUNDS, n_z)), DMA((ROUNDS,)), DMA((n_all,)), DMA((n_all,))],
            compiler_params=pltpu.CompilerParams(vmem_limit_bytes=VMEM_LIMIT, collective_id=0, has_side_effects=True), name='head',
        )(hidden, labels[None, :], tok_mask[None, :], norm_gain[None, :], w_rows.T)
        return sums[0, d], grad_hidden, dw_t[:vocab_tp].T, sums[0, :d]

    return jax.shard_map(per_device, mesh=mesh, in_specs=(P('fsdp', None), P('fsdp'), P('fsdp'), P(), P('fsdp', 'tp')), out_specs=(P(), P('fsdp', None), P('fsdp', 'tp'), P()), check_vma=False)
```

```python
import functools

import jax
import jax.numpy as jnp
from jax import lax
from jax.experimental import pallas as pl
from jax.experimental.pallas import tpu as pltpu
from jax.sharding import PartitionSpec as P

NORM_EPS = 1e-6
LOG2E = 1.4426950408889634
NEG = -1e30
CHUNK = 512
TOK = 1024
EARLY = 4
AHEAD = 5
ROUNDS = 2
VMEM_LIMIT = 67_043_328
MESH = pl.DeviceIdType.MESH
scope = jax.named_scope
f32, bf16 = jnp.float32, jnp.bfloat16


def dot_nt(a, b):
    return lax.dot_general(a, b, (((1,), (1,)), ((), ())), preferred_element_type=f32)


def dot_tn(a, b):
    return lax.dot_general(a, b, (((0,), (0,)), ((), ())), preferred_element_type=f32)


def dot_nn(a, b):
    return lax.dot_general(a, b, (((1,), (0,)), ((), ())), preferred_element_type=f32)


def cols(k, size):
    return pl.ds(pl.multiple_of(k * size, size), size)


def rows_at(row0, rows):
    return pl.ds(pl.multiple_of(row0, 16), rows)


class Sizes:
    def __init__(self, vocab_tp, n_fsdp, chunk):
        self.n = n_fsdp
        self.rows = -(-vocab_tp // (n_fsdp * 16)) * 16
        self.short = n_fsdp * self.rows - vocab_tp
        self.full = self.rows // chunk
        self.rem = self.rows - self.full * chunk
        self.solid = self.rem - self.short
        assert self.rem > self.short and self.rem % 16 == 0 and self.short % 16 == 0


class Place:
    def __init__(self, n_fsdp, n_tp):
        self.n_fsdp, self.n_tp, self.n_all = n_fsdp, n_tp, n_fsdp * n_tp
        self.f, self.tp = lax.axis_index('fsdp'), lax.axis_index('tp')
        self.x, self.c = self.f // 2, lax.rem(self.f, 2)
        self.n_z = n_tp // 2
        self.z, self.y = self.tp // 2, lax.rem(self.tp, 2)
        self.index = self.tp * n_fsdp + self.f

    def other(self, k):
        i = lax.rem(self.index + k, self.n_all)
        return i // self.n_fsdp, lax.rem(i, self.n_fsdp)

    def every(self, fn):
        def go(k, _):
            fn(k)
            return 0
        lax.fori_loop(1, self.n_all, go, 0)


def dev(tp, f):
    return {'tp': tp, 'fsdp': f}


def rcopy(src, dst, ssem, rsem, to):
    return pltpu.make_async_remote_copy(src_ref=src, dst_ref=dst, send_sem=ssem, recv_sem=rsem, device_id=to, device_id_type=MESH)


def enter(at):
    barrier = pltpu.get_barrier_semaphore()

    def tell(k):
        tp, f = at.other(k)
        pl.semaphore_signal(barrier, inc=1, device_id=dev(tp, f), device_id_type=MESH)

    at.every(tell)
    pl.semaphore_wait(barrier, at.n_all - 1)


def head_kernel(sz, n_tp, vocab_tp, chunk, tok, early,
                h_hbm, lab_ref, mask_ref, gain, w_hbm,
                dw_hbm, gh_hbm, gg_out, l_hbm, g_hbm, h_all, ds_hbm,
                z, w, l0, l1, l2, l3, g0, g1, g2, g3, q0, q1, m, s, scale, lab, lab_in, mask_in, st_loc, got, res, st, top_row, hit, hid,
                acc, stage, sib_out, sib_in, y_sum, y_out, y_in, part, z_out, z_in, z_own, x_out, x_in, gh, gg, gg_in,
                w_s, w_r, loc, hsem, lsem, gsem, qsem, bsem, vsem, ssend, srecv, rsend, rrecv, tok_s, tok_r, blk, hx_s, hx_r, hz_s, hz_r, hy_s, hy_r, hc_s, hc_r,
                hid_sem, dw_copy, dw_send, dw_recv, own_sem, sib_s, sib_r, y_s, y_r, zz_s, zz_r, x_s, x_r, ag_s, ag_r, fw_s, fw_r, gh_sem, gain_s, gain_r):
    at = Place(sz.n, n_tp)
    me, n, n_z, width = at.f, sz.n, at.n_z, w_hbm.shape[1]
    per_f, d = h_hbm.shape
    tokens, own = per_f * n, per_f // n_tp
    lbufs, gbufs, qbufs, hbufs = (l0, l1, l2, l3), (g0, g1, g2, g3), (q0, q1), (sib_out.at[0], sib_out.at[1])
    far, sib = 1 - at.x, at.x * 2 + 1 - at.c
    through = far * 2 + at.c
    sibling, y_peer, x_peer = dev(at.tp, sib), dev(at.z * 2 + 1 - at.y, me), dev(at.tp, through)
    row_rem = sz.full * chunk
    row_odd = row_rem + sz.solid

    with scope('enter'):
        enter(at)

    def slab(f, tp):
        return pl.ds(pl.multiple_of((f * n_tp + tp) * own, own), own)

    def block(f):
        return pl.ds(pl.multiple_of(f * per_f, per_f), per_f)

    def h_to_x():
        return rcopy(h_hbm.at[pl.ds(pl.multiple_of(at.tp * own, own), own), :], h_all.at[slab(me, at.tp), :], hx_s.at[0], hx_r.at[0], x_peer)

    def h_from_x():
        return rcopy(h_all.at[slab(through, at.tp), :], h_all.at[slab(through, at.tp), :], hx_s.at[0], hx_r.at[0], x_peer)

    def block_out():
        return rcopy(h_hbm, h_all.at[block(me), :], blk.at[0], blk.at[1], sibling)

    def block_in():
        return rcopy(h_hbm, h_all.at[block(sib), :], blk.at[0], blk.at[1], sibling)

    def moved(tp, ssem, rsem, to):
        here = h_all.at[slab(through, tp), :]
        return rcopy(here, here, ssem, rsem, to)

    def z_from(jj):
        return lax.rem(at.z + n_z - jj - 1, n_z)

    def h_to_z(jj):
        return moved(at.tp, hz_s.at[jj], hz_r.at[jj], dev(lax.rem(at.z + jj + 1, n_z) * 2 + at.y, me))

    def h_from_z(jj):
        return moved(z_from(jj) * 2 + at.y, hz_s.at[jj], hz_r.at[jj], sibling)

    def h_to_y(zo):
        return moved(zo * 2 + at.y, hy_s.at[zo], hy_r.at[zo], y_peer)

    def h_from_y(zo):
        return moved(zo * 2 + 1 - at.y, hy_s.at[zo], hy_r.at[zo], y_peer)

    def h_to_core(tp):
        return moved(tp, hc_s.at[tp], hc_r.at[tp], sibling)

    def h_from_core(tp):
        here = h_all.at[slab(far * 2 + 1 - at.c, tp), :]
        return rcopy(here, here, hc_s.at[tp], hc_r.at[tp], sibling)

    def tok_out(k):
        to = dev(at.tp, lax.rem(me + k, n))
        return [rcopy(lab_ref, lab_in.at[me], tok_s.at[0, k], tok_r.at[0, k], to), rcopy(mask_ref, mask_in.at[me], tok_s.at[1, k], tok_r.at[1, k], to)]

    def tok_in(k):
        src = lax.rem(me + n - k, n)
        return [rcopy(lab_ref, lab_in.at[src], tok_s.at[0, k], tok_r.at[0, k], sibling), rcopy(mask_ref, mask_in.at[src], tok_s.at[1, k], tok_r.at[1, k], sibling)]

    h_to_x().start()
    block_out().start()
    for k in range(1, n):
        for cp in tok_out(k):
            cp.start()
    lab_in[me] = lab_ref[...]
    mask_in[me] = mask_ref[...]

    def remote(k, c, row0, rows):
        dest = lax.rem(me + k, n)
        return rcopy(w_hbm.at[rows_at(dest * sz.rows + row0, rows), :], w.at[rows_at(row0, rows), cols(me, width)], w_s.at[c, k], w_r.at[c, k], dev(at.tp, dest))

    def arrival(k, c, row0, rows):
        src = lax.rem(me + n - k, n)
        return rcopy(w_hbm.at[pl.ds(0, rows), :], w.at[rows_at(row0, rows), cols(src, width)], w_s.at[c, k], w_r.at[c, k], sibling)

    def local(c, row0, rows):
        return pltpu.make_async_copy(w_hbm.at[rows_at(me * sz.rows + row0, rows), :], w.at[rows_at(row0, rows), cols(me, width)], loc.at[c])

    def issue(c):
        local(c, c * chunk, chunk).start()
        for k in range(1, n):
            remote(k, c, c * chunk, chunk).start()

    def when_not_last(dest, fn):
        if sz.short:
            pl.when(dest != n - 1)(fn)

    def issue_rem():
        local(sz.full, row_rem, sz.solid).start()
        when_not_last(me, lambda: local(sz.full + 1, row_odd, sz.short).start())
        for k in range(1, n):
            remote(k, sz.full, row_rem, sz.solid).start()
            when_not_last(lax.rem(me + k, n), lambda: remote(k, sz.full + 1, row_odd, sz.short).start())

    ahead = min(AHEAD, sz.full)
    for c in range(ahead):
        issue(c)
    if sz.short:
        @pl.when(me == n - 1)
        def _():
            w[row_odd:, :] = jnp.zeros((sz.short, d), bf16)

    sub = min(256, own)
    slices, per_own = per_f // sub, own // sub
    lane = min(128, sub)

    def place(t, i):
        near = jnp.where(t == 0, me, sib) * per_f + i * sub
        j = i // per_own
        f = jnp.where(j < n_z, through, far * 2 + 1 - at.c)
        y = jnp.where(t == 2, at.y, 1 - at.y)
        away = (f * n_tp + lax.rem(j, n_z) * 2 + y) * own + lax.rem(i, per_own) * sub
        return pl.multiple_of(jnp.where(t < 2, near, away), sub)

    def norm(t):
        def load(i, b):
            if t == 0:
                return pltpu.make_async_copy(h_hbm.at[cols(i, sub), :], hbufs[b], hsem.at[b])
            return pltpu.make_async_copy(h_all.at[pl.ds(place(t, i), sub), :], hbufs[b], hsem.at[b])

        load(0, 0).start()
        load(1, 1).start()

        def pair(i2, _):
            for b in (0, 1):
                i = 2 * i2 + b
                load(i, b).wait()
                h = hbufs[b][...].astype(f32)
                inv = lax.rsqrt(jnp.mean(h * h, axis=-1, keepdims=True) + NORM_EPS)
                z[pl.ds(place(t, i), sub), :] = (h * inv * gain[...].astype(f32)).astype(bf16)

                @pl.when(i + 2 < slices)
                def _():
                    load(i + 2, b).start()
            return 0

        with scope(f'norm{t}'):
            lax.fori_loop(0, slices // 2, pair, 0)

    norm(0)
    with scope('blk_wait'):
        block_in().wait_recv()
    norm(1)
    with scope('x_wait'):
        h_from_x().wait_recv()
    for jj in range(n_z - 1):
        h_to_z(jj).start()
    h_to_y(at.z).start()
    h_to_core(at.tp).start()
    with scope('tok_wait'):
        for k in range(1, n):
            for cp in tok_in(k):
                cp.wait_recv()
    count = jnp.sum(mask_in[...], axis=(0, 2), keepdims=True)[0]
    for f in range(n):
        here = pl.ds(f * per_f, per_f)
        scale[0:1, here] = mask_in[f] / count
        rel = lab_in[f] - at.tp * vocab_tp
        lab[0:1, here] = jnp.where(jnp.logical_and(rel >= 0, rel < vocab_tp), rel - me * sz.rows, -1)

    def spread_z():
        with scope('z_wait'):
            for jj in range(n_z - 1):
                h_from_z(jj).wait_recv()
                h_to_y(z_from(jj)).start()
                h_to_core(z_from(jj) * 2 + at.y).start()

    def spread_y():
        with scope('hy_wait'):
            for k in range(n_z):
                zo = lax.rem(at.z + n_z - k, n_z)
                h_from_y(zo).wait_recv()
                h_to_core(zo * 2 + 1 - at.y).start()

    def far_ready(y):
        with scope('core_wait'):
            for zo in range(n_z):
                h_from_core(zo * 2 + y).wait_recv()

    m[...] = jnp.full(m.shape, NEG, f32)
    s[...] = jnp.zeros(s.shape, f32)
    per_buf = tok // sub
    n_buf = slices // per_buf

    def out_copies(row0, rows, t, b):
        return [pltpu.make_async_copy(lbufs[b * n_buf + i // per_buf].at[pl.ds(0, rows), pl.ds(i % per_buf * sub, sub)],
                                      l_hbm.at[rows_at(row0, rows), pl.ds(place(t, i), sub)], lsem.at[b * n_buf + i // per_buf]) for i in range(slices)]

    def out_done(rows, b):
        for i in range(n_buf):
            pltpu.make_async_copy(lbufs[b * n_buf + i].at[pl.ds(0, rows), :], l_hbm.at[pl.ds(0, rows), pl.ds(0, tok)], lsem.at[b * n_buf + i]).wait()

    def statistics(read, rows, t0):
        group = min(4, rows // 8)
        for c1 in range(0, sub, lane):
            sl = pl.ds(pl.multiple_of(t0 + c1, lane), lane)
            big, tot = m[:, sl], s[:, sl]
            for g in range(0, rows // 8, group):
                piece = [read(r, c1) for r in range(g, min(g + group, rows // 8))]
                new = functools.reduce(jnp.maximum, piece, big)
                tot = tot * jnp.exp2(big - new)
                for x in piece:
                    tot += jnp.exp2(x - new)
                big = new
            m[:, sl], s[:, sl] = big, tot

    def slice_at(b, i):
        return lbufs[b * n_buf + i // per_buf], i % per_buf * sub

    def late_statistics(t, b):
        for i in range(slices - lag, slices):
            buf, i0 = slice_at(b, i)
            statistics(lambda r, c1: buf[8 * r:8 * r + 8, i0 + c1:i0 + c1 + lane], chunk, place(t, i))

    def logits_tile(row0, rows, t, b, masked):
        for i in range(slices):
            t0 = place(t, i)
            logits = dot_nt(w[rows_at(row0, rows), :], z[pl.ds(t0, sub), :]) * LOG2E
            if masked:
                ids = lax.broadcasted_iota(jnp.int32, (rows, sub), 0)
                logits = jnp.where(ids < jnp.where(me == n - 1, sz.solid, sz.rem), logits, NEG)
            buf, i0 = slice_at(b, i)
            buf[0:rows, i0:i0 + sub] = logits
            if masked or i < slices - lag:
                statistics(lambda r, c1: logits[8 * r:8 * r + 8, c1:c1 + lane], rows, t0)

    lag = 2
    for i in range(slices - lag, slices):
        buf, i0 = slice_at(1, i)
        buf[:, i0:i0 + sub] = jnp.full((chunk, sub), NEG, f32)

    n_a = min(3, sz.full)
    n_c = min(3, sz.full - n_a)
    k_b, k_c = 2 * n_a, 3 * n_a
    k_d = k_c + 3 * n_c
    k_e = k_d + n_a + n_c

    def item(k):
        u, v = k - k_c, k - k_e
        c = jnp.where(k < k_b, k // 2, jnp.where(k < k_c, k - k_b, jnp.where(k < k_d, n_a + u // 3, jnp.where(k < k_e, k - k_d, n_a + n_c + v // 4))))
        t = jnp.where(k < k_b, lax.rem(k, 2), jnp.where(k < k_c, 2, jnp.where(k < k_d, lax.rem(u, 3), jnp.where(k < k_e, 3, lax.rem(v, 4)))))
        return c, t

    def work(i2, _):
        for b in (0, 1):
            k = 2 * i2 + b
            c, t = item(k)

            @pl.when(t == 0)
            def _():
                with scope('w_wait'):
                    local(c, c * chunk, chunk).wait()
                    for j in range(1, n):
                        arrival(j, c, c * chunk, chunk).wait_recv()

                @pl.when(c + ahead < sz.full)
                def _():
                    issue(c + ahead)

                @pl.when(c + ahead == sz.full)
                def _():
                    issue_rem()

            @pl.when(k == k_b)
            def _():
                spread_z()
                far_ready(at.y)
                norm(2)

            @pl.when(k == max(k_d - 3, k_c))
            def _():
                spread_y()

            @pl.when(k == k_d)
            def _():
                far_ready(1 - at.y)
                norm(3)

            with scope('l_wait'):
                @pl.when(k >= 2)
                def _():
                    out_done(chunk, b)
            with scope('l_tile'):
                late_statistics(item(jnp.maximum(k - 1, 0))[1], 1 - b)
                logits_tile(c * chunk, chunk, t, b, False)
            for cp in out_copies(c * chunk, chunk, t, b):
                cp.start()
        return 0

    lax.fori_loop(0, sz.full * 2, work, 0)
    late_statistics(item(4 * sz.full - 1)[1], 1)
    with scope('w_wait_rem'):
        local(sz.full, row_rem, sz.solid).wait()
        when_not_last(me, lambda: local(sz.full + 1, row_odd, sz.short).wait())
        for k in range(1, n):
            arrival(k, sz.full, row_rem, sz.solid).wait_recv()
            when_not_last(me, lambda: arrival(k, sz.full + 1, row_odd, sz.short).wait_recv())

    def work_rem(i2, _):
        for b in (0, 1):
            @pl.when(i2 == 0)
            def _():
                out_done(chunk, b)

            @pl.when(i2 > 0)
            def _():
                out_done(sz.rem, b)
            logits_tile(row_rem, sz.rem, 2 * i2 + b, b, True)
            for cp in out_copies(row_rem, sz.rem, 2 * i2 + b, b):
                cp.start()
        return 0

    with scope('l_rem'):
        lax.fori_loop(0, 2, work_rem, 0)

    big = jnp.max(m[...], axis=0, keepdims=True)
    st_loc[0:1, :] = big
    st_loc[1:2, :] = jnp.sum(s[...] * jnp.exp2(m[...] - big), axis=0, keepdims=True)
    mine = slab(at.f, at.tp)

    def ask(k):
        tp, f = at.other(k)
        return rcopy(st_loc.at[:, slab(f, tp)], got.at[k], ssend.at[k], srecv.at[k], dev(tp, f))

    def answer(k):
        tp, f = at.other(k)
        return rcopy(res, st.at[:, mine], rsend.at[k], rrecv.at[k], dev(tp, f))

    def answered(k):
        tp, f = at.other(at.n_all - k)
        return rcopy(res, st.at[:, slab(f, tp)], rsend.at[k], rrecv.at[k], dev(tp, f))

    n_tok = tokens // tok

    def load_l(row0, rows, k, b):
        return pltpu.make_async_copy(l_hbm.at[rows_at(row0, rows), cols(k, tok)], lbufs[b].at[pl.ds(0, rows), :], lsem.at[b])

    def load_g(row0, rows, k, b):
        return pltpu.make_async_copy(g_hbm.at[rows_at(row0, rows), cols(k, tok)], gbufs[b].at[pl.ds(0, rows), :], gsem.at[b])

    def save_g(row0, rows, k, b):
        return pltpu.make_async_copy(gbufs[b].at[pl.ds(0, rows), :], g_hbm.at[rows_at(row0, rows), cols(k, tok)], gsem.at[b])

    at.every(lambda k: ask(k).start())
    got[0] = st_loc[:, mine]
    for b in (0, 1):
        out_done(sz.rem, b)
    for b in range(4):
        load_l(0, chunk, b, b).start()
    h_load = pltpu.make_async_copy(h_hbm.at[pl.ds(pl.multiple_of(at.tp * own, own), own), :], hid, hid_sem.at[0])
    h_load.start()
    acc[...] = jnp.zeros(acc.shape, f32)
    hit[...] = jnp.zeros(hit.shape, f32)
    with scope('ask_wait'):
        at.every(lambda k: ask(k).wait_recv())
    tops = got[:, 0:1, :]
    top = jnp.max(tops, axis=0)
    res[...] = top + jnp.log2(jnp.sum(got[:, 1:2, :] * jnp.exp2(tops - top[None]), axis=0))
    at.every(lambda k: answer(k).start())
    st[:, mine] = res[...]
    with scope('answer_wait'):
        at.every(lambda k: answered(k).wait_recv())
    top_row[...] = st[...] - jnp.log2(scale[...])

    def gradient(x, sl, row0):
        rows = x.shape[0]
        sc = scale[0:1, sl]
        x3 = x.reshape(rows // 8, 8, x.shape[1])
        p = jnp.exp2(x3 - top_row[0:1, sl][None])
        is_label = lax.broadcasted_iota(jnp.int32, p.shape, 0) * 8 == (lab[0:1, sl] - row0 - lax.broadcasted_iota(jnp.int32, (8, x.shape[1]), 0))[None]
        hit[...] += jnp.sum(jnp.where(is_label, x3, 0.0), axis=0) * sc
        return jnp.where(is_label, p - sc[None], p).reshape(x.shape).astype(bf16)

    step = min(256, tok)

    def grad_tile(row0, rows, k, b, fresh):
        total = None
        for c0 in range(0, tok, step):
            if fresh:
                for c1 in range(c0, c0 + step, lane):
                    gbufs[b][0:rows, c1:c1 + lane] = gradient(lbufs[b][0:rows, c1:c1 + lane], pl.ds(pl.multiple_of(k * tok + c1, lane), lane), row0)
            p = dot_nn(gbufs[b][0:rows, c0:c0 + step], z[pl.ds(pl.multiple_of(k * tok + c0, step), step), :])
            total = p if total is None else total + p
        acc[0:rows, :] += total

    def aside(c, rows):
        slot = lax.rem(c, 2)
        return pltpu.make_async_copy(stage.at[slot, pl.ds(0, rows), :], ds_hbm.at[rows_at(c * chunk, rows), :], dw_copy.at[slot])

    def keep_own(c, row0, rows):
        slot = lax.rem(c, 2)
        return pltpu.make_async_copy(stage.at[slot, pl.ds(row0, rows), cols(me, width)], dw_hbm.at[rows_at(me * sz.rows + c * chunk + row0, rows), :], own_sem.at[slot])

    def sends(c, row0, rows, sem):
        out = []
        for i, f in enumerate((far * 2, far * 2 + 1, sib)):
            out.append(rcopy(ds_hbm.at[rows_at(c * chunk + row0, rows), cols(f, width)], dw_hbm.at[rows_at(me * sz.rows + c * chunk + row0, rows), :],
                             dw_send.at[sem, i], dw_recv.at[lax.rem(f + n - me, n)], dev(at.tp, f)))
        return out

    def ship(c, rows):
        with scope('ship'):
            stage[lax.rem(c, 2), 0:rows, :] = acc[0:rows, :].astype(bf16)
            acc[...] = jnp.zeros(acc.shape, f32)
        aside(c, rows).start()
        if rows == chunk:
            keep_own(c, 0, rows).start()

    def flush(c, rows):
        aside(c, rows).wait()
        keep_own(c, 0, rows).wait()
        for cp in sends(c, 0, rows, c):
            cp.start()

    def flush_rem():
        keep_own(sz.full, 0, sz.solid).start()
        keep_own(sz.full, 0, sz.solid).wait()

        def odd():
            cp = keep_own(sz.full, sz.solid, sz.short)
            cp.start()
            cp.wait()
        when_not_last(me, odd)
        aside(sz.full, sz.rem).wait()
        for cp in sends(sz.full, 0, sz.solid, sz.full):
            cp.start()
        when_not_last(me, lambda: [cp.start() for cp in sends(sz.full, sz.solid, sz.short, sz.full + 1)] and None)

    def early_chunk(c, _):
        def quad(i, _):
            for b in range(4):
                k = 4 * i + b
                with scope('b1_wait'):
                    load_l(0, chunk, 0, b).wait()

                    @pl.when(jnp.logical_not(jnp.logical_and(c == 0, i == 0)))
                    def _():
                        save_g(0, chunk, 0, b).wait()
                with scope('b1_tile'):
                    grad_tile(c * chunk, chunk, k, b, True)
                save_g(c * chunk, chunk, k, b).start()
                wrap = k + 4 >= n_tok
                c2 = jnp.where(wrap, c + 1, c)

                @pl.when(c2 < early)
                def _():
                    load_l(c2 * chunk, chunk, jnp.where(wrap, k + 4 - n_tok, k + 4), b).start()

            @pl.when(jnp.logical_and(i == 0, c > 0))
            def _():
                flush(c - 1, chunk)
            return 0
        lax.fori_loop(0, n_tok // 4, quad, 0)
        ship(c, chunk)
        return 0

    lax.fori_loop(0, early, early_chunk, 0)

    half = own // ROUNDS
    groups = 2 * n_z
    last = ROUNDS * groups
    row_low = early * chunk
    low = [(j, chunk) for j in range(sz.full - early)] + [(sz.full - early, sz.rem)]
    per_l = tok // half

    def group_of(q):
        r, g = q // groups, lax.rem(q, groups)
        xi, jj = g // n_z, lax.rem(g, n_z)
        return r, xi, jj, jnp.where(xi == 0, far, at.x), lax.rem(at.z + jj + 1, n_z)

    def pieces(q, b):
        r, _, _, xb, zb = group_of(q)
        cb = at.c if b == 1 else 1 - at.c
        return [pl.multiple_of((xb * 2 + cb) * per_f + (zb * 2 + yb) * own + r * half, half) for yb in (1 - at.y, at.y)]

    def l_part(b, j, i, rows):
        p = 2 * j + i
        return lbufs[2 * b + p // per_l].at[pl.ds(0, rows), pl.ds(p % per_l * half, half)]

    def block_loads(q, b):
        out = []
        for i, t0 in enumerate(pieces(q, b)):
            out.append(pltpu.make_async_copy(g_hbm.at[pl.ds(0, row_low), pl.ds(t0, half)], qbufs[b].at[pl.ds(0, row_low), pl.ds(i * half, half)], qsem.at[b, i]))
            for j, rows in low:
                out.append(pltpu.make_async_copy(l_hbm.at[pl.ds(row_low + j * chunk, rows), pl.ds(t0, half)], l_part(b, j, i, rows), bsem.at[b, 2 * j + i]))
        return out

    def block_saves(q, b):
        return [pltpu.make_async_copy(qbufs[b].at[pl.ds(row_low, sz.rows - row_low), pl.ds(i * half, half)],
                                      g_hbm.at[pl.ds(row_low, sz.rows - row_low), pl.ds(t0, half)], vsem.at[b, i]) for i, t0 in enumerate(pieces(q, b))]

    def block_dot(q, b):
        for i, t0 in enumerate(pieces(q, b)):
            for j, rows in low:
                row0 = row_low + j * chunk
                qbufs[b][row0:row0 + rows, i * half:(i + 1) * half] = gradient(l_part(b, j, i, rows)[...], pl.ds(t0, half), row0)
        return dot_tn(qbufs[b][...], w[...])

    def to_sib(q):
        slot = lax.rem(q, 2)
        return rcopy(sib_out.at[slot], sib_in.at[slot], sib_s.at[slot], sib_r.at[slot], sibling)

    def to_y(q):
        slot, land = lax.rem(q, 2), lax.rem(q, y_in.shape[0])
        return rcopy(y_out.at[slot], y_in.at[land], y_s.at[slot], y_r.at[land], y_peer)

    def to_z(q):
        r, xi, jj, _, zb = group_of(q)
        return rcopy(z_out.at[jj], z_in.at[r, xi, jj], zz_s.at[jj], zz_r.at[r, xi, jj], dev(zb * 2 + at.y, me))

    def to_x(r):
        return rcopy(x_out, x_in.at[r], x_s.at[0], x_r.at[r], x_peer)

    def z_stage(q):
        _, xi, jj, _, _ = group_of(q)
        with scope('y_wait'):
            to_y(q).wait_recv()
        val = part[lax.rem(q, part.shape[0])] + y_in[lax.rem(q, y_in.shape[0])].astype(f32)

        @pl.when(jj == n_z - 1)
        def _():
            z_own[xi] = val

        @pl.when(jj < n_z - 1)
        def _():
            @pl.when(q >= n_z)
            def _():
                to_z(q - n_z).wait_send()
            z_out[jj] = val.astype(bf16)
            to_z(q).start()

    def z_sum(r, xi):
        val = z_own[xi]
        for jj in range(n_z - 1):
            rcopy(z_out.at[0], z_in.at[r, xi, jj], zz_s.at[jj], zz_r.at[r, xi, jj], sibling).wait_recv()
            val = val + z_in[r, xi, jj].astype(f32)
        return val

    def x_stage(r):
        @pl.when(r > 0)
        def _():
            to_x(0).wait_send()
        with scope('x_stage'):
            x_out[...] = z_sum(r, 0).astype(bf16)
        to_x(r).start()

    def home(tp, r):
        return gh_hbm.at[pl.ds(pl.multiple_of(tp * own + r * half, half), half), :]

    def gathers(r):
        out = [rcopy(gh.at[r], home(at.tp, r), ag_s.at[r, n_z - 1], fw_r.at[r, at.z], y_peer)]
        for jj in range(n_z - 1):
            to = lax.rem(at.z + jj + 1, n_z)
            out.append(rcopy(gh.at[r], home(at.tp, r), ag_s.at[r, jj], ag_r.at[r, jj], dev(to * 2 + at.y, me)))
        return out

    def keep(r):
        return pltpu.make_async_copy(gh.at[r], home(at.tp, r), gh_sem.at[r])

    def arrived(r, jj):
        return rcopy(gh.at[r], home(z_from(jj) * 2 + at.y, r), ag_s.at[r, jj], ag_r.at[r, jj], sibling)

    def onward(r, jj):
        here = home(z_from(jj) * 2 + at.y, r)
        return rcopy(here, here, fw_s.at[r, jj], fw_r.at[r, z_from(jj)], y_peer)

    def tell_gain(k):
        tp, f = at.other(k)
        return rcopy(gg, gg_in.at[at.index], gain_s.at[k], gain_r.at[k], dev(tp, f))

    def heard_gain(k):
        i = lax.rem(at.index + at.n_all - k, at.n_all)
        return rcopy(gg, gg_in.at[i], gain_s.at[k], gain_r.at[k], sibling)

    def final(r):
        with scope('final_wait'):
            to_x(r).wait_recv()
            dz = z_sum(r, 1) + x_in[r].astype(f32)
        h = hid[pl.ds(pl.multiple_of(r * half, half), half), :].astype(f32)
        inv = lax.rsqrt(jnp.mean(h * h, axis=-1, keepdims=True) + NORM_EPS)
        normed = h * inv
        a = dz * gain[...].astype(f32)
        gh[r] = (inv * (a - normed * jnp.mean(a * normed, axis=-1, keepdims=True))).astype(bf16)
        gg[0:1, 0:d] += jnp.sum(dz * normed, axis=0, keepdims=True)
        if r == 1:
            hits = jnp.sum(jnp.sum(hit[...], axis=0, keepdims=True), axis=1, keepdims=True)
            gg[0:1, d:] = jnp.broadcast_to(hits, (1, gg.shape[1] - d))
            at.every(lambda k: tell_gain(k).start())
            gg_in[at.index] = gg[...]
        keep(r).start()
        for cp in gathers(r):
            cp.start()

    def forwards(r):
        for jj in range(n_z - 1):
            with scope('fw_wait'):
                arrived(r, jj).wait_recv()
            onward(r, jj).start()

    for b in range(4):
        save_g(0, chunk, 0, b).wait()
    h_load.wait()
    gg[...] = jnp.zeros(gg.shape, f32)
    for b in (0, 1):
        for cp in block_loads(0, b):
            cp.start()

    def dz_group(q, _):
        for b in (0, 1):
            with scope('a_wait'):
                for cp in block_loads(q, b):
                    cp.wait()

                @pl.when(q > 0)
                def _():
                    for cp in block_saves(q - 1, b):
                        cp.wait()
            slot = lax.rem(q, 2)
            if b == 0:
                @pl.when(q >= 2)
                def _():
                    to_sib(q - 2).wait_send()
                with scope('a_dot0'):
                    sib_out[slot] = block_dot(q, b).astype(bf16)
                to_sib(q).start()
            else:
                @pl.when(q >= 2)
                def _():
                    to_y(q - 2).wait_send()
                with scope('a_dot1'):
                    val = block_dot(q, b)
                    y_sum[...] = val[0:half]
                    part[lax.rem(q, part.shape[0])] = val[half:]
                with scope('sib_wait'):
                    to_sib(q).wait_recv()
                y_out[slot] = (y_sum[...] + sib_in[slot, 0:half].astype(f32)).astype(bf16)
                part[lax.rem(q, part.shape[0])] += sib_in[slot, half:].astype(f32)
                to_y(q).start()
            for cp in block_saves(q, b):
                cp.start()

            @pl.when(q + 1 < last)
            def _():
                for cp in block_loads(q + 1, b):
                    cp.start()

        @pl.when(q == 0)
        def _():
            flush(early - 1, chunk)

        @pl.when(q >= 2)
        def _():
            z_stage(q - 2)

        @pl.when(q == n_z + 3)
        def _():
            x_stage(0)

        @pl.when(q == max(last - 6, n_z + 4))
        def _():
            final(0)
        return 0

    lax.fori_loop(0, last, dz_group, 0)
    z_stage(last - 2)
    x_stage(1)
    forwards(0)
    for b in (0, 1):
        for cp in block_saves(last - 1, b):
            cp.wait()

    for b in range(4):
        load_g(early * chunk, chunk, b, b).start()

    def late_chunk(c, _):
        def quad(i, _):
            for b in range(4):
                k = 4 * i + b
                with scope('b2_wait'):
                    load_g(0, chunk, 0, b).wait()
                with scope('b2_tile'):
                    grad_tile(c * chunk, chunk, k, b, False)
                wrap = k + 4 >= n_tok
                c2, k2 = jnp.where(wrap, c + 1, c), jnp.where(wrap, k + 4 - n_tok, k + 4)

                @pl.when(c2 < sz.full)
                def _():
                    load_g(c2 * chunk, chunk, k2, b).start()

                @pl.when(c2 == sz.full)
                def _():
                    load_g(row_rem, sz.rem, k2, b).start()

            @pl.when(jnp.logical_and(i == 0, c > early))
            def _():
                flush(c - 1, chunk)

            @pl.when(jnp.logical_and(i == 0, c == sz.full - 1))
            def _():
                forwards(1)
            return 0
        lax.fori_loop(0, n_tok // 4, quad, 0)
        ship(c, chunk)

        @pl.when(c == early)
        def _():
            z_stage(last - 1)

        @pl.when(c == early + 1)
        def _():
            final(1)
        return 0

    lax.fori_loop(early, sz.full, late_chunk, 0)

    def late_rem(i, _):
        for b in range(4):
            with scope('b2_wait'):
                load_g(row_rem, sz.rem, 0, b).wait()
            with scope('b2_rem'):
                grad_tile(row_rem, sz.rem, 4 * i + b, b, False)

            @pl.when(4 * i + b + 4 < n_tok)
            def _():
                load_g(row_rem, sz.rem, 4 * i + b + 4, b).start()

        @pl.when(i == 0)
        def _():
            flush(sz.full - 1, chunk)
        return 0

    lax.fori_loop(0, n_tok // 4, late_rem, 0)
    ship(sz.full, sz.rem)
    flush_rem()

    with scope('t_gain'):
        at.every(lambda k: heard_gain(k).wait_recv())
    total = jnp.sum(gg_in[...], axis=0)
    gg_out[0:1, 0:d] = total[0:1, 0:d]
    gg_out[0:1, d:] = (jnp.sum(st[...] * scale[...], axis=1, keepdims=True) - total[0:1, d:]) * (1.0 / LOG2E)
    with scope('t_small'):
        at.every(lambda k: ask(k).wait_send())
        at.every(lambda k: answer(k).wait_send())
        at.every(lambda k: tell_gain(k).wait_send())
        for k in range(1, n):
            for cp in tok_out(k):
                cp.wait_send()
        h_to_x().wait_send()
        block_out().wait_send()
        for jj in range(n_z - 1):
            h_to_z(jj).wait_send()
        for zo in range(n_z):
            h_to_y(zo).wait_send()
        for tp in range(n_tp):
            h_to_core(tp).wait_send()

        def w_sent(c, _):
            for k in range(1, n):
                remote(k, c, c * chunk, chunk).wait_send()
            return 0

        lax.fori_loop(0, sz.full, w_sent, 0)
        for k in range(1, n):
            remote(k, sz.full, row_rem, sz.solid).wait_send()
            when_not_last(lax.rem(me + k, n), lambda: remote(k, sz.full + 1, row_odd, sz.short).wait_send())
        for q in (last - 2, last - 1):
            to_sib(q).wait_send()
            to_y(q).wait_send()
        for q in range(last - n_z, last - 1):
            to_z(q).wait_send()
        to_x(1).wait_send()
    with scope('t_send'):
        def sent(c, _):
            for cp in sends(c, 0, chunk, c):
                cp.wait_send()
            return 0
        lax.fori_loop(0, sz.full, sent, 0)
        for cp in sends(sz.full, 0, sz.solid, sz.full):
            cp.wait_send()
        when_not_last(me, lambda: [cp.wait_send() for cp in sends(sz.full, sz.solid, sz.short, sz.full + 1)] and None)
    for r in range(ROUNDS):
        with scope(f't_gather{r}'):
            keep(r).wait()
            for cp in gathers(r):
                cp.wait_send()
            for jj in range(n_z - 1):
                onward(r, jj).wait_send()
            for zo in range(n_z):
                rcopy(gh.at[r], home(zo * 2 + 1 - at.y, r), ag_s.at[r, 0], fw_r.at[r, zo], y_peer).wait_recv()
    with scope('t_dw'):
        for k in range(1, n):
            src = lax.rem(me + n - k, n)

            def all_in(rows):
                rcopy(dw_hbm.at[pl.ds(0, rows), :], dw_hbm.at[rows_at(src * sz.rows, rows), :], dw_send.at[0, 0], dw_recv.at[k], sibling).wait_recv()

            @pl.when(src != n - 1)
            def _():
                all_in(sz.rows)

            @pl.when(src == n - 1)
            def _():
                all_in(sz.rows - sz.short)


HBM = pl.BlockSpec(memory_space=pl.ANY)
VM = pl.BlockSpec(memory_space=pltpu.VMEM)
DMA = pltpu.SemaphoreType.DMA


def solution(mesh, chunk=CHUNK, tok=TOK, early=EARLY):
    n_fsdp, n_tp = mesh.shape['fsdp'], mesh.shape['tp']
    n_all, n_z = n_fsdp * n_tp, n_tp // 2
    S, V = jax.ShapeDtypeStruct, pltpu.VMEM
    i32 = jnp.int32

    def per_device(hidden, labels, tok_mask, norm_gain, w_rows):
        per_f, d = hidden.shape
        width, vocab_tp = w_rows.shape
        tokens, own = per_f * n_fsdp, per_f // n_tp
        half = own // ROUNDS
        sz = Sizes(vocab_tp, n_fsdp, chunk)
        n_low = sz.full - early + 1

        dw_t, grad_hidden, sums, *_ = pl.pallas_call(
            functools.partial(head_kernel, sz, n_tp, vocab_tp, chunk, tok, early),
            out_shape=(S((vocab_tp, width), bf16), S(hidden.shape, bf16), S((1, d + 128), f32),
                       S((sz.rows, tokens), f32), S((sz.rows, tokens), bf16), S((tokens, d), bf16), S(((sz.full + 1) * chunk, d), bf16)),
            in_specs=[HBM, VM, VM, VM, HBM], out_specs=(HBM, HBM, VM, HBM, HBM, HBM, HBM),
            scratch_shapes=[
                V((tokens, d), bf16), V((sz.rows, d), bf16), *[V((chunk, tok), f32)] * 4, *[V((chunk, tok), bf16)] * 4, *[V((sz.rows, 2 * half), bf16)] * 2,
                V((8, tokens), f32), V((8, tokens), f32), V((1, tokens), f32), V((1, tokens), i32), V((n_fsdp, 1, per_f), i32), V((n_fsdp, 1, per_f), f32),
                V((2, tokens), f32), V((n_all, 2, own), f32), V((1, own), f32), V((1, tokens), f32), V((1, tokens), f32), V((8, min(128, half)), f32), V((own, d), bf16),
                V((chunk, d), f32), V((2, chunk, d), bf16), V((2, 2 * half, d), bf16), V((2, 2 * half, d), bf16), V((half, d), f32),
                V((2, half, d), bf16), V((6, half, d), bf16), V((3, half, d), f32), V((n_z - 1, half, d), bf16), V((ROUNDS, 2, n_z - 1, half, d), bf16), V((2, half, d), f32),
                V((half, d), bf16), V((ROUNDS, half, d), bf16), V((ROUNDS, half, d), bf16), V((1, d + 128), f32), V((n_all, 1, d + 128), f32),
                DMA((sz.full + 2, n_fsdp)), DMA((sz.full + 2, n_fsdp)), DMA((sz.full + 2,)), DMA((2,)), DMA((4,)), DMA((4,)), DMA((2, 2)), DMA((2, 2 * n_low)), DMA((2, 2)),
                DMA((n_all,)), DMA((n_all,)), DMA((n_all,)), DMA((n_all,)), DMA((2, n_fsdp)), DMA((2, n_fsdp)), DMA((2,)), DMA((1,)), DMA((1,)),
                DMA((n_z - 1,)), DMA((n_z - 1,)), DMA((n_z,)), DMA((n_z,)), DMA((n_tp,)), DMA((n_tp,)),
                DMA((1,)), DMA((2,)), DMA((sz.full + 2, 3)), DMA((n_fsdp,)), DMA((2,)), DMA((2,)), DMA((2,)), DMA((2,)), DMA((8,)),
                DMA((n_z - 1,)), DMA((ROUNDS, 2, n_z - 1)), DMA((1,)), DMA((ROUNDS,)),
                DMA((ROUNDS, n_z)), DMA((ROUNDS, n_z)), DMA((ROUNDS, n_z)), DMA((ROUNDS, n_z)), DMA((ROUNDS,)), DMA((n_all,)), DMA((n_all,))],
            compiler_params=pltpu.CompilerParams(vmem_limit_bytes=VMEM_LIMIT, collective_id=0, has_side_effects=True), name='head',
        )(hidden, labels[None, :], tok_mask[None, :], norm_gain[None, :], w_rows.T)
        return sums[0, d], grad_hidden, dw_t.T, sums[0, :d]

    return jax.shard_map(per_device, mesh=mesh, in_specs=(P('fsdp', None), P('fsdp'), P('fsdp'), P(), P('fsdp', 'tp')), out_specs=(P(), P('fsdp', None), P('fsdp', 'tp'), P()), check_vma=False)
```

```python
import functools

import jax
import jax.numpy as jnp
from jax import lax
from jax.experimental import pallas as pl
from jax.experimental.pallas import tpu as pltpu
from jax.sharding import PartitionSpec as P

NORM_EPS = 1e-6
LOG2E = 1.4426950408889634
NEG = -1e30
CHUNK = 512
TOK = 1024
EARLY = 5
AHEAD = 5
ROUNDS = 2
VMEM_LIMIT = 67_043_328
MESH = pl.DeviceIdType.MESH
scope = jax.named_scope
f32, bf16 = jnp.float32, jnp.bfloat16


def dot_nt(a, b):
    return lax.dot_general(a, b, (((1,), (1,)), ((), ())), preferred_element_type=f32)


def dot_tn(a, b):
    return lax.dot_general(a, b, (((0,), (0,)), ((), ())), preferred_element_type=f32)


def dot_nn(a, b):
    return lax.dot_general(a, b, (((1,), (0,)), ((), ())), preferred_element_type=f32)


def cols(k, size):
    return pl.ds(pl.multiple_of(k * size, size), size)


def rows_at(row0, rows):
    return pl.ds(pl.multiple_of(row0, 16), rows)


class Sizes:
    def __init__(self, vocab_tp, n_fsdp, chunk):
        self.n = n_fsdp
        self.rows = -(-vocab_tp // (n_fsdp * 16)) * 16
        self.short = n_fsdp * self.rows - vocab_tp
        self.full = self.rows // chunk
        self.rem = self.rows - self.full * chunk
        self.solid = self.rem - self.short
        assert self.rem > self.short and self.rem % 16 == 0 and self.short % 16 == 0


class Place:
    def __init__(self, n_fsdp, n_tp):
        self.n_fsdp, self.n_tp, self.n_all = n_fsdp, n_tp, n_fsdp * n_tp
        self.f, self.tp = lax.axis_index('fsdp'), lax.axis_index('tp')
        self.x, self.c = self.f // 2, lax.rem(self.f, 2)
        self.n_z = n_tp // 2
        self.z, self.y = self.tp // 2, lax.rem(self.tp, 2)
        self.index = self.tp * n_fsdp + self.f

    def other(self, k):
        i = lax.rem(self.index + k, self.n_all)
        return i // self.n_fsdp, lax.rem(i, self.n_fsdp)

    def every(self, fn):
        def go(k, _):
            fn(k)
            return 0
        lax.fori_loop(1, self.n_all, go, 0)


def dev(tp, f):
    return {'tp': tp, 'fsdp': f}


def rcopy(src, dst, ssem, rsem, to):
    return pltpu.make_async_remote_copy(src_ref=src, dst_ref=dst, send_sem=ssem, recv_sem=rsem, device_id=to, device_id_type=MESH)


def enter(at):
    barrier = pltpu.get_barrier_semaphore()

    def tell(k):
        tp, f = at.other(k)
        pl.semaphore_signal(barrier, inc=1, device_id=dev(tp, f), device_id_type=MESH)

    at.every(tell)
    pl.semaphore_wait(barrier, at.n_all - 1)


def head_kernel(sz, n_tp, vocab_tp, chunk, tok, early,
                h_hbm, lab_ref, mask_ref, gain, w_hbm,
                dw_hbm, gh_hbm, gg_out, l_hbm, g_hbm, h_all, ds_hbm,
                z, w, l0, l1, l2, l3, g0, g1, g2, g3, q0, q1, m, s, scale, lab, lab_in, mask_in, st_loc, got, res, st, top_row, hit, hid,
                acc, stage, sib_out, sib_in, y_sum, y_out, y_in, part, z_out, z_in, z_own, x_out, x_in, gh, gg, gg_in,
                w_s, w_r, loc, hsem, lsem, gsem, qsem, bsem, vsem, ssend, srecv, rsend, rrecv, tok_s, tok_r, blk, hx_s, hx_r, hz_s, hz_r, hy_s, hy_r, hc_s, hc_r,
                hid_sem, dw_copy, dw_send, dw_recv, own_sem, sib_s, sib_r, y_s, y_r, zz_s, zz_r, x_s, x_r, ag_s, ag_r, fw_s, fw_r, gh_sem, gain_s, gain_r):
    at = Place(sz.n, n_tp)
    me, n, n_z, width = at.f, sz.n, at.n_z, w_hbm.shape[1]
    per_f, d = h_hbm.shape
    tokens, own = per_f * n, per_f // n_tp
    lbufs, gbufs, qbufs = (l0, l1, l2, l3), (g0, g1, g2, g3), (q0, q1)
    far, sib = 1 - at.x, at.x * 2 + 1 - at.c
    through = far * 2 + at.c
    sibling, y_peer, x_peer = dev(at.tp, sib), dev(at.z * 2 + 1 - at.y, me), dev(at.tp, through)
    row_rem = sz.full * chunk
    row_odd = row_rem + sz.solid

    with scope('enter'):
        enter(at)

    def slab(f, tp):
        return pl.ds(pl.multiple_of((f * n_tp + tp) * own, own), own)

    def block(f):
        return pl.ds(pl.multiple_of(f * per_f, per_f), per_f)

    own2 = own // 2

    def part_of(f, tp, p):
        return pl.ds(pl.multiple_of((f * n_tp + tp) * own + p * own2, own2), own2)

    def h_to_x(p):
        return rcopy(h_hbm.at[pl.ds(pl.multiple_of(at.tp * own + p * own2, own2), own2), :], h_all.at[part_of(me, at.tp, p), :], hx_s.at[p], hx_r.at[p], x_peer)

    def h_from_x(p):
        here = h_all.at[part_of(through, at.tp, p), :]
        return rcopy(here, here, hx_s.at[p], hx_r.at[p], x_peer)

    def block_out():
        return rcopy(h_hbm, h_all.at[block(me), :], blk.at[0], blk.at[1], sibling)

    def block_in():
        return rcopy(h_hbm, h_all.at[block(sib), :], blk.at[0], blk.at[1], sibling)

    def moved(tp, ssem, rsem, to):
        here = h_all.at[slab(through, tp), :]
        return rcopy(here, here, ssem, rsem, to)

    def z_from(jj):
        return lax.rem(at.z + n_z - jj - 1, n_z)

    def h_to_z(jj, p):
        here = h_all.at[part_of(through, at.tp, p), :]
        return rcopy(here, here, hz_s.at[jj, p], hz_r.at[jj, p], dev(lax.rem(at.z + jj + 1, n_z) * 2 + at.y, me))

    def h_from_z(jj, p):
        here = h_all.at[part_of(through, z_from(jj) * 2 + at.y, p), :]
        return rcopy(here, here, hz_s.at[jj, p], hz_r.at[jj, p], sibling)

    def h_to_y(zo):
        return moved(zo * 2 + at.y, hy_s.at[zo], hy_r.at[zo], y_peer)

    def h_from_y(zo):
        return moved(zo * 2 + 1 - at.y, hy_s.at[zo], hy_r.at[zo], y_peer)

    def h_to_core(tp):
        return moved(tp, hc_s.at[tp], hc_r.at[tp], sibling)

    def h_from_core(tp):
        here = h_all.at[slab(far * 2 + 1 - at.c, tp), :]
        return rcopy(here, here, hc_s.at[tp], hc_r.at[tp], sibling)

    def tok_out(k):
        to = dev(at.tp, lax.rem(me + k, n))
        return [rcopy(lab_ref, lab_in.at[me], tok_s.at[0, k], tok_r.at[0, k], to), rcopy(mask_ref, mask_in.at[me], tok_s.at[1, k], tok_r.at[1, k], to)]

    def tok_in(k):
        src = lax.rem(me + n - k, n)
        return [rcopy(lab_ref, lab_in.at[src], tok_s.at[0, k], tok_r.at[0, k], sibling), rcopy(mask_ref, mask_in.at[src], tok_s.at[1, k], tok_r.at[1, k], sibling)]

    for p in (0, 1):
        h_to_x(p).start()
    block_out().start()
    for k in range(1, n):
        for cp in tok_out(k):
            cp.start()
    lab_in[me] = lab_ref[...]
    mask_in[me] = mask_ref[...]

    def remote(k, c, row0, rows):
        dest = lax.rem(me + k, n)
        return rcopy(w_hbm.at[rows_at(dest * sz.rows + row0, rows), :], w.at[rows_at(row0, rows), cols(me, width)], w_s.at[c, k], w_r.at[c, k], dev(at.tp, dest))

    def arrival(k, c, row0, rows):
        src = lax.rem(me + n - k, n)
        return rcopy(w_hbm.at[pl.ds(0, rows), :], w.at[rows_at(row0, rows), cols(src, width)], w_s.at[c, k], w_r.at[c, k], sibling)

    def local(c, row0, rows):
        return pltpu.make_async_copy(w_hbm.at[rows_at(me * sz.rows + row0, rows), :], w.at[rows_at(row0, rows), cols(me, width)], loc.at[c])

    def issue(c):
        local(c, c * chunk, chunk).start()
        for k in range(1, n):
            remote(k, c, c * chunk, chunk).start()

    def when_not_last(dest, fn):
        if sz.short:
            pl.when(dest != n - 1)(fn)

    def issue_rem():
        local(sz.full, row_rem, sz.solid).start()
        when_not_last(me, lambda: local(sz.full + 1, row_odd, sz.short).start())
        for k in range(1, n):
            remote(k, sz.full, row_rem, sz.solid).start()
            when_not_last(lax.rem(me + k, n), lambda: remote(k, sz.full + 1, row_odd, sz.short).start())

    ahead = min(AHEAD, sz.full)
    for c in range(ahead):
        issue(c)
    if sz.short:
        @pl.when(me == n - 1)
        def _():
            w[row_odd:, :] = jnp.zeros((sz.short, d), bf16)

    sub = min(256, own)
    slices, per_own = per_f // sub, own // sub
    lane = min(128, sub)

    def place(t, i):
        near = jnp.where(t == 0, me, sib) * per_f + i * sub
        j = i // per_own
        f = jnp.where(j < n_z, through, far * 2 + 1 - at.c)
        y = jnp.where(t == 2, at.y, 1 - at.y)
        away = (f * n_tp + lax.rem(j, n_z) * 2 + y) * own + lax.rem(i, per_own) * sub
        return pl.multiple_of(jnp.where(t < 2, near, away), sub)

    def norm(t):
        def load(i):
            here = pl.ds(place(t, i), sub)
            return pltpu.make_async_copy(h_hbm.at[cols(i, sub), :] if t == 0 else h_all.at[here, :], z.at[here, :], hsem.at[i])

        def begin(i, _):
            load(i).start()
            return 0

        def one(i, _):
            load(i).wait()
            here = pl.ds(place(t, i), sub)
            h = z[here, :].astype(f32)
            inv = lax.rsqrt(jnp.mean(h * h, axis=-1, keepdims=True) + NORM_EPS)
            z[here, :] = (h * inv * gain[...].astype(f32)).astype(bf16)
            return 0

        with scope(f'norm{t}'):
            lax.fori_loop(0, slices, begin, 0)
            lax.fori_loop(0, slices, one, 0)

    def spread_x(p):
        with scope('x_wait'):
            h_from_x(p).wait_recv()
        for jj in (2, 0, 1):
            if jj < n_z - 1:
                h_to_z(jj, p).start()

    norm(0)
    spread_x(0)
    with scope('blk_wait'):
        block_in().wait_recv()
    norm(1)
    spread_x(1)
    h_to_y(at.z).start()
    h_to_core(at.tp).start()
    with scope('tok_wait'):
        for k in range(1, n):
            for cp in tok_in(k):
                cp.wait_recv()
    count = jnp.sum(mask_in[...], axis=(0, 2), keepdims=True)[0]
    for f in range(n):
        here = pl.ds(f * per_f, per_f)
        scale[0:1, here] = mask_in[f] / count
        rel = lab_in[f] - at.tp * vocab_tp
        lab[0:1, here] = jnp.where(jnp.logical_and(rel >= 0, rel < vocab_tp), rel - me * sz.rows, -1)

    def spread_z():
        with scope('z_wait'):
            for jj in range(n_z - 1):
                for p in (0, 1):
                    h_from_z(jj, p).wait_recv()
                h_to_y(z_from(jj)).start()
                h_to_core(z_from(jj) * 2 + at.y).start()

    def spread_y():
        with scope('hy_wait'):
            for k in range(n_z):
                zo = lax.rem(at.z + n_z - k, n_z)
                h_from_y(zo).wait_recv()
                h_to_core(zo * 2 + 1 - at.y).start()

    def far_ready(y):
        with scope('core_wait'):
            for zo in range(n_z):
                h_from_core(zo * 2 + y).wait_recv()

    m[...] = jnp.full(m.shape, NEG, f32)
    s[...] = jnp.zeros(s.shape, f32)
    per_buf = tok // sub
    n_buf = slices // per_buf

    def out_copies(row0, rows, t, b):
        return [pltpu.make_async_copy(lbufs[b * n_buf + i // per_buf].at[pl.ds(0, rows), pl.ds(i % per_buf * sub, sub)],
                                      l_hbm.at[rows_at(row0, rows), pl.ds(place(t, i), sub)], lsem.at[b * n_buf + i // per_buf]) for i in range(slices)]

    def out_done(rows, b):
        for i in range(n_buf):
            pltpu.make_async_copy(lbufs[b * n_buf + i].at[pl.ds(0, rows), :], l_hbm.at[pl.ds(0, rows), pl.ds(0, tok)], lsem.at[b * n_buf + i]).wait()

    def statistics(read, rows, t0):
        group = min(4, rows // 8)
        for c1 in range(0, sub, lane):
            sl = pl.ds(pl.multiple_of(t0 + c1, lane), lane)
            big, tot = m[:, sl], s[:, sl]
            for g in range(0, rows // 8, group):
                piece = [read(r, c1) for r in range(g, min(g + group, rows // 8))]
                new = functools.reduce(jnp.maximum, piece, big)
                tot = tot * jnp.exp2(big - new)
                for x in piece:
                    tot += jnp.exp2(x - new)
                big = new
            m[:, sl], s[:, sl] = big, tot

    def slice_at(b, i):
        return lbufs[b * n_buf + i // per_buf], i % per_buf * sub

    def late_statistics(t, b):
        for i in range(slices - lag, slices):
            buf, i0 = slice_at(b, i)
            statistics(lambda r, c1: buf[8 * r:8 * r + 8, i0 + c1:i0 + c1 + lane], chunk, place(t, i))

    def logits_tile(row0, rows, t, b, masked):
        for i in range(slices):
            t0 = place(t, i)
            logits = dot_nt(w[rows_at(row0, rows), :], z[pl.ds(t0, sub), :]) * LOG2E
            if masked:
                ids = lax.broadcasted_iota(jnp.int32, (rows, sub), 0)
                logits = jnp.where(ids < jnp.where(me == n - 1, sz.solid, sz.rem), logits, NEG)
            buf, i0 = slice_at(b, i)
            buf[0:rows, i0:i0 + sub] = logits
            if masked or i < slices - lag:
                statistics(lambda r, c1: logits[8 * r:8 * r + 8, c1:c1 + lane], rows, t0)

    lag = 2
    for i in range(slices - lag, slices):
        buf, i0 = slice_at(1, i)
        buf[:, i0:i0 + sub] = jnp.full((chunk, sub), NEG, f32)

    n_a = min(3, sz.full)
    n_c = min(3, sz.full - n_a)
    k_b, k_c = 2 * n_a, 3 * n_a
    k_d = k_c + 3 * n_c
    k_e = k_d + n_a + n_c

    def item(k):
        u, v = k - k_c, k - k_e
        c = jnp.where(k < k_b, k // 2, jnp.where(k < k_c, k - k_b, jnp.where(k < k_d, n_a + u // 3, jnp.where(k < k_e, k - k_d, n_a + n_c + v // 4))))
        t = jnp.where(k < k_b, lax.rem(k, 2), jnp.where(k < k_c, 2, jnp.where(k < k_d, lax.rem(u, 3), jnp.where(k < k_e, 3, lax.rem(v, 4)))))
        return c, t

    def work(i2, _):
        for b in (0, 1):
            k = 2 * i2 + b
            c, t = item(k)

            @pl.when(t == 0)
            def _():
                with scope('w_wait'):
                    local(c, c * chunk, chunk).wait()
                    for j in range(1, n):
                        arrival(j, c, c * chunk, chunk).wait_recv()

                @pl.when(c + ahead < sz.full)
                def _():
                    issue(c + ahead)

                @pl.when(c + ahead == sz.full)
                def _():
                    issue_rem()

            @pl.when(k == k_b)
            def _():
                spread_z()
                far_ready(at.y)
                norm(2)

            @pl.when(k == max(k_d - 3, k_c))
            def _():
                spread_y()

            @pl.when(k == k_d)
            def _():
                far_ready(1 - at.y)
                norm(3)

            with scope('l_wait'):
                @pl.when(k >= 2)
                def _():
                    out_done(chunk, b)
            with scope('l_tile'):
                late_statistics(item(jnp.maximum(k - 1, 0))[1], 1 - b)
                logits_tile(c * chunk, chunk, t, b, False)
            for cp in out_copies(c * chunk, chunk, t, b):
                cp.start()
        return 0

    lax.fori_loop(0, sz.full * 2, work, 0)
    late_statistics(item(4 * sz.full - 1)[1], 1)
    with scope('w_wait_rem'):
        local(sz.full, row_rem, sz.solid).wait()
        when_not_last(me, lambda: local(sz.full + 1, row_odd, sz.short).wait())
        for k in range(1, n):
            arrival(k, sz.full, row_rem, sz.solid).wait_recv()
            when_not_last(me, lambda: arrival(k, sz.full + 1, row_odd, sz.short).wait_recv())

    def work_rem(i2, _):
        for b in (0, 1):
            @pl.when(i2 == 0)
            def _():
                out_done(chunk, b)

            @pl.when(i2 > 0)
            def _():
                out_done(sz.rem, b)
            logits_tile(row_rem, sz.rem, 2 * i2 + b, b, True)
            for cp in out_copies(row_rem, sz.rem, 2 * i2 + b, b):
                cp.start()
        return 0

    with scope('l_rem'):
        lax.fori_loop(0, 2, work_rem, 0)

    big = jnp.max(m[...], axis=0, keepdims=True)
    st_loc[0:1, :] = big
    st_loc[1:2, :] = jnp.sum(s[...] * jnp.exp2(m[...] - big), axis=0, keepdims=True)
    mine = slab(at.f, at.tp)

    def ask(k):
        tp, f = at.other(k)
        return rcopy(st_loc.at[:, slab(f, tp)], got.at[k], ssend.at[k], srecv.at[k], dev(tp, f))

    def answer(k):
        tp, f = at.other(k)
        return rcopy(res, st.at[:, mine], rsend.at[k], rrecv.at[k], dev(tp, f))

    def answered(k):
        tp, f = at.other(at.n_all - k)
        return rcopy(res, st.at[:, slab(f, tp)], rsend.at[k], rrecv.at[k], dev(tp, f))

    n_tok = tokens // tok

    def load_l(row0, rows, k, b):
        return pltpu.make_async_copy(l_hbm.at[rows_at(row0, rows), cols(k, tok)], lbufs[b].at[pl.ds(0, rows), :], lsem.at[b])

    def load_g(row0, rows, k, b):
        return pltpu.make_async_copy(g_hbm.at[rows_at(row0, rows), cols(k, tok)], gbufs[b].at[pl.ds(0, rows), :], gsem.at[b])

    def save_g(row0, rows, k, b):
        return pltpu.make_async_copy(gbufs[b].at[pl.ds(0, rows), :], g_hbm.at[rows_at(row0, rows), cols(k, tok)], gsem.at[b])

    at.every(lambda k: ask(k).start())
    got[0] = st_loc[:, mine]
    for b in (0, 1):
        out_done(sz.rem, b)
    for b in range(4):
        load_l(0, chunk, b, b).start()
    h_load = pltpu.make_async_copy(h_hbm.at[pl.ds(pl.multiple_of(at.tp * own, own), own), :], hid, hid_sem.at[0])
    h_load.start()
    acc[...] = jnp.zeros(acc.shape, f32)
    hit[...] = jnp.zeros(hit.shape, f32)
    with scope('ask_wait'):
        at.every(lambda k: ask(k).wait_recv())
    tops = got[:, 0:1, :]
    top = jnp.max(tops, axis=0)
    res[...] = top + jnp.log2(jnp.sum(got[:, 1:2, :] * jnp.exp2(tops - top[None]), axis=0))
    at.every(lambda k: answer(k).start())
    st[:, mine] = res[...]
    with scope('answer_wait'):
        at.every(lambda k: answered(k).wait_recv())
    top_row[...] = st[...] - jnp.log2(scale[...])

    def gradient(x, sl, row0):
        rows = x.shape[0]
        sc = scale[0:1, sl]
        x3 = x.reshape(rows // 8, 8, x.shape[1])
        p = jnp.exp2(x3 - top_row[0:1, sl][None])
        is_label = lax.broadcasted_iota(jnp.int32, p.shape, 0) * 8 == (lab[0:1, sl] - row0 - lax.broadcasted_iota(jnp.int32, (8, x.shape[1]), 0))[None]
        hit[...] += jnp.sum(jnp.where(is_label, x3, 0.0), axis=0) * sc
        return jnp.where(is_label, p - sc[None], p).reshape(x.shape).astype(bf16)

    step = min(256, tok)

    def grad_tile(row0, rows, k, b, fresh):
        total = None
        for c0 in range(0, tok, step):
            if fresh:
                for c1 in range(c0, c0 + step, lane):
                    gbufs[b][0:rows, c1:c1 + lane] = gradient(lbufs[b][0:rows, c1:c1 + lane], pl.ds(pl.multiple_of(k * tok + c1, lane), lane), row0)
            p = dot_nn(gbufs[b][0:rows, c0:c0 + step], z[pl.ds(pl.multiple_of(k * tok + c0, step), step), :])
            total = p if total is None else total + p
        acc[0:rows, :] += total

    def aside(c, rows):
        slot = lax.rem(c, 2)
        return pltpu.make_async_copy(stage.at[slot, pl.ds(0, rows), :], ds_hbm.at[rows_at(c * chunk, rows), :], dw_copy.at[slot])

    def keep_own(c, rows):
        slot = lax.rem(c, 2)
        return pltpu.make_async_copy(stage.at[slot, pl.ds(0, rows), cols(me, width)], dw_hbm.at[rows_at(me * sz.rows + c * chunk, rows), :], own_sem.at[slot])

    def sends(c, rows):
        out = []
        for i, f in enumerate((far * 2, far * 2 + 1, sib)):
            out.append(rcopy(ds_hbm.at[rows_at(c * chunk, rows), cols(f, width)], dw_hbm.at[rows_at(me * sz.rows + c * chunk, rows), :],
                             dw_send.at[c, i], dw_recv.at[lax.rem(f + n - me, n)], dev(at.tp, f)))
        return out

    def ship(c, rows):
        with scope('ship'):
            stage[lax.rem(c, 2), 0:rows, :] = acc[0:rows, :].astype(bf16)
            acc[...] = jnp.zeros(acc.shape, f32)
        aside(c, rows).start()
        keep_own(c, rows).start()

    def flush(c, rows):
        aside(c, rows).wait()
        keep_own(c, rows).wait()
        for cp in sends(c, rows):
            cp.start()

    def early_chunk(c, _):
        def quad(i, _):
            for b in range(4):
                k = 4 * i + b
                with scope('b1_wait'):
                    load_l(0, chunk, 0, b).wait()

                    @pl.when(jnp.logical_not(jnp.logical_and(c == 0, i == 0)))
                    def _():
                        save_g(0, chunk, 0, b).wait()
                with scope('b1_tile'):
                    grad_tile(c * chunk, chunk, k, b, True)
                save_g(c * chunk, chunk, k, b).start()
                wrap = k + 4 >= n_tok
                c2 = jnp.where(wrap, c + 1, c)

                @pl.when(c2 < early)
                def _():
                    load_l(c2 * chunk, chunk, jnp.where(wrap, k + 4 - n_tok, k + 4), b).start()

            @pl.when(jnp.logical_and(i == 0, c > 0))
            def _():
                flush(c - 1, chunk)
            return 0
        lax.fori_loop(0, n_tok // 4, quad, 0)
        ship(c, chunk)
        return 0

    lax.fori_loop(0, early, early_chunk, 0)

    half = own // ROUNDS
    groups = 2 * n_z
    last = ROUNDS * groups
    row_low = early * chunk
    low = [(j, chunk) for j in range(sz.full - early)] + [(sz.full - early, sz.rem)]
    per_l = tok // half

    def group_of(q):
        r, g = q // groups, lax.rem(q, groups)
        xi, jj = g // n_z, lax.rem(g, n_z)
        return r, xi, jj, jnp.where(xi == 0, far, at.x), lax.rem(at.z + jj + 1, n_z)

    def pieces(q, b):
        r, _, _, xb, zb = group_of(q)
        cb = at.c if b == 1 else 1 - at.c
        return [pl.multiple_of((xb * 2 + cb) * per_f + (zb * 2 + yb) * own + r * half, half) for yb in (1 - at.y, at.y)]

    def l_part(b, j, i, rows):
        p = 2 * j + i
        return lbufs[2 * b + p // per_l].at[pl.ds(0, rows), pl.ds(p % per_l * half, half)]

    def block_loads(q, b):
        out = []
        for i, t0 in enumerate(pieces(q, b)):
            out.append(pltpu.make_async_copy(g_hbm.at[pl.ds(0, row_low), pl.ds(t0, half)], qbufs[b].at[pl.ds(0, row_low), pl.ds(i * half, half)], qsem.at[b, i]))
            for j, rows in low:
                out.append(pltpu.make_async_copy(l_hbm.at[pl.ds(row_low + j * chunk, rows), pl.ds(t0, half)], l_part(b, j, i, rows), bsem.at[b, 2 * j + i]))
        return out

    def block_saves(q, b):
        return [pltpu.make_async_copy(qbufs[b].at[pl.ds(row_low, sz.rows - row_low), pl.ds(i * half, half)],
                                      g_hbm.at[pl.ds(row_low, sz.rows - row_low), pl.ds(t0, half)], vsem.at[b, i]) for i, t0 in enumerate(pieces(q, b))]

    def block_dot(q, b):
        for i, t0 in enumerate(pieces(q, b)):
            for j, rows in low:
                row0 = row_low + j * chunk
                qbufs[b][row0:row0 + rows, i * half:(i + 1) * half] = gradient(l_part(b, j, i, rows)[...], pl.ds(t0, half), row0)
        return dot_tn(qbufs[b][...], w[...])

    def to_sib(q):
        slot = lax.rem(q, 2)
        return rcopy(sib_out.at[slot], sib_in.at[slot], sib_s.at[slot], sib_r.at[slot], sibling)

    def to_y(q):
        slot, land = lax.rem(q, 2), lax.rem(q, y_in.shape[0])
        return rcopy(y_out.at[slot], y_in.at[land], y_s.at[slot], y_r.at[land], y_peer)

    def to_z(q):
        r, xi, jj, _, zb = group_of(q)
        return rcopy(z_out.at[jj], z_in.at[r, xi, jj], zz_s.at[jj], zz_r.at[r, xi, jj], dev(zb * 2 + at.y, me))

    def to_x(r):
        return rcopy(x_out, x_in.at[r], x_s.at[0], x_r.at[r], x_peer)

    def z_stage(q):
        _, xi, jj, _, _ = group_of(q)
        with scope('y_wait'):
            to_y(q).wait_recv()
        val = part[lax.rem(q, part.shape[0])] + y_in[lax.rem(q, y_in.shape[0])].astype(f32)

        @pl.when(jj == n_z - 1)
        def _():
            z_own[xi] = val

        @pl.when(jj < n_z - 1)
        def _():
            @pl.when(q >= n_z)
            def _():
                to_z(q - n_z).wait_send()
            z_out[jj] = val.astype(bf16)
            to_z(q).start()

    def z_sum(r, xi):
        val = z_own[xi]
        for jj in range(n_z - 1):
            rcopy(z_out.at[0], z_in.at[r, xi, jj], zz_s.at[jj], zz_r.at[r, xi, jj], sibling).wait_recv()
            val = val + z_in[r, xi, jj].astype(f32)
        return val

    def x_stage(r):
        @pl.when(r > 0)
        def _():
            to_x(0).wait_send()
        with scope('x_stage'):
            x_out[...] = z_sum(r, 0).astype(bf16)
        to_x(r).start()

    def home(tp, r):
        return gh_hbm.at[pl.ds(pl.multiple_of(tp * own + r * half, half), half), :]

    def gathers(r):
        out = [rcopy(gh.at[r], home(at.tp, r), ag_s.at[r, n_z - 1], fw_r.at[r, at.z], y_peer)]
        for jj in range(n_z - 1):
            to = lax.rem(at.z + jj + 1, n_z)
            out.append(rcopy(gh.at[r], home(at.tp, r), ag_s.at[r, jj], ag_r.at[r, jj], dev(to * 2 + at.y, me)))
        return out

    def keep(r):
        return pltpu.make_async_copy(gh.at[r], home(at.tp, r), gh_sem.at[r])

    def arrived(r, jj):
        return rcopy(gh.at[r], home(z_from(jj) * 2 + at.y, r), ag_s.at[r, jj], ag_r.at[r, jj], sibling)

    def onward(r, jj):
        here = home(z_from(jj) * 2 + at.y, r)
        return rcopy(here, here, fw_s.at[r, jj], fw_r.at[r, z_from(jj)], y_peer)

    def tell_gain(k):
        tp, f = at.other(k)
        return rcopy(gg, gg_in.at[at.index], gain_s.at[k], gain_r.at[k], dev(tp, f))

    def heard_gain(k):
        i = lax.rem(at.index + at.n_all - k, at.n_all)
        return rcopy(gg, gg_in.at[i], gain_s.at[k], gain_r.at[k], sibling)

    def final(r):
        with scope('final_wait'):
            to_x(r).wait_recv()
            dz = z_sum(r, 1) + x_in[r].astype(f32)
        h = hid[pl.ds(pl.multiple_of(r * half, half), half), :].astype(f32)
        inv = lax.rsqrt(jnp.mean(h * h, axis=-1, keepdims=True) + NORM_EPS)
        normed = h * inv
        a = dz * gain[...].astype(f32)
        gh[r] = (inv * (a - normed * jnp.mean(a * normed, axis=-1, keepdims=True))).astype(bf16)
        gg[0:1, 0:d] += jnp.sum(dz * normed, axis=0, keepdims=True)
        if r == 1:
            hits = jnp.sum(jnp.sum(hit[...], axis=0, keepdims=True), axis=1, keepdims=True)
            gg[0:1, d:] = jnp.broadcast_to(hits, (1, gg.shape[1] - d))
            at.every(lambda k: tell_gain(k).start())
            gg_in[at.index] = gg[...]
        keep(r).start()
        for cp in gathers(r):
            cp.start()

    def forward(r, jj):
        with scope('fw_wait'):
            arrived(r, jj).wait_recv()
        onward(r, jj).start()

    for b in range(4):
        save_g(0, chunk, 0, b).wait()
    h_load.wait()
    gg[...] = jnp.zeros(gg.shape, f32)
    for b in (0, 1):
        for cp in block_loads(0, b):
            cp.start()

    def dz_group(q, _):
        for b in (0, 1):
            with scope('a_wait'):
                for cp in block_loads(q, b):
                    cp.wait()

                @pl.when(q > 0)
                def _():
                    for cp in block_saves(q - 1, b):
                        cp.wait()
            slot = lax.rem(q, 2)
            if b == 0:
                @pl.when(q >= 2)
                def _():
                    to_sib(q - 2).wait_send()
                with scope('a_dot0'):
                    sib_out[slot] = block_dot(q, b).astype(bf16)
                to_sib(q).start()
            else:
                @pl.when(q >= 2)
                def _():
                    to_y(q - 2).wait_send()
                with scope('a_dot1'):
                    val = block_dot(q, b)
                    y_sum[...] = val[0:half]
                    part[lax.rem(q, part.shape[0])] = val[half:]
                with scope('sib_wait'):
                    to_sib(q).wait_recv()
                y_out[slot] = (y_sum[...] + sib_in[slot, 0:half].astype(f32)).astype(bf16)
                part[lax.rem(q, part.shape[0])] += sib_in[slot, half:].astype(f32)
                to_y(q).start()
            for cp in block_saves(q, b):
                cp.start()

            @pl.when(q + 1 < last)
            def _():
                for cp in block_loads(q + 1, b):
                    cp.start()

        @pl.when(q == 0)
        def _():
            flush(early - 1, chunk)

        @pl.when(q >= 2)
        def _():
            z_stage(q - 2)

        @pl.when(q == n_z + 3)
        def _():
            x_stage(0)

        @pl.when(q == max(last - 6, n_z + 4))
        def _():
            final(0)
        return 0

    lax.fori_loop(0, last, dz_group, 0)
    z_stage(last - 2)
    for jj in range(n_z - 1):
        forward(0, jj)
    for b in (0, 1):
        for cp in block_saves(last - 1, b):
            cp.wait()

    for b in range(4):
        load_g(early * chunk, chunk, b, b).start()

    quads = n_tok // 4
    steps = [jj for jj in (2, 0, 1) if jj < n_z - 1]
    first_step = early + 2

    def late_chunk(c, _):
        def quad(i, _):
            for b in range(4):
                k = 4 * i + b
                with scope('b2_wait'):
                    load_g(0, chunk, 0, b).wait()
                with scope('b2_tile'):
                    grad_tile(c * chunk, chunk, k, b, False)
                wrap = k + 4 >= n_tok
                c2, k2 = jnp.where(wrap, c + 1, c), jnp.where(wrap, k + 4 - n_tok, k + 4)

                @pl.when(c2 < sz.full)
                def _():
                    load_g(c2 * chunk, chunk, k2, b).start()

                @pl.when(c2 == sz.full)
                def _():
                    load_g(row_rem, sz.rem, k2, b).start()
                if b == 0:
                    @pl.when(jnp.logical_and(i == 0, c > early))
                    def _():
                        flush(c - 1, chunk)

            for t, jj in enumerate(steps):
                @pl.when((c - first_step) * quads + i == t)
                def _():
                    forward(1, jj)
            return 0
        lax.fori_loop(0, quads, quad, 0)
        ship(c, chunk)

        @pl.when(c == early)
        def _():
            z_stage(last - 1)
            x_stage(1)

        @pl.when(c == early + 1)
        def _():
            final(1)
        return 0

    lax.fori_loop(early, sz.full, late_chunk, 0)
    for t, jj in enumerate(steps):
        if t >= (sz.full - first_step) * quads:
            forward(1, jj)

    def late_rem(i, _):
        for b in range(4):
            with scope('b2_wait'):
                load_g(row_rem, sz.rem, 0, b).wait()
            with scope('b2_rem'):
                grad_tile(row_rem, sz.rem, 4 * i + b, b, False)

            @pl.when(4 * i + b + 4 < n_tok)
            def _():
                load_g(row_rem, sz.rem, 4 * i + b + 4, b).start()
            if b == 0:
                @pl.when(i == 0)
                def _():
                    flush(sz.full - 1, chunk)
        return 0

    lax.fori_loop(0, n_tok // 4, late_rem, 0)
    ship(sz.full, sz.rem)
    flush(sz.full, sz.rem)

    with scope('t_gain'):
        at.every(lambda k: heard_gain(k).wait_recv())
    total = jnp.sum(gg_in[...], axis=0)
    gg_out[0:1, 0:d] = total[0:1, 0:d]
    gg_out[0:1, d:] = (jnp.sum(st[...] * scale[...], axis=1, keepdims=True) - total[0:1, d:]) * (1.0 / LOG2E)
    with scope('t_small'):
        at.every(lambda k: ask(k).wait_send())
        at.every(lambda k: answer(k).wait_send())
        at.every(lambda k: tell_gain(k).wait_send())
        for k in range(1, n):
            for cp in tok_out(k):
                cp.wait_send()
        block_out().wait_send()
        for p in (0, 1):
            h_to_x(p).wait_send()
            for jj in range(n_z - 1):
                h_to_z(jj, p).wait_send()
        for zo in range(n_z):
            h_to_y(zo).wait_send()
        for tp in range(n_tp):
            h_to_core(tp).wait_send()

        def w_sent(c, _):
            for k in range(1, n):
                remote(k, c, c * chunk, chunk).wait_send()
            return 0

        lax.fori_loop(0, sz.full, w_sent, 0)
        for k in range(1, n):
            remote(k, sz.full, row_rem, sz.solid).wait_send()
            when_not_last(lax.rem(me + k, n), lambda: remote(k, sz.full + 1, row_odd, sz.short).wait_send())
        for q in (last - 2, last - 1):
            to_sib(q).wait_send()
            to_y(q).wait_send()
        for q in range(last - n_z, last - 1):
            to_z(q).wait_send()
        to_x(1).wait_send()
    with scope('t_send'):
        def sent(c, _):
            for cp in sends(c, chunk):
                cp.wait_send()
            return 0
        lax.fori_loop(0, sz.full, sent, 0)
        for cp in sends(sz.full, sz.rem):
            cp.wait_send()
    for r in range(ROUNDS):
        with scope(f't_gather{r}'):
            keep(r).wait()
            for cp in gathers(r):
                cp.wait_send()
            for jj in range(n_z - 1):
                onward(r, jj).wait_send()
            for zo in range(n_z):
                rcopy(gh.at[r], home(zo * 2 + 1 - at.y, r), ag_s.at[r, 0], fw_r.at[r, zo], y_peer).wait_recv()
    with scope('t_dw'):
        for k in range(1, n):
            src = lax.rem(me + n - k, n)
            rcopy(dw_hbm.at[pl.ds(0, sz.rows), :], dw_hbm.at[rows_at(src * sz.rows, sz.rows), :], dw_send.at[0, 0], dw_recv.at[k], sibling).wait_recv()


HBM = pl.BlockSpec(memory_space=pl.ANY)
VM = pl.BlockSpec(memory_space=pltpu.VMEM)
DMA = pltpu.SemaphoreType.DMA


def solution(mesh, chunk=CHUNK, tok=TOK, early=EARLY):
    n_fsdp, n_tp = mesh.shape['fsdp'], mesh.shape['tp']
    n_all, n_z = n_fsdp * n_tp, n_tp // 2
    S, V = jax.ShapeDtypeStruct, pltpu.VMEM
    i32 = jnp.int32

    def per_device(hidden, labels, tok_mask, norm_gain, w_rows):
        per_f, d = hidden.shape
        width, vocab_tp = w_rows.shape
        tokens, own = per_f * n_fsdp, per_f // n_tp
        half = own // ROUNDS
        sz = Sizes(vocab_tp, n_fsdp, chunk)
        n_low = sz.full - early + 1

        dw_t, grad_hidden, sums, *_ = pl.pallas_call(
            functools.partial(head_kernel, sz, n_tp, vocab_tp, chunk, tok, early),
            out_shape=(S((n_fsdp * sz.rows, width), bf16), S(hidden.shape, bf16), S((1, d + 128), f32),
                       S((sz.rows, tokens), f32), S((sz.rows, tokens), bf16), S((tokens, d), bf16), S(((sz.full + 1) * chunk, d), bf16)),
            in_specs=[HBM, VM, VM, VM, HBM], out_specs=(HBM, HBM, VM, HBM, HBM, HBM, HBM),
            scratch_shapes=[
                V((tokens, d), bf16), V((sz.rows, d), bf16), *[V((chunk, tok), f32)] * 4, *[V((chunk, tok), bf16)] * 4, *[V((sz.rows, 2 * half), bf16)] * 2,
                V((8, tokens), f32), V((8, tokens), f32), V((1, tokens), f32), V((1, tokens), i32), V((n_fsdp, 1, per_f), i32), V((n_fsdp, 1, per_f), f32),
                V((2, tokens), f32), V((n_all, 2, own), f32), V((1, own), f32), V((1, tokens), f32), V((1, tokens), f32), V((8, min(128, half)), f32), V((own, d), bf16),
                V((chunk, d), f32), V((2, chunk, d), bf16), V((2, 2 * half, d), bf16), V((2, 2 * half, d), bf16), V((half, d), f32),
                V((2, half, d), bf16), V((6, half, d), bf16), V((3, half, d), f32), V((n_z - 1, half, d), bf16), V((ROUNDS, 2, n_z - 1, half, d), bf16), V((2, half, d), f32),
                V((half, d), bf16), V((ROUNDS, half, d), bf16), V((ROUNDS, half, d), bf16), V((1, d + 128), f32), V((n_all, 1, d + 128), f32),
                DMA((sz.full + 2, n_fsdp)), DMA((sz.full + 2, n_fsdp)), DMA((sz.full + 2,)), DMA((per_f // min(256, own),)), DMA((4,)), DMA((4,)), DMA((2, 2)), DMA((2, 2 * n_low)), DMA((2, 2)),
                DMA((n_all,)), DMA((n_all,)), DMA((n_all,)), DMA((n_all,)), DMA((2, n_fsdp)), DMA((2, n_fsdp)), DMA((2,)), DMA((2,)), DMA((2,)),
                DMA((n_z - 1, 2)), DMA((n_z - 1, 2)), DMA((n_z,)), DMA((n_z,)), DMA((n_tp,)), DMA((n_tp,)),
                DMA((1,)), DMA((2,)), DMA((sz.full + 1, 3)), DMA((n_fsdp,)), DMA((2,)), DMA((2,)), DMA((2,)), DMA((2,)), DMA((8,)),
                DMA((n_z - 1,)), DMA((ROUNDS, 2, n_z - 1)), DMA((1,)), DMA((ROUNDS,)),
                DMA((ROUNDS, n_z)), DMA((ROUNDS, n_z)), DMA((ROUNDS, n_z)), DMA((ROUNDS, n_z)), DMA((ROUNDS,)), DMA((n_all,)), DMA((n_all,))],
            compiler_params=pltpu.CompilerParams(vmem_limit_bytes=VMEM_LIMIT, collective_id=0, has_side_effects=True), name='head',
        )(hidden, labels[None, :], tok_mask[None, :], norm_gain[None, :], w_rows.T)
        return sums[0, d], grad_hidden, dw_t[:vocab_tp].T, sums[0, :d]

    return jax.shard_map(per_device, mesh=mesh, in_specs=(P('fsdp', None), P('fsdp'), P('fsdp'), P(), P('fsdp', 'tp')), out_specs=(P(), P('fsdp', None), P('fsdp', 'tp'), P()), check_vma=False)
```

```python
import functools

import jax
import jax.numpy as jnp
from jax import lax
from jax.experimental import pallas as pl
from jax.experimental.pallas import tpu as pltpu
from jax.sharding import PartitionSpec as P

NORM_EPS = 1e-6
LOG2E = 1.4426950408889634
NEG = -1e30
CHUNK = 512
TOK = 1024
EARLY = 5
AHEAD = 5
ROUNDS = 2
VMEM_LIMIT = 67_043_328
MESH = pl.DeviceIdType.MESH
scope = jax.named_scope
f32, bf16 = jnp.float32, jnp.bfloat16


def dot_nt(a, b):
    return lax.dot_general(a, b, (((1,), (1,)), ((), ())), preferred_element_type=f32)


def dot_tn(a, b):
    return lax.dot_general(a, b, (((0,), (0,)), ((), ())), preferred_element_type=f32)


def dot_nn(a, b):
    return lax.dot_general(a, b, (((1,), (0,)), ((), ())), preferred_element_type=f32)


def cols(k, size):
    return pl.ds(pl.multiple_of(k * size, size), size)


def rows_at(row0, rows):
    return pl.ds(pl.multiple_of(row0, 16), rows)


class Sizes:
    def __init__(self, vocab_tp, n_fsdp, chunk):
        self.n = n_fsdp
        self.rows = -(-vocab_tp // (n_fsdp * 16)) * 16
        self.short = n_fsdp * self.rows - vocab_tp
        self.full = self.rows // chunk
        self.rem = self.rows - self.full * chunk
        self.solid = self.rem - self.short
        assert self.rem > self.short and self.rem % 16 == 0 and self.short % 16 == 0


class Place:
    def __init__(self, n_fsdp, n_tp):
        self.n_fsdp, self.n_tp, self.n_all = n_fsdp, n_tp, n_fsdp * n_tp
        self.f, self.tp = lax.axis_index('fsdp'), lax.axis_index('tp')
        self.x, self.c = self.f // 2, lax.rem(self.f, 2)
        self.n_z = n_tp // 2
        self.z, self.y = self.tp // 2, lax.rem(self.tp, 2)
        self.index = self.tp * n_fsdp + self.f

    def other(self, k):
        i = lax.rem(self.index + k, self.n_all)
        return i // self.n_fsdp, lax.rem(i, self.n_fsdp)

    def every(self, fn):
        def go(k, _):
            fn(k)
            return 0
        lax.fori_loop(1, self.n_all, go, 0)


def dev(tp, f):
    return {'tp': tp, 'fsdp': f}


def rcopy(src, dst, ssem, rsem, to):
    return pltpu.make_async_remote_copy(src_ref=src, dst_ref=dst, send_sem=ssem, recv_sem=rsem, device_id=to, device_id_type=MESH)


def enter(at):
    barrier = pltpu.get_barrier_semaphore()

    def tell(k):
        tp, f = at.other(k)
        pl.semaphore_signal(barrier, inc=1, device_id=dev(tp, f), device_id_type=MESH)

    at.every(tell)
    pl.semaphore_wait(barrier, at.n_all - 1)


def head_kernel(sz, n_tp, vocab_tp, chunk, tok, early,
                h_hbm, lab_ref, mask_ref, gain, w_hbm,
                dw_hbm, gh_hbm, gg_out, l_hbm, g_hbm, h_all, ds_hbm,
                z, w, l0, l1, l2, l3, g0, g1, g2, g3, q0, q1, m, s, scale, lab, lab_in, mask_in, st_loc, got, res, st, top_row, hit, hid,
                acc, stage, sib_out, sib_in, y_sum, y_out, y_in, part, z_out, z_in, z_own, x_out, x_in, gh, gg, gg_in,
                w_s, w_r, loc, hsem, lsem, gsem, qsem, bsem, vsem, ssend, srecv, rsend, rrecv, tok_s, tok_r, blk, hx_s, hx_r, hz_s, hz_r, hy_s, hy_r, hc_s, hc_r,
                hid_sem, dw_copy, dw_send, dw_recv, own_sem, sib_s, sib_r, y_s, y_r, zz_s, zz_r, x_s, x_r, ag_s, ag_r, fw_s, fw_r, gh_sem, gain_s, gain_r):
    at = Place(sz.n, n_tp)
    me, n, n_z, width = at.f, sz.n, at.n_z, w_hbm.shape[1]
    per_f, d = h_hbm.shape
    tokens, own = per_f * n, per_f // n_tp
    lbufs, gbufs, qbufs = (l0, l1, l2, l3), (g0, g1, g2, g3), (q0, q1)
    far, sib = 1 - at.x, at.x * 2 + 1 - at.c
    through = far * 2 + at.c
    sibling, y_peer, x_peer = dev(at.tp, sib), dev(at.z * 2 + 1 - at.y, me), dev(at.tp, through)
    row_rem = sz.full * chunk
    row_odd = row_rem + sz.solid

    with scope('enter'):
        enter(at)

    def slab(f, tp):
        return pl.ds(pl.multiple_of((f * n_tp + tp) * own, own), own)

    def block(f):
        return pl.ds(pl.multiple_of(f * per_f, per_f), per_f)

    own2 = own // 2

    def part_of(f, tp, p):
        return pl.ds(pl.multiple_of((f * n_tp + tp) * own + p * own2, own2), own2)

    def h_to_x(p):
        return rcopy(h_hbm.at[pl.ds(pl.multiple_of(at.tp * own + p * own2, own2), own2), :], h_all.at[part_of(me, at.tp, p), :], hx_s.at[p], hx_r.at[p], x_peer)

    def h_from_x(p):
        here = h_all.at[part_of(through, at.tp, p), :]
        return rcopy(here, here, hx_s.at[p], hx_r.at[p], x_peer)

    def block_out():
        return rcopy(h_hbm, h_all.at[block(me), :], blk.at[0], blk.at[1], sibling)

    def block_in():
        return rcopy(h_hbm, h_all.at[block(sib), :], blk.at[0], blk.at[1], sibling)

    def moved(tp, ssem, rsem, to):
        here = h_all.at[slab(through, tp), :]
        return rcopy(here, here, ssem, rsem, to)

    def z_from(jj):
        return lax.rem(at.z + n_z - jj - 1, n_z)

    def h_to_z(jj, p):
        here = h_all.at[part_of(through, at.tp, p), :]
        return rcopy(here, here, hz_s.at[jj, p], hz_r.at[jj, p], dev(lax.rem(at.z + jj + 1, n_z) * 2 + at.y, me))

    def h_from_z(jj, p):
        here = h_all.at[part_of(through, z_from(jj) * 2 + at.y, p), :]
        return rcopy(here, here, hz_s.at[jj, p], hz_r.at[jj, p], sibling)

    def h_to_y(zo):
        return moved(zo * 2 + at.y, hy_s.at[zo], hy_r.at[zo], y_peer)

    def h_from_y(zo):
        return moved(zo * 2 + 1 - at.y, hy_s.at[zo], hy_r.at[zo], y_peer)

    def h_to_core(tp):
        return moved(tp, hc_s.at[tp], hc_r.at[tp], sibling)

    def h_from_core(tp):
        here = h_all.at[slab(far * 2 + 1 - at.c, tp), :]
        return rcopy(here, here, hc_s.at[tp], hc_r.at[tp], sibling)

    def tok_out(k):
        to = dev(at.tp, lax.rem(me + k, n))
        return [rcopy(lab_ref, lab_in.at[me], tok_s.at[0, k], tok_r.at[0, k], to), rcopy(mask_ref, mask_in.at[me], tok_s.at[1, k], tok_r.at[1, k], to)]

    def tok_in(k):
        src = lax.rem(me + n - k, n)
        return [rcopy(lab_ref, lab_in.at[src], tok_s.at[0, k], tok_r.at[0, k], sibling), rcopy(mask_ref, mask_in.at[src], tok_s.at[1, k], tok_r.at[1, k], sibling)]

    for p in (0, 1):
        h_to_x(p).start()
    block_out().start()
    for k in range(1, n):
        for cp in tok_out(k):
            cp.start()
    lab_in[me] = lab_ref[...]
    mask_in[me] = mask_ref[...]

    def remote(k, c, row0, rows):
        dest = lax.rem(me + k, n)
        return rcopy(w_hbm.at[rows_at(dest * sz.rows + row0, rows), :], w.at[rows_at(row0, rows), cols(me, width)], w_s.at[c, k], w_r.at[c, k], dev(at.tp, dest))

    def arrival(k, c, row0, rows):
        src = lax.rem(me + n - k, n)
        return rcopy(w_hbm.at[pl.ds(0, rows), :], w.at[rows_at(row0, rows), cols(src, width)], w_s.at[c, k], w_r.at[c, k], sibling)

    def local(c, row0, rows):
        return pltpu.make_async_copy(w_hbm.at[rows_at(me * sz.rows + row0, rows), :], w.at[rows_at(row0, rows), cols(me, width)], loc.at[c])

    def issue(c):
        local(c, c * chunk, chunk).start()
        for k in range(1, n):
            remote(k, c, c * chunk, chunk).start()

    def when_not_last(dest, fn):
        if sz.short:
            pl.when(dest != n - 1)(fn)

    def issue_rem():
        local(sz.full, row_rem, sz.solid).start()
        when_not_last(me, lambda: local(sz.full + 1, row_odd, sz.short).start())
        for k in range(1, n):
            remote(k, sz.full, row_rem, sz.solid).start()
            when_not_last(lax.rem(me + k, n), lambda: remote(k, sz.full + 1, row_odd, sz.short).start())

    ahead = min(AHEAD, sz.full)
    for c in range(ahead):
        issue(c)
    if sz.short:
        @pl.when(me == n - 1)
        def _():
            w[row_odd:, :] = jnp.zeros((sz.short, d), bf16)

    sub = min(256, own)
    slices, per_own = per_f // sub, own // sub
    lane = min(128, sub)

    def place(t, i):
        near = jnp.where(t == 0, me, sib) * per_f + i * sub
        j = i // per_own
        f = jnp.where(j < n_z, through, far * 2 + 1 - at.c)
        y = jnp.where(t == 2, at.y, 1 - at.y)
        away = (f * n_tp + lax.rem(j, n_z) * 2 + y) * own + lax.rem(i, per_own) * sub
        return pl.multiple_of(jnp.where(t < 2, near, away), sub)

    def norm(t):
        def load(i):
            here = pl.ds(place(t, i), sub)
            return pltpu.make_async_copy(h_hbm.at[cols(i, sub), :] if t == 0 else h_all.at[here, :], z.at[here, :], hsem.at[i])

        def begin(i, _):
            load(i).start()
            return 0

        def one(i, _):
            load(i).wait()
            here = pl.ds(place(t, i), sub)
            h = z[here, :].astype(f32)
            inv = lax.rsqrt(jnp.mean(h * h, axis=-1, keepdims=True) + NORM_EPS)
            z[here, :] = (h * inv * gain[...].astype(f32)[None, :]).astype(bf16)
            return 0

        with scope(f'norm{t}'):
            lax.fori_loop(0, slices, begin, 0)
            lax.fori_loop(0, slices, one, 0)

    def spread_x(p):
        with scope('x_wait'):
            h_from_x(p).wait_recv()
        for jj in (2, 0, 1):
            if jj < n_z - 1:
                h_to_z(jj, p).start()

    norm(0)
    spread_x(0)
    with scope('blk_wait'):
        block_in().wait_recv()
    norm(1)
    spread_x(1)
    h_to_y(at.z).start()
    h_to_core(at.tp).start()
    with scope('tok_wait'):
        for k in range(1, n):
            for cp in tok_in(k):
                cp.wait_recv()
    count = jnp.sum(mask_in[...], axis=(0, 2), keepdims=True)[0]
    for f in range(n):
        here = pl.ds(f * per_f, per_f)
        scale[0:1, here] = mask_in[f] / count
        rel = lab_in[f] - at.tp * vocab_tp
        lab[0:1, here] = jnp.where(jnp.logical_and(rel >= 0, rel < vocab_tp), rel - me * sz.rows, -1)

    def spread_z():
        with scope('z_wait'):
            for jj in range(n_z - 1):
                for p in (0, 1):
                    h_from_z(jj, p).wait_recv()
                h_to_y(z_from(jj)).start()
                h_to_core(z_from(jj) * 2 + at.y).start()

    def spread_y():
        with scope('hy_wait'):
            for k in range(n_z):
                zo = lax.rem(at.z + n_z - k, n_z)
                h_from_y(zo).wait_recv()
                h_to_core(zo * 2 + 1 - at.y).start()

    def far_ready(y):
        with scope('core_wait'):
            for zo in range(n_z):
                h_from_core(zo * 2 + y).wait_recv()

    m[...] = jnp.full(m.shape, NEG, f32)
    s[...] = jnp.zeros(s.shape, f32)
    per_buf = tok // sub
    n_buf = slices // per_buf

    def out_copies(row0, rows, t, b):
        return [pltpu.make_async_copy(lbufs[b * n_buf + i // per_buf].at[pl.ds(0, rows), pl.ds(i % per_buf * sub, sub)],
                                      l_hbm.at[rows_at(row0, rows), pl.ds(place(t, i), sub)], lsem.at[b * n_buf + i // per_buf]) for i in range(slices)]

    def out_done(rows, b):
        for i in range(n_buf):
            pltpu.make_async_copy(lbufs[b * n_buf + i].at[pl.ds(0, rows), :], l_hbm.at[pl.ds(0, rows), pl.ds(0, tok)], lsem.at[b * n_buf + i]).wait()

    def statistics(read, rows, t0):
        group = min(4, rows // 8)
        for c1 in range(0, sub, lane):
            sl = pl.ds(pl.multiple_of(t0 + c1, lane), lane)
            big, tot = m[:, sl], s[:, sl]
            for g in range(0, rows // 8, group):
                piece = [read(r, c1) for r in range(g, min(g + group, rows // 8))]
                new = functools.reduce(jnp.maximum, piece, big)
                tot = tot * jnp.exp2(big - new)
                for x in piece:
                    tot += jnp.exp2(x - new)
                big = new
            m[:, sl], s[:, sl] = big, tot

    def slice_at(b, i):
        return lbufs[b * n_buf + i // per_buf], i % per_buf * sub

    def late_statistics(t, b):
        for i in range(slices - lag, slices):
            buf, i0 = slice_at(b, i)
            statistics(lambda r, c1: buf[8 * r:8 * r + 8, i0 + c1:i0 + c1 + lane], chunk, place(t, i))

    def logits_tile(row0, rows, t, b, masked):
        for i in range(slices):
            t0 = place(t, i)
            logits = dot_nt(w[rows_at(row0, rows), :], z[pl.ds(t0, sub), :]) * LOG2E
            if masked:
                ids = lax.broadcasted_iota(jnp.int32, (rows, sub), 0)
                logits = jnp.where(ids < jnp.where(me == n - 1, sz.solid, sz.rem), logits, NEG)
            buf, i0 = slice_at(b, i)
            buf[0:rows, i0:i0 + sub] = logits
            if masked or i < slices - lag:
                statistics(lambda r, c1: logits[8 * r:8 * r + 8, c1:c1 + lane], rows, t0)

    lag = 2
    for i in range(slices - lag, slices):
        buf, i0 = slice_at(1, i)
        buf[:, i0:i0 + sub] = jnp.full((chunk, sub), NEG, f32)

    n_a = min(3, sz.full)
    n_c = min(3, sz.full - n_a)
    k_b, k_c = 2 * n_a, 3 * n_a
    k_d = k_c + 3 * n_c
    k_e = k_d + n_a + n_c

    def item(k):
        u, v = k - k_c, k - k_e
        c = jnp.where(k < k_b, k // 2, jnp.where(k < k_c, k - k_b, jnp.where(k < k_d, n_a + u // 3, jnp.where(k < k_e, k - k_d, n_a + n_c + v // 4))))
        t = jnp.where(k < k_b, lax.rem(k, 2), jnp.where(k < k_c, 2, jnp.where(k < k_d, lax.rem(u, 3), jnp.where(k < k_e, 3, lax.rem(v, 4)))))
        return c, t

    def work(i2, _):
        for b in (0, 1):
            k = 2 * i2 + b
            c, t = item(k)

            @pl.when(t == 0)
            def _():
                with scope('w_wait'):
                    local(c, c * chunk, chunk).wait()
                    for j in range(1, n):
                        arrival(j, c, c * chunk, chunk).wait_recv()

                @pl.when(c + ahead < sz.full)
                def _():
                    issue(c + ahead)

                @pl.when(c + ahead == sz.full)
                def _():
                    issue_rem()

            @pl.when(k == k_b)
            def _():
                spread_z()
                far_ready(at.y)
                norm(2)

            @pl.when(k == max(k_d - 3, k_c))
            def _():
                spread_y()

            @pl.when(k == k_d)
            def _():
                far_ready(1 - at.y)
                norm(3)

            with scope('l_wait'):
                @pl.when(k >= 2)
                def _():
                    out_done(chunk, b)
            with scope('l_tile'):
                late_statistics(item(jnp.maximum(k - 1, 0))[1], 1 - b)
                logits_tile(c * chunk, chunk, t, b, False)
            for cp in out_copies(c * chunk, chunk, t, b):
                cp.start()
        return 0

    lax.fori_loop(0, sz.full * 2, work, 0)
    late_statistics(item(4 * sz.full - 1)[1], 1)
    with scope('w_wait_rem'):
        local(sz.full, row_rem, sz.solid).wait()
        when_not_last(me, lambda: local(sz.full + 1, row_odd, sz.short).wait())
        for k in range(1, n):
            arrival(k, sz.full, row_rem, sz.solid).wait_recv()
            when_not_last(me, lambda: arrival(k, sz.full + 1, row_odd, sz.short).wait_recv())

    def work_rem(i2, _):
        for b in (0, 1):
            @pl.when(i2 == 0)
            def _():
                out_done(chunk, b)

            @pl.when(i2 > 0)
            def _():
                out_done(sz.rem, b)
            logits_tile(row_rem, sz.rem, 2 * i2 + b, b, True)
            for cp in out_copies(row_rem, sz.rem, 2 * i2 + b, b):
                cp.start()
        return 0

    with scope('l_rem'):
        lax.fori_loop(0, 2, work_rem, 0)

    big = jnp.max(m[...], axis=0, keepdims=True)
    st_loc[0:1, :] = big
    st_loc[1:2, :] = jnp.sum(s[...] * jnp.exp2(m[...] - big), axis=0, keepdims=True)
    mine = slab(at.f, at.tp)

    def ask(k):
        tp, f = at.other(k)
        return rcopy(st_loc.at[:, slab(f, tp)], got.at[k], ssend.at[k], srecv.at[k], dev(tp, f))

    def answer(k):
        tp, f = at.other(k)
        return rcopy(res, st.at[:, mine], rsend.at[k], rrecv.at[k], dev(tp, f))

    def answered(k):
        tp, f = at.other(at.n_all - k)
        return rcopy(res, st.at[:, slab(f, tp)], rsend.at[k], rrecv.at[k], dev(tp, f))

    n_tok = tokens // tok

    def load_l(row0, rows, k, b):
        return pltpu.make_async_copy(l_hbm.at[rows_at(row0, rows), cols(k, tok)], lbufs[b].at[pl.ds(0, rows), :], lsem.at[b])

    def load_g(row0, rows, k, b):
        return pltpu.make_async_copy(g_hbm.at[rows_at(row0, rows), cols(k, tok)], gbufs[b].at[pl.ds(0, rows), :], gsem.at[b])

    def save_g(row0, rows, k, b):
        return pltpu.make_async_copy(gbufs[b].at[pl.ds(0, rows), :], g_hbm.at[rows_at(row0, rows), cols(k, tok)], gsem.at[b])

    at.every(lambda k: ask(k).start())
    got[0] = st_loc[:, mine]
    for b in (0, 1):
        out_done(sz.rem, b)
    for b in range(4):
        load_l(0, chunk, b, b).start()
    h_load = pltpu.make_async_copy(h_hbm.at[pl.ds(pl.multiple_of(at.tp * own, own), own), :], hid, hid_sem.at[0])
    h_load.start()
    acc[...] = jnp.zeros(acc.shape, f32)
    hit[...] = jnp.zeros(hit.shape, f32)
    with scope('ask_wait'):
        at.every(lambda k: ask(k).wait_recv())
    tops = got[:, 0:1, :]
    top = jnp.max(tops, axis=0)
    res[...] = top + jnp.log2(jnp.sum(got[:, 1:2, :] * jnp.exp2(tops - top[None]), axis=0))
    at.every(lambda k: answer(k).start())
    st[:, mine] = res[...]
    with scope('answer_wait'):
        at.every(lambda k: answered(k).wait_recv())
    top_row[...] = st[...] - jnp.log2(scale[...])

    def gradient(x, sl, row0):
        rows = x.shape[0]
        sc = scale[0:1, sl]
        x3 = x.reshape(rows // 8, 8, x.shape[1])
        p = jnp.exp2(x3 - top_row[0:1, sl][None])
        is_label = lax.broadcasted_iota(jnp.int32, p.shape, 0) * 8 == (lab[0:1, sl] - row0 - lax.broadcasted_iota(jnp.int32, (8, x.shape[1]), 0))[None]
        hit[...] += jnp.sum(jnp.where(is_label, x3, 0.0), axis=0) * sc
        return jnp.where(is_label, p - sc[None], p).reshape(x.shape).astype(bf16)

    step = min(256, tok)

    def grad_tile(row0, rows, k, b, fresh):
        total = None
        for c0 in range(0, tok, step):
            if fresh:
                for c1 in range(c0, c0 + step, lane):
                    gbufs[b][0:rows, c1:c1 + lane] = gradient(lbufs[b][0:rows, c1:c1 + lane], pl.ds(pl.multiple_of(k * tok + c1, lane), lane), row0)
            p = dot_nn(gbufs[b][0:rows, c0:c0 + step], z[pl.ds(pl.multiple_of(k * tok + c0, step), step), :])
            total = p if total is None else total + p
        acc[0:rows, :] += total

    def aside(c, rows):
        slot = lax.rem(c, 2)
        return pltpu.make_async_copy(stage.at[slot, pl.ds(0, rows), :], ds_hbm.at[rows_at(c * chunk, rows), :], dw_copy.at[slot])

    def keep_own(c, rows):
        slot = lax.rem(c, 2)
        return pltpu.make_async_copy(stage.at[slot, pl.ds(0, rows), cols(me, width)], dw_hbm.at[rows_at(me * sz.rows + c * chunk, rows), :], own_sem.at[slot])

    def sends(c, rows):
        out = []
        for i, f in enumerate((far * 2, far * 2 + 1, sib)):
            out.append(rcopy(ds_hbm.at[rows_at(c * chunk, rows), cols(f, width)], dw_hbm.at[rows_at(me * sz.rows + c * chunk, rows), :],
                             dw_send.at[c, i], dw_recv.at[lax.rem(f + n - me, n)], dev(at.tp, f)))
        return out

    def ship(c, rows):
        with scope('ship'):
            stage[lax.rem(c, 2), 0:rows, :] = acc[0:rows, :].astype(bf16)
            acc[...] = jnp.zeros(acc.shape, f32)
        aside(c, rows).start()
        keep_own(c, rows).start()

    def flush(c, rows):
        aside(c, rows).wait()
        keep_own(c, rows).wait()
        for cp in sends(c, rows):
            cp.start()

    def early_chunk(c, _):
        def quad(i, _):
            for b in range(4):
                k = 4 * i + b
                with scope('b1_wait'):
                    load_l(0, chunk, 0, b).wait()

                    @pl.when(jnp.logical_not(jnp.logical_and(c == 0, i == 0)))
                    def _():
                        save_g(0, chunk, 0, b).wait()
                with scope('b1_tile'):
                    grad_tile(c * chunk, chunk, k, b, True)
                save_g(c * chunk, chunk, k, b).start()
                wrap = k + 4 >= n_tok
                c2 = jnp.where(wrap, c + 1, c)

                @pl.when(c2 < early)
                def _():
                    load_l(c2 * chunk, chunk, jnp.where(wrap, k + 4 - n_tok, k + 4), b).start()

            @pl.when(jnp.logical_and(i == 0, c > 0))
            def _():
                flush(c - 1, chunk)
            return 0
        lax.fori_loop(0, n_tok // 4, quad, 0)
        ship(c, chunk)
        return 0

    lax.fori_loop(0, early, early_chunk, 0)

    half = own // ROUNDS
    groups = 2 * n_z
    last = ROUNDS * groups
    row_low = early * chunk
    low = [(j, chunk) for j in range(sz.full - early)] + [(sz.full - early, sz.rem)]
    per_l = tok // half

    def group_of(q):
        r, g = q // groups, lax.rem(q, groups)
        xi, jj = g // n_z, lax.rem(g, n_z)
        return r, xi, jj, jnp.where(xi == 0, far, at.x), lax.rem(at.z + jj + 1, n_z)

    def pieces(q, b):
        r, _, _, xb, zb = group_of(q)
        cb = at.c if b == 1 else 1 - at.c
        return [pl.multiple_of((xb * 2 + cb) * per_f + (zb * 2 + yb) * own + r * half, half) for yb in (1 - at.y, at.y)]

    def l_part(b, j, i, rows):
        p = 2 * j + i
        return lbufs[2 * b + p // per_l].at[pl.ds(0, rows), pl.ds(p % per_l * half, half)]

    def block_loads(q, b):
        out = []
        for i, t0 in enumerate(pieces(q, b)):
            out.append(pltpu.make_async_copy(g_hbm.at[pl.ds(0, row_low), pl.ds(t0, half)], qbufs[b].at[pl.ds(0, row_low), pl.ds(i * half, half)], qsem.at[b, i]))
            for j, rows in low:
                out.append(pltpu.make_async_copy(l_hbm.at[pl.ds(row_low + j * chunk, rows), pl.ds(t0, half)], l_part(b, j, i, rows), bsem.at[b, 2 * j + i]))
        return out

    def block_saves(q, b):
        return [pltpu.make_async_copy(qbufs[b].at[pl.ds(row_low, sz.rows - row_low), pl.ds(i * half, half)],
                                      g_hbm.at[pl.ds(row_low, sz.rows - row_low), pl.ds(t0, half)], vsem.at[b, i]) for i, t0 in enumerate(pieces(q, b))]

    def block_dot(q, b):
        for i, t0 in enumerate(pieces(q, b)):
            for j, rows in low:
                row0 = row_low + j * chunk
                qbufs[b][row0:row0 + rows, i * half:(i + 1) * half] = gradient(l_part(b, j, i, rows)[...], pl.ds(t0, half), row0)
        return dot_tn(qbufs[b][...], w[...])

    def to_sib(q):
        slot = lax.rem(q, 2)
        return rcopy(sib_out.at[slot], sib_in.at[slot], sib_s.at[slot], sib_r.at[slot], sibling)

    def to_y(q):
        slot, land = lax.rem(q, 2), lax.rem(q, y_in.shape[0])
        return rcopy(y_out.at[slot], y_in.at[land], y_s.at[slot], y_r.at[land], y_peer)

    def to_z(q):
        r, xi, jj, _, zb = group_of(q)
        return rcopy(z_out.at[jj], z_in.at[r, xi, jj], zz_s.at[jj], zz_r.at[r, xi, jj], dev(zb * 2 + at.y, me))

    def to_x(r):
        return rcopy(x_out, x_in.at[r], x_s.at[0], x_r.at[r], x_peer)

    def z_stage(q):
        _, xi, jj, _, _ = group_of(q)
        with scope('y_wait'):
            to_y(q).wait_recv()
        val = part[lax.rem(q, part.shape[0])] + y_in[lax.rem(q, y_in.shape[0])].astype(f32)

        @pl.when(jj == n_z - 1)
        def _():
            z_own[xi] = val

        @pl.when(jj < n_z - 1)
        def _():
            @pl.when(q >= n_z)
            def _():
                to_z(q - n_z).wait_send()
            z_out[jj] = val.astype(bf16)
            to_z(q).start()

    def z_sum(r, xi):
        val = z_own[xi]
        for jj in range(n_z - 1):
            rcopy(z_out.at[0], z_in.at[r, xi, jj], zz_s.at[jj], zz_r.at[r, xi, jj], sibling).wait_recv()
            val = val + z_in[r, xi, jj].astype(f32)
        return val

    def x_stage(r):
        @pl.when(r > 0)
        def _():
            to_x(0).wait_send()
        with scope('x_stage'):
            x_out[...] = z_sum(r, 0).astype(bf16)
        to_x(r).start()

    def home(tp, r):
        return gh_hbm.at[pl.ds(pl.multiple_of(tp * own + r * half, half), half), :]

    def gathers(r):
        out = [rcopy(gh.at[r], home(at.tp, r), ag_s.at[r, n_z - 1], fw_r.at[r, at.z], y_peer)]
        for jj in range(n_z - 1):
            to = lax.rem(at.z + jj + 1, n_z)
            out.append(rcopy(gh.at[r], home(at.tp, r), ag_s.at[r, jj], ag_r.at[r, jj], dev(to * 2 + at.y, me)))
        return out

    def keep(r):
        return pltpu.make_async_copy(gh.at[r], home(at.tp, r), gh_sem.at[r])

    def arrived(r, jj):
        return rcopy(gh.at[r], home(z_from(jj) * 2 + at.y, r), ag_s.at[r, jj], ag_r.at[r, jj], sibling)

    def onward(r, jj):
        here = home(z_from(jj) * 2 + at.y, r)
        return rcopy(here, here, fw_s.at[r, jj], fw_r.at[r, z_from(jj)], y_peer)

    def tell_gain(k):
        tp, f = at.other(k)
        return rcopy(gg, gg_in.at[at.index], gain_s.at[k], gain_r.at[k], dev(tp, f))

    def heard_gain(k):
        i = lax.rem(at.index + at.n_all - k, at.n_all)
        return rcopy(gg, gg_in.at[i], gain_s.at[k], gain_r.at[k], sibling)

    def final(r):
        with scope('final_wait'):
            to_x(r).wait_recv()
            dz = z_sum(r, 1) + x_in[r].astype(f32)
        h = hid[pl.ds(pl.multiple_of(r * half, half), half), :].astype(f32)
        inv = lax.rsqrt(jnp.mean(h * h, axis=-1, keepdims=True) + NORM_EPS)
        normed = h * inv
        a = dz * gain[...].astype(f32)[None, :]
        gh[r] = (inv * (a - normed * jnp.mean(a * normed, axis=-1, keepdims=True))).astype(bf16)
        gg[0:1, 0:d] += jnp.sum(dz * normed, axis=0, keepdims=True)
        if r == 1:
            hits = jnp.sum(jnp.sum(hit[...], axis=0, keepdims=True), axis=1, keepdims=True)
            gg[0:1, d:] = jnp.broadcast_to(hits, (1, gg.shape[1] - d))
            at.every(lambda k: tell_gain(k).start())
            gg_in[at.index] = gg[...]
        keep(r).start()
        if r == 1:
            gather_start(1)

    def gather_start(r):
        for cp in gathers(r):
            cp.start()

    def forward(r, jj):
        with scope('fw_wait'):
            arrived(r, jj).wait_recv()
        onward(r, jj).start()

    for b in range(4):
        save_g(0, chunk, 0, b).wait()
    h_load.wait()
    gg[...] = jnp.zeros(gg.shape, f32)
    for b in (0, 1):
        for cp in block_loads(0, b):
            cp.start()

    def dz_group(q, _):
        for b in (0, 1):
            with scope('a_wait'):
                for cp in block_loads(q, b):
                    cp.wait()

                @pl.when(q > 0)
                def _():
                    for cp in block_saves(q - 1, b):
                        cp.wait()
            slot = lax.rem(q, 2)
            if b == 0:
                @pl.when(q >= 2)
                def _():
                    to_sib(q - 2).wait_send()
                with scope('a_dot0'):
                    sib_out[slot] = block_dot(q, b).astype(bf16)
                to_sib(q).start()
            else:
                @pl.when(q >= 2)
                def _():
                    to_y(q - 2).wait_send()
                with scope('a_dot1'):
                    val = block_dot(q, b)
                    y_sum[...] = val[0:half]
                    part[lax.rem(q, part.shape[0])] = val[half:]
                with scope('sib_wait'):
                    to_sib(q).wait_recv()
                y_out[slot] = (y_sum[...] + sib_in[slot, 0:half].astype(f32)).astype(bf16)
                part[lax.rem(q, part.shape[0])] += sib_in[slot, half:].astype(f32)
                to_y(q).start()
            for cp in block_saves(q, b):
                cp.start()

            @pl.when(q + 1 < last)
            def _():
                for cp in block_loads(q + 1, b):
                    cp.start()

        @pl.when(q == 0)
        def _():
            flush(early - 1, chunk)

        @pl.when(q >= 2)
        def _():
            z_stage(q - 2)

        @pl.when(q == n_z + 3)
        def _():
            x_stage(0)

        @pl.when(q == max(last - 6, n_z + 4))
        def _():
            final(0)
        return 0

    lax.fori_loop(0, last, dz_group, 0)
    z_stage(last - 2)
    gather_start(0)
    for b in (0, 1):
        for cp in block_saves(last - 1, b):
            cp.wait()

    for b in range(4):
        load_g(early * chunk, chunk, b, b).start()

    quads = n_tok // 4
    nearest = [jj for jj in (2, 0, 1) if jj < n_z - 1]
    steps = [(3 + 3 * r + t, r, jj) for r in range(ROUNDS) for t, jj in enumerate(nearest)]

    def late_chunk(c, _):
        def quad(i, _):
            for b in range(4):
                k = 4 * i + b
                with scope('b2_wait'):
                    load_g(0, chunk, 0, b).wait()
                with scope('b2_tile'):
                    grad_tile(c * chunk, chunk, k, b, False)
                wrap = k + 4 >= n_tok
                c2, k2 = jnp.where(wrap, c + 1, c), jnp.where(wrap, k + 4 - n_tok, k + 4)

                @pl.when(c2 < sz.full)
                def _():
                    load_g(c2 * chunk, chunk, k2, b).start()

                @pl.when(c2 == sz.full)
                def _():
                    load_g(row_rem, sz.rem, k2, b).start()
                if b == 0:
                    @pl.when(jnp.logical_and(i == 0, c > early))
                    def _():
                        flush(c - 1, chunk)

            for t, r, jj in steps:
                @pl.when((c - early) * quads + i == t)
                def _():
                    forward(r, jj)
            return 0
        lax.fori_loop(0, quads, quad, 0)
        ship(c, chunk)

        @pl.when(c == early)
        def _():
            z_stage(last - 1)
            x_stage(1)

        @pl.when(c == early + 1)
        def _():
            final(1)
        return 0

    lax.fori_loop(early, sz.full, late_chunk, 0)
    def late_rem(i, _):
        for b in range(4):
            with scope('b2_wait'):
                load_g(row_rem, sz.rem, 0, b).wait()
            with scope('b2_rem'):
                grad_tile(row_rem, sz.rem, 4 * i + b, b, False)

            @pl.when(4 * i + b + 4 < n_tok)
            def _():
                load_g(row_rem, sz.rem, 4 * i + b + 4, b).start()
            if b == 0:
                @pl.when(i == 0)
                def _():
                    flush(sz.full - 1, chunk)
        return 0

    lax.fori_loop(0, n_tok // 4, late_rem, 0)
    ship(sz.full, sz.rem)
    flush(sz.full, sz.rem)
    for t, r, jj in steps:
        if t >= (sz.full - early) * quads:
            forward(r, jj)

    with scope('t_gain'):
        at.every(lambda k: heard_gain(k).wait_recv())
    total = jnp.sum(gg_in[...], axis=0)
    gg_out[0:1, 0:d] = total[0:1, 0:d]
    gg_out[0:1, d:] = (jnp.sum(st[...] * scale[...], axis=1, keepdims=True) - total[0:1, d:]) * (1.0 / LOG2E)
    with scope('t_small'):
        at.every(lambda k: ask(k).wait_send())
        at.every(lambda k: answer(k).wait_send())
        at.every(lambda k: tell_gain(k).wait_send())
        for k in range(1, n):
            for cp in tok_out(k):
                cp.wait_send()
        block_out().wait_send()
        for p in (0, 1):
            h_to_x(p).wait_send()
            for jj in range(n_z - 1):
                h_to_z(jj, p).wait_send()
        for zo in range(n_z):
            h_to_y(zo).wait_send()
        for tp in range(n_tp):
            h_to_core(tp).wait_send()

        def w_sent(c, _):
            for k in range(1, n):
                remote(k, c, c * chunk, chunk).wait_send()
            return 0

        lax.fori_loop(0, sz.full, w_sent, 0)
        for k in range(1, n):
            remote(k, sz.full, row_rem, sz.solid).wait_send()
            when_not_last(lax.rem(me + k, n), lambda: remote(k, sz.full + 1, row_odd, sz.short).wait_send())
        for q in (last - 2, last - 1):
            to_sib(q).wait_send()
            to_y(q).wait_send()
        for q in range(last - n_z, last - 1):
            to_z(q).wait_send()
        to_x(1).wait_send()
    with scope('t_send'):
        def sent(c, _):
            for cp in sends(c, chunk):
                cp.wait_send()
            return 0
        lax.fori_loop(0, sz.full, sent, 0)
        for cp in sends(sz.full, sz.rem):
            cp.wait_send()
    for r in range(ROUNDS):
        with scope(f't_gather{r}'):
            keep(r).wait()
            for cp in gathers(r):
                cp.wait_send()
            for jj in range(n_z - 1):
                onward(r, jj).wait_send()
            for zo in range(n_z):
                rcopy(gh.at[r], home(zo * 2 + 1 - at.y, r), ag_s.at[r, 0], fw_r.at[r, zo], y_peer).wait_recv()
    with scope('t_dw'):
        for k in range(1, n):
            src = lax.rem(me + n - k, n)
            rcopy(dw_hbm.at[pl.ds(0, sz.rows), :], dw_hbm.at[rows_at(src * sz.rows, sz.rows), :], dw_send.at[0, 0], dw_recv.at[k], sibling).wait_recv()


HBM = pl.BlockSpec(memory_space=pl.ANY)
VM = pl.BlockSpec(memory_space=pltpu.VMEM)
DMA = pltpu.SemaphoreType.DMA


def solution(mesh, chunk=CHUNK, tok=TOK, early=EARLY):
    n_fsdp, n_tp = mesh.shape['fsdp'], mesh.shape['tp']
    n_all, n_z = n_fsdp * n_tp, n_tp // 2
    S, V = jax.ShapeDtypeStruct, pltpu.VMEM
    i32 = jnp.int32

    def per_device(hidden, labels, tok_mask, norm_gain, w_rows):
        per_f, d = hidden.shape
        width, vocab_tp = w_rows.shape
        tokens, own = per_f * n_fsdp, per_f // n_tp
        half = own // ROUNDS
        sz = Sizes(vocab_tp, n_fsdp, chunk)
        n_low = sz.full - early + 1

        dw_t, grad_hidden, sums, *_ = pl.pallas_call(
            functools.partial(head_kernel, sz, n_tp, vocab_tp, chunk, tok, early),
            out_shape=(S((n_fsdp * sz.rows, width), bf16), S(hidden.shape, bf16), S((1, d + 128), f32),
                       S((sz.rows, tokens), f32), S((sz.rows, tokens), bf16), S((tokens, d), bf16), S(((sz.full + 1) * chunk, d), bf16)),
            in_specs=[HBM, VM, VM, VM, HBM], out_specs=(HBM, HBM, VM, HBM, HBM, HBM, HBM),
            scratch_shapes=[
                V((tokens, d), bf16), V((sz.rows, d), bf16), *[V((chunk, tok), f32)] * 4, *[V((chunk, tok), bf16)] * 4, *[V((sz.rows, 2 * half), bf16)] * 2,
                V((8, tokens), f32), V((8, tokens), f32), V((1, tokens), f32), V((1, tokens), i32), V((n_fsdp, 1, per_f), i32), V((n_fsdp, 1, per_f), f32),
                V((2, tokens), f32), V((n_all, 2, own), f32), V((1, own), f32), V((1, tokens), f32), V((1, tokens), f32), V((8, min(128, half)), f32), V((own, d), bf16),
                V((chunk, d), f32), V((2, chunk, d), bf16), V((2, 2 * half, d), bf16), V((2, 2 * half, d), bf16), V((half, d), f32),
                V((2, half, d), bf16), V((6, half, d), bf16), V((3, half, d), f32), V((n_z - 1, half, d), bf16), V((ROUNDS, 2, n_z - 1, half, d), bf16), V((2, half, d), f32),
                V((half, d), bf16), V((ROUNDS, half, d), bf16), V((ROUNDS, half, d), bf16), V((1, d + 128), f32), V((n_all, 1, d + 128), f32),
                DMA((sz.full + 2, n_fsdp)), DMA((sz.full + 2, n_fsdp)), DMA((sz.full + 2,)), DMA((per_f // min(256, own),)), DMA((4,)), DMA((4,)), DMA((2, 2)), DMA((2, 2 * n_low)), DMA((2, 2)),
                DMA((n_all,)), DMA((n_all,)), DMA((n_all,)), DMA((n_all,)), DMA((2, n_fsdp)), DMA((2, n_fsdp)), DMA((2,)), DMA((2,)), DMA((2,)),
                DMA((n_z - 1, 2)), DMA((n_z - 1, 2)), DMA((n_z,)), DMA((n_z,)), DMA((n_tp,)), DMA((n_tp,)),
                DMA((1,)), DMA((2,)), DMA((sz.full + 1, 3)), DMA((n_fsdp,)), DMA((2,)), DMA((2,)), DMA((2,)), DMA((2,)), DMA((8,)),
                DMA((n_z - 1,)), DMA((ROUNDS, 2, n_z - 1)), DMA((1,)), DMA((ROUNDS,)),
                DMA((ROUNDS, n_z)), DMA((ROUNDS, n_z)), DMA((ROUNDS, n_z)), DMA((ROUNDS, n_z)), DMA((ROUNDS,)), DMA((n_all,)), DMA((n_all,))],
            compiler_params=pltpu.CompilerParams(vmem_limit_bytes=VMEM_LIMIT, collective_id=0, has_side_effects=True), name='head',
        )(hidden, labels[None, :], tok_mask[None, :], norm_gain, w_rows.T)
        return sums[0, d], grad_hidden, dw_t[:vocab_tp].T, sums[0, :d]

    return jax.shard_map(per_device, mesh=mesh, in_specs=(P('fsdp', None), P('fsdp'), P('fsdp'), P(), P('fsdp', 'tp')), out_specs=(P(), P('fsdp', None), P('fsdp', 'tp'), P()), check_vma=False)
```

```python
import functools

import jax
import jax.numpy as jnp
from jax import lax
from jax.experimental import pallas as pl
from jax.experimental.pallas import tpu as pltpu
from jax.sharding import PartitionSpec as P

NORM_EPS = 1e-6
LOG2E = 1.4426950408889634
NEG = -1e30
CHUNK = 512
TOK = 1024
EARLY = (2, 5)
AHEAD = 5
ROUNDS = 2
VMEM_LIMIT = 67_043_328
MESH = pl.DeviceIdType.MESH
scope = jax.named_scope
f32, bf16 = jnp.float32, jnp.bfloat16


def dot_nt(a, b):
    return lax.dot_general(a, b, (((1,), (1,)), ((), ())), preferred_element_type=f32)


def dot_tn(a, b):
    return lax.dot_general(a, b, (((0,), (0,)), ((), ())), preferred_element_type=f32)


def dot_nn(a, b):
    return lax.dot_general(a, b, (((1,), (0,)), ((), ())), preferred_element_type=f32)


def cols(k, size):
    return pl.ds(pl.multiple_of(k * size, size), size)


def rows_at(row0, rows):
    return pl.ds(pl.multiple_of(row0, 16), rows)


class Sizes:
    def __init__(self, vocab_tp, n_fsdp, chunk):
        self.n = n_fsdp
        self.rows = -(-vocab_tp // (n_fsdp * 16)) * 16
        self.short = n_fsdp * self.rows - vocab_tp
        self.full = self.rows // chunk
        self.rem = self.rows - self.full * chunk
        self.solid = self.rem - self.short
        assert self.rem > self.short and self.rem % 16 == 0 and self.short % 16 == 0


class Place:
    def __init__(self, n_fsdp, n_tp):
        self.n_fsdp, self.n_tp, self.n_all = n_fsdp, n_tp, n_fsdp * n_tp
        self.f, self.tp = lax.axis_index('fsdp'), lax.axis_index('tp')
        self.x, self.c = self.f // 2, lax.rem(self.f, 2)
        self.n_z = n_tp // 2
        self.z, self.y = self.tp // 2, lax.rem(self.tp, 2)
        self.index = self.tp * n_fsdp + self.f

    def other(self, k):
        i = lax.rem(self.index + k, self.n_all)
        return i // self.n_fsdp, lax.rem(i, self.n_fsdp)

    def every(self, fn):
        def go(k, _):
            fn(k)
            return 0
        lax.fori_loop(1, self.n_all, go, 0)


def dev(tp, f):
    return {'tp': tp, 'fsdp': f}


def rcopy(src, dst, ssem, rsem, to):
    return pltpu.make_async_remote_copy(src_ref=src, dst_ref=dst, send_sem=ssem, recv_sem=rsem, device_id=to, device_id_type=MESH)


def enter(at):
    barrier = pltpu.get_barrier_semaphore()

    def tell(k):
        tp, f = at.other(k)
        pl.semaphore_signal(barrier, inc=1, device_id=dev(tp, f), device_id_type=MESH)

    at.every(tell)
    pl.semaphore_wait(barrier, at.n_all - 1)


def head_kernel(sz, n_tp, vocab_tp, chunk, tok, early,
                h_hbm, lab_ref, mask_ref, gain, w_hbm,
                dw_hbm, gh_hbm, gg_out, l_hbm, g_hbm, h_all, ds_hbm,
                z, w, l0, l1, l2, l3, g0, g1, g2, g3, q0, q1, m, s, scale, lab, lab_in, mask_in, st_loc, got, res, st, top_row, hit, hid,
                acc, stage, sib_out, sib_in, y_sum, y_out, y_in, part, z_out, z_in, z_own, x_out, x_in, gh, gg, gg_in,
                w_s, w_r, loc, hsem, lsem, gsem, qsem, bsem, vsem, ssend, srecv, rsend, rrecv, tok_s, tok_r, blk, hx_s, hx_r, hz_s, hz_r, hy_s, hy_r, hc_s, hc_r,
                hid_sem, dw_copy, dw_send, dw_recv, own_sem, sib_s, sib_r, y_s, y_r, zz_s, zz_r, x_s, x_r, ag_s, ag_r, fw_s, fw_r, gh_sem, gain_s, gain_r):
    at = Place(sz.n, n_tp)
    me, n, n_z, width = at.f, sz.n, at.n_z, w_hbm.shape[1]
    per_f, d = h_hbm.shape
    tokens, own = per_f * n, per_f // n_tp
    lbufs, gbufs, qbufs = (l0, l1, l2, l3), (g0, g1, g2, g3), (q0, q1)
    far, sib = 1 - at.x, at.x * 2 + 1 - at.c
    through = far * 2 + at.c
    sibling, y_peer, x_peer = dev(at.tp, sib), dev(at.z * 2 + 1 - at.y, me), dev(at.tp, through)
    row_rem = sz.full * chunk
    row_odd = row_rem + sz.solid

    with scope('enter'):
        enter(at)

    def slab(f, tp):
        return pl.ds(pl.multiple_of((f * n_tp + tp) * own, own), own)

    def block(f):
        return pl.ds(pl.multiple_of(f * per_f, per_f), per_f)

    own2 = own // 2

    def part_of(f, tp, p):
        return pl.ds(pl.multiple_of((f * n_tp + tp) * own + p * own2, own2), own2)

    def h_to_x(p):
        return rcopy(h_hbm.at[pl.ds(pl.multiple_of(at.tp * own + p * own2, own2), own2), :], h_all.at[part_of(me, at.tp, p), :], hx_s.at[p], hx_r.at[p], x_peer)

    def h_from_x(p):
        here = h_all.at[part_of(through, at.tp, p), :]
        return rcopy(here, here, hx_s.at[p], hx_r.at[p], x_peer)

    def block_out():
        return rcopy(h_hbm, h_all.at[block(me), :], blk.at[0], blk.at[1], sibling)

    def block_in():
        return rcopy(h_hbm, h_all.at[block(sib), :], blk.at[0], blk.at[1], sibling)

    def moved(tp, ssem, rsem, to):
        here = h_all.at[slab(through, tp), :]
        return rcopy(here, here, ssem, rsem, to)

    def z_from(jj):
        return lax.rem(at.z + n_z - jj - 1, n_z)

    def h_to_z(jj, p):
        here = h_all.at[part_of(through, at.tp, p), :]
        return rcopy(here, here, hz_s.at[jj, p], hz_r.at[jj, p], dev(lax.rem(at.z + jj + 1, n_z) * 2 + at.y, me))

    def h_from_z(jj, p):
        here = h_all.at[part_of(through, z_from(jj) * 2 + at.y, p), :]
        return rcopy(here, here, hz_s.at[jj, p], hz_r.at[jj, p], sibling)

    def h_to_y(zo):
        return moved(zo * 2 + at.y, hy_s.at[zo], hy_r.at[zo], y_peer)

    def h_from_y(zo):
        return moved(zo * 2 + 1 - at.y, hy_s.at[zo], hy_r.at[zo], y_peer)

    def h_to_core(tp):
        return moved(tp, hc_s.at[tp], hc_r.at[tp], sibling)

    def h_from_core(tp):
        here = h_all.at[slab(far * 2 + 1 - at.c, tp), :]
        return rcopy(here, here, hc_s.at[tp], hc_r.at[tp], sibling)

    def tok_out(k):
        to = dev(at.tp, lax.rem(me + k, n))
        return [rcopy(lab_ref, lab_in.at[me], tok_s.at[0, k], tok_r.at[0, k], to), rcopy(mask_ref, mask_in.at[me], tok_s.at[1, k], tok_r.at[1, k], to)]

    def tok_in(k):
        src = lax.rem(me + n - k, n)
        return [rcopy(lab_ref, lab_in.at[src], tok_s.at[0, k], tok_r.at[0, k], sibling), rcopy(mask_ref, mask_in.at[src], tok_s.at[1, k], tok_r.at[1, k], sibling)]

    for p in (0, 1):
        h_to_x(p).start()
    block_out().start()
    for k in range(1, n):
        for cp in tok_out(k):
            cp.start()
    lab_in[me] = lab_ref[...]
    mask_in[me] = mask_ref[...]

    def remote(k, c, row0, rows):
        dest = lax.rem(me + k, n)
        return rcopy(w_hbm.at[rows_at(dest * sz.rows + row0, rows), :], w.at[rows_at(row0, rows), cols(me, width)], w_s.at[c, k], w_r.at[c, k], dev(at.tp, dest))

    def arrival(k, c, row0, rows):
        src = lax.rem(me + n - k, n)
        return rcopy(w_hbm.at[pl.ds(0, rows), :], w.at[rows_at(row0, rows), cols(src, width)], w_s.at[c, k], w_r.at[c, k], sibling)

    def local(c, row0, rows):
        return pltpu.make_async_copy(w_hbm.at[rows_at(me * sz.rows + row0, rows), :], w.at[rows_at(row0, rows), cols(me, width)], loc.at[c])

    def issue(c):
        local(c, c * chunk, chunk).start()
        for k in range(1, n):
            remote(k, c, c * chunk, chunk).start()

    def when_not_last(dest, fn):
        if sz.short:
            pl.when(dest != n - 1)(fn)

    def issue_rem():
        local(sz.full, row_rem, sz.solid).start()
        when_not_last(me, lambda: local(sz.full + 1, row_odd, sz.short).start())
        for k in range(1, n):
            remote(k, sz.full, row_rem, sz.solid).start()
            when_not_last(lax.rem(me + k, n), lambda: remote(k, sz.full + 1, row_odd, sz.short).start())

    ahead = min(AHEAD, sz.full)
    for c in range(ahead):
        issue(c)
    if sz.short:
        @pl.when(me == n - 1)
        def _():
            w[row_odd:, :] = jnp.zeros((sz.short, d), bf16)

    sub = min(256, own)
    slices, per_own = per_f // sub, own // sub
    lane = min(128, sub)

    def place(t, i):
        near = jnp.where(t == 0, me, sib) * per_f + i * sub
        j = i // per_own
        f = jnp.where(j < n_z, through, far * 2 + 1 - at.c)
        y = jnp.where(t == 2, at.y, 1 - at.y)
        away = (f * n_tp + lax.rem(j, n_z) * 2 + y) * own + lax.rem(i, per_own) * sub
        return pl.multiple_of(jnp.where(t < 2, near, away), sub)

    def norm(t):
        def load(i):
            here = pl.ds(place(t, i), sub)
            return pltpu.make_async_copy(h_hbm.at[cols(i, sub), :] if t == 0 else h_all.at[here, :], z.at[here, :], hsem.at[i])

        def begin(i, _):
            load(i).start()
            return 0

        def one(i, _):
            load(i).wait()
            here = pl.ds(place(t, i), sub)
            h = z[here, :].astype(f32)
            inv = lax.rsqrt(jnp.mean(h * h, axis=-1, keepdims=True) + NORM_EPS)
            z[here, :] = (h * inv * gain[...].astype(f32)[None, :]).astype(bf16)
            return 0

        with scope(f'norm{t}'):
            lax.fori_loop(0, slices, begin, 0)
            lax.fori_loop(0, slices, one, 0)

    def spread_x(p):
        with scope('x_wait'):
            h_from_x(p).wait_recv()
        for jj in (2, 0, 1):
            if jj < n_z - 1:
                h_to_z(jj, p).start()

    norm(0)
    spread_x(0)
    with scope('blk_wait'):
        block_in().wait_recv()
    norm(1)
    spread_x(1)
    h_to_y(at.z).start()
    h_to_core(at.tp).start()
    with scope('tok_wait'):
        for k in range(1, n):
            for cp in tok_in(k):
                cp.wait_recv()
    count = jnp.sum(mask_in[...], axis=(0, 2), keepdims=True)[0]
    for f in range(n):
        here = pl.ds(f * per_f, per_f)
        scale[0:1, here] = mask_in[f] / count
        rel = lab_in[f] - at.tp * vocab_tp
        lab[0:1, here] = jnp.where(jnp.logical_and(rel >= 0, rel < vocab_tp), rel - me * sz.rows, -1)

    def spread_z():
        with scope('z_wait'):
            for jj in range(n_z - 1):
                for p in (0, 1):
                    h_from_z(jj, p).wait_recv()
                h_to_y(z_from(jj)).start()
                h_to_core(z_from(jj) * 2 + at.y).start()

    def spread_y():
        with scope('hy_wait'):
            for k in range(n_z):
                zo = lax.rem(at.z + n_z - k, n_z)
                h_from_y(zo).wait_recv()
                h_to_core(zo * 2 + 1 - at.y).start()

    def far_ready(y):
        with scope('core_wait'):
            for zo in range(n_z):
                h_from_core(zo * 2 + y).wait_recv()

    m[...] = jnp.full(m.shape, NEG, f32)
    s[...] = jnp.zeros(s.shape, f32)
    per_buf = tok // sub
    n_buf = slices // per_buf

    def out_copies(row0, rows, t, b):
        return [pltpu.make_async_copy(lbufs[b * n_buf + i // per_buf].at[pl.ds(0, rows), pl.ds(i % per_buf * sub, sub)],
                                      l_hbm.at[rows_at(row0, rows), pl.ds(place(t, i), sub)], lsem.at[b * n_buf + i // per_buf]) for i in range(slices)]

    def out_done(rows, b):
        for i in range(n_buf):
            pltpu.make_async_copy(lbufs[b * n_buf + i].at[pl.ds(0, rows), :], l_hbm.at[pl.ds(0, rows), pl.ds(0, tok)], lsem.at[b * n_buf + i]).wait()

    def statistics(read, rows, t0):
        group = min(4, rows // 8)
        for c1 in range(0, sub, lane):
            sl = pl.ds(pl.multiple_of(t0 + c1, lane), lane)
            big, tot = m[:, sl], s[:, sl]
            for g in range(0, rows // 8, group):
                piece = [read(r, c1) for r in range(g, min(g + group, rows // 8))]
                new = functools.reduce(jnp.maximum, piece, big)
                tot = tot * jnp.exp2(big - new)
                for x in piece:
                    tot += jnp.exp2(x - new)
                big = new
            m[:, sl], s[:, sl] = big, tot

    def slice_at(b, i):
        return lbufs[b * n_buf + i // per_buf], i % per_buf * sub

    def late_statistics(t, b):
        for i in range(slices - lag, slices):
            buf, i0 = slice_at(b, i)
            statistics(lambda r, c1: buf[8 * r:8 * r + 8, i0 + c1:i0 + c1 + lane], chunk, place(t, i))

    def logits_tile(row0, rows, t, b, masked):
        for i in range(slices):
            t0 = place(t, i)
            logits = dot_nt(w[rows_at(row0, rows), :], z[pl.ds(t0, sub), :]) * LOG2E
            if masked:
                ids = lax.broadcasted_iota(jnp.int32, (rows, sub), 0)
                logits = jnp.where(ids < jnp.where(me == n - 1, sz.solid, sz.rem), logits, NEG)
            buf, i0 = slice_at(b, i)
            buf[0:rows, i0:i0 + sub] = logits
            if masked or i < slices - lag:
                statistics(lambda r, c1: logits[8 * r:8 * r + 8, c1:c1 + lane], rows, t0)

    lag = 2
    for i in range(slices - lag, slices):
        buf, i0 = slice_at(1, i)
        buf[:, i0:i0 + sub] = jnp.full((chunk, sub), NEG, f32)

    n_a = min(3, sz.full)
    n_c = min(3, sz.full - n_a)
    k_b, k_c = 2 * n_a, 3 * n_a
    k_d = k_c + 3 * n_c
    k_e = k_d + n_a + n_c

    def item(k):
        u, v = k - k_c, k - k_e
        c = jnp.where(k < k_b, k // 2, jnp.where(k < k_c, k - k_b, jnp.where(k < k_d, n_a + u // 3, jnp.where(k < k_e, k - k_d, n_a + n_c + v // 4))))
        t = jnp.where(k < k_b, lax.rem(k, 2), jnp.where(k < k_c, 2, jnp.where(k < k_d, lax.rem(u, 3), jnp.where(k < k_e, 3, lax.rem(v, 4)))))
        return c, t

    def work(i2, _):
        for b in (0, 1):
            k = 2 * i2 + b
            c, t = item(k)

            @pl.when(t == 0)
            def _():
                with scope('w_wait'):
                    local(c, c * chunk, chunk).wait()
                    for j in range(1, n):
                        arrival(j, c, c * chunk, chunk).wait_recv()

                @pl.when(c + ahead < sz.full)
                def _():
                    issue(c + ahead)

                @pl.when(c + ahead == sz.full)
                def _():
                    issue_rem()

            @pl.when(k == k_b)
            def _():
                spread_z()
                far_ready(at.y)
                norm(2)

            @pl.when(k == max(k_d - 3, k_c))
            def _():
                spread_y()

            @pl.when(k == k_d)
            def _():
                far_ready(1 - at.y)
                norm(3)

            with scope('l_wait'):
                @pl.when(k >= 2)
                def _():
                    out_done(chunk, b)
            with scope('l_tile'):
                late_statistics(item(jnp.maximum(k - 1, 0))[1], 1 - b)
                logits_tile(c * chunk, chunk, t, b, False)
            for cp in out_copies(c * chunk, chunk, t, b):
                cp.start()
        return 0

    lax.fori_loop(0, sz.full * 2, work, 0)
    late_statistics(item(4 * sz.full - 1)[1], 1)
    with scope('w_wait_rem'):
        local(sz.full, row_rem, sz.solid).wait()
        when_not_last(me, lambda: local(sz.full + 1, row_odd, sz.short).wait())
        for k in range(1, n):
            arrival(k, sz.full, row_rem, sz.solid).wait_recv()
            when_not_last(me, lambda: arrival(k, sz.full + 1, row_odd, sz.short).wait_recv())

    def work_rem(i2, _):
        for b in (0, 1):
            @pl.when(i2 == 0)
            def _():
                out_done(chunk, b)

            @pl.when(i2 > 0)
            def _():
                out_done(sz.rem, b)
            logits_tile(row_rem, sz.rem, 2 * i2 + b, b, True)
            for cp in out_copies(row_rem, sz.rem, 2 * i2 + b, b):
                cp.start()
        return 0

    with scope('l_rem'):
        lax.fori_loop(0, 2, work_rem, 0)

    big = jnp.max(m[...], axis=0, keepdims=True)
    st_loc[0:1, :] = big
    st_loc[1:2, :] = jnp.sum(s[...] * jnp.exp2(m[...] - big), axis=0, keepdims=True)
    mine = slab(at.f, at.tp)

    def ask(k):
        tp, f = at.other(k)
        return rcopy(st_loc.at[:, slab(f, tp)], got.at[k], ssend.at[k], srecv.at[k], dev(tp, f))

    def answer(k):
        tp, f = at.other(k)
        return rcopy(res, st.at[:, mine], rsend.at[k], rrecv.at[k], dev(tp, f))

    def answered(k):
        tp, f = at.other(at.n_all - k)
        return rcopy(res, st.at[:, slab(f, tp)], rsend.at[k], rrecv.at[k], dev(tp, f))

    n_tok = tokens // tok

    def load_l(row0, rows, k, b):
        return pltpu.make_async_copy(l_hbm.at[rows_at(row0, rows), cols(k, tok)], lbufs[b].at[pl.ds(0, rows), :], lsem.at[b])

    def load_g(row0, rows, k, b):
        return pltpu.make_async_copy(g_hbm.at[rows_at(row0, rows), cols(k, tok)], gbufs[b].at[pl.ds(0, rows), :], gsem.at[b])

    def save_g(row0, rows, k, b):
        return pltpu.make_async_copy(gbufs[b].at[pl.ds(0, rows), :], g_hbm.at[rows_at(row0, rows), cols(k, tok)], gsem.at[b])

    at.every(lambda k: ask(k).start())
    got[0] = st_loc[:, mine]
    for b in (0, 1):
        out_done(sz.rem, b)
    for b in range(4):
        load_l(0, chunk, b, b).start()
    h_load = pltpu.make_async_copy(h_hbm.at[pl.ds(pl.multiple_of(at.tp * own, own), own), :], hid, hid_sem.at[0])
    h_load.start()
    acc[...] = jnp.zeros(acc.shape, f32)
    hit[...] = jnp.zeros(hit.shape, f32)
    with scope('ask_wait'):
        at.every(lambda k: ask(k).wait_recv())
    tops = got[:, 0:1, :]
    top = jnp.max(tops, axis=0)
    res[...] = top + jnp.log2(jnp.sum(got[:, 1:2, :] * jnp.exp2(tops - top[None]), axis=0))
    at.every(lambda k: answer(k).start())
    st[:, mine] = res[...]
    with scope('answer_wait'):
        at.every(lambda k: answered(k).wait_recv())
    top_row[...] = st[...] - jnp.log2(scale[...])

    def gradient(x, sl, row0, count=True):
        rows = x.shape[0]
        sc = scale[0:1, sl]
        x3 = x.reshape(rows // 8, 8, x.shape[1])
        p = jnp.exp2(x3 - top_row[0:1, sl][None])
        is_label = lax.broadcasted_iota(jnp.int32, p.shape, 0) * 8 == (lab[0:1, sl] - row0 - lax.broadcasted_iota(jnp.int32, (8, x.shape[1]), 0))[None]
        if count:
            hit[...] += jnp.sum(jnp.where(is_label, x3, 0.0), axis=0) * sc
        return jnp.where(is_label, p - sc[None], p).reshape(x.shape).astype(bf16)

    step = min(256, tok)

    half = own // ROUNDS

    def grad_tile(row0, rows, k, b, fresh, first_round=0):
        total = None
        for c0 in range(0, tok, step):
            if fresh:
                for c1 in range(c0, c0 + step, lane):
                    gbufs[b][0:rows, c1:c1 + lane] = gradient(lbufs[b][0:rows, c1:c1 + lane], pl.ds(pl.multiple_of(k * tok + c1, lane), lane), row0, c1 % own // half >= first_round)
            p = dot_nn(gbufs[b][0:rows, c0:c0 + step], z[pl.ds(pl.multiple_of(k * tok + c0, step), step), :])
            total = p if total is None else total + p
        acc[0:rows, :] += total

    def aside(c, rows):
        slot = lax.rem(c, 2)
        return pltpu.make_async_copy(stage.at[slot, pl.ds(0, rows), :], ds_hbm.at[rows_at(c * chunk, rows), :], dw_copy.at[slot])

    def keep_own(c, rows):
        slot = lax.rem(c, 2)
        return pltpu.make_async_copy(stage.at[slot, pl.ds(0, rows), cols(me, width)], dw_hbm.at[rows_at(me * sz.rows + c * chunk, rows), :], own_sem.at[slot])

    def sends(c, rows):
        out = []
        for i, f in enumerate((far * 2, far * 2 + 1, sib)):
            out.append(rcopy(ds_hbm.at[rows_at(c * chunk, rows), cols(f, width)], dw_hbm.at[rows_at(me * sz.rows + c * chunk, rows), :],
                             dw_send.at[c, i], dw_recv.at[lax.rem(f + n - me, n)], dev(at.tp, f)))
        return out

    def ship(c, rows):
        with scope('ship'):
            stage[lax.rem(c, 2), 0:rows, :] = acc[0:rows, :].astype(bf16)
            acc[...] = jnp.zeros(acc.shape, f32)
        aside(c, rows).start()
        keep_own(c, rows).start()

    def flush(c, rows):
        aside(c, rows).wait()
        keep_own(c, rows).wait()
        for cp in sends(c, rows):
            cp.start()

    def early_chunks(lo, hi, first_round, after):
        def one(c, _):
            def quad(i, _):
                for b in range(4):
                    k = 4 * i + b
                    with scope('b1_wait'):
                        load_l(0, chunk, 0, b).wait()

                        @pl.when(jnp.logical_not(jnp.logical_and(c == lo, i == 0)))
                        def _():
                            save_g(0, chunk, 0, b).wait()
                    with scope('b1_tile'):
                        grad_tile(c * chunk, chunk, k, b, True, first_round)
                    save_g(c * chunk, chunk, k, b).start()
                    wrap = k + 4 >= n_tok
                    c2 = jnp.where(wrap, c + 1, c)

                    @pl.when(c2 < hi)
                    def _():
                        load_l(c2 * chunk, chunk, jnp.where(wrap, k + 4 - n_tok, k + 4), b).start()

                @pl.when(jnp.logical_and(i == 0, c > lo))
                def _():
                    flush(c - 1, chunk)
                return 0
            lax.fori_loop(0, n_tok // 4, quad, 0)
            ship(c, chunk)
            after(c)
            return 0
        lax.fori_loop(lo, hi, one, 0)
        for b in range(4):
            save_g(0, chunk, 0, b).wait()

    early_chunks(0, early[0], 0, lambda c: None)

    groups = 2 * n_z
    last = ROUNDS * groups

    def low(e):
        return [(j, chunk) for j in range(sz.full - e)] + [(sz.full - e, sz.rem)]
    per_l = tok // half

    def group_of(q):
        r, g = q // groups, lax.rem(q, groups)
        xi, jj = g // n_z, lax.rem(g, n_z)
        return r, xi, jj, jnp.where(xi == 0, far, at.x), lax.rem(at.z + jj + 1, n_z)

    def pieces(q, b):
        r, _, _, xb, zb = group_of(q)
        cb = at.c if b == 1 else 1 - at.c
        return [pl.multiple_of((xb * 2 + cb) * per_f + (zb * 2 + yb) * own + r * half, half) for yb in (1 - at.y, at.y)]

    def l_part(b, j, i, rows):
        p = 2 * j + i
        return lbufs[2 * b + p // per_l].at[pl.ds(0, rows), pl.ds(p % per_l * half, half)]

    def block_loads(q, b, e):
        row_low = e * chunk
        out = []
        for i, t0 in enumerate(pieces(q, b)):
            out.append(pltpu.make_async_copy(g_hbm.at[pl.ds(0, row_low), pl.ds(t0, half)], qbufs[b].at[pl.ds(0, row_low), pl.ds(i * half, half)], qsem.at[b, i]))
            for j, rows in low(e):
                out.append(pltpu.make_async_copy(l_hbm.at[pl.ds(row_low + j * chunk, rows), pl.ds(t0, half)], l_part(b, j, i, rows), bsem.at[b, 2 * j + i]))
        return out

    def block_saves(q, b, e):
        row_low = e * chunk
        return [pltpu.make_async_copy(qbufs[b].at[pl.ds(row_low, sz.rows - row_low), pl.ds(i * half, half)],
                                      g_hbm.at[pl.ds(row_low, sz.rows - row_low), pl.ds(t0, half)], vsem.at[b, i]) for i, t0 in enumerate(pieces(q, b))]

    def block_dot(q, b, e):
        row_low = e * chunk
        for i, t0 in enumerate(pieces(q, b)):
            for j, rows in low(e):
                row0 = row_low + j * chunk
                qbufs[b][row0:row0 + rows, i * half:(i + 1) * half] = gradient(l_part(b, j, i, rows)[...], pl.ds(t0, half), row0)
        return dot_tn(qbufs[b][...], w[...])

    def to_sib(q):
        slot = lax.rem(q, 2)
        return rcopy(sib_out.at[slot], sib_in.at[slot], sib_s.at[slot], sib_r.at[slot], sibling)

    def to_y(q):
        slot, land = lax.rem(q, 2), lax.rem(q, y_in.shape[0])
        return rcopy(y_out.at[slot], y_in.at[land], y_s.at[slot], y_r.at[land], y_peer)

    def to_z(q):
        r, xi, jj, _, zb = group_of(q)
        return rcopy(z_out.at[jj], z_in.at[r, xi, jj], zz_s.at[jj], zz_r.at[r, xi, jj], dev(zb * 2 + at.y, me))

    def to_x(r):
        return rcopy(x_out, x_in.at[r], x_s.at[0], x_r.at[r], x_peer)

    def z_stage(q):
        _, xi, jj, _, _ = group_of(q)
        with scope('y_wait'):
            to_y(q).wait_recv()
        val = part[lax.rem(q, part.shape[0])] + y_in[lax.rem(q, y_in.shape[0])].astype(f32)

        @pl.when(jj == n_z - 1)
        def _():
            z_own[xi] = val

        @pl.when(jj < n_z - 1)
        def _():
            @pl.when(q >= n_z)
            def _():
                to_z(q - n_z).wait_send()
            z_out[jj] = val.astype(bf16)
            to_z(q).start()

    def z_sum(r, xi):
        val = z_own[xi]
        for jj in range(n_z - 1):
            rcopy(z_out.at[0], z_in.at[r, xi, jj], zz_s.at[jj], zz_r.at[r, xi, jj], sibling).wait_recv()
            val = val + z_in[r, xi, jj].astype(f32)
        return val

    def x_stage(r):
        @pl.when(r > 0)
        def _():
            to_x(0).wait_send()
        with scope('x_stage'):
            x_out[...] = z_sum(r, 0).astype(bf16)
        to_x(r).start()

    def home(tp, r):
        return gh_hbm.at[pl.ds(pl.multiple_of(tp * own + r * half, half), half), :]

    def gathers(r):
        out = [rcopy(gh.at[r], home(at.tp, r), ag_s.at[r, n_z - 1], fw_r.at[r, at.z], y_peer)]
        for jj in (0, 2, 1):
            if jj >= n_z - 1:
                continue
            to = lax.rem(at.z + jj + 1, n_z)
            out.append(rcopy(gh.at[r], home(at.tp, r), ag_s.at[r, jj], ag_r.at[r, jj], dev(to * 2 + at.y, me)))
        return out

    def keep(r):
        return pltpu.make_async_copy(gh.at[r], home(at.tp, r), gh_sem.at[r])

    def arrived(r, jj):
        return rcopy(gh.at[r], home(z_from(jj) * 2 + at.y, r), ag_s.at[r, jj], ag_r.at[r, jj], sibling)

    def onward(r, jj):
        here = home(z_from(jj) * 2 + at.y, r)
        return rcopy(here, here, fw_s.at[r, jj], fw_r.at[r, z_from(jj)], y_peer)

    def tell_gain(k):
        tp, f = at.other(k)
        return rcopy(gg, gg_in.at[at.index], gain_s.at[k], gain_r.at[k], dev(tp, f))

    def heard_gain(k):
        i = lax.rem(at.index + at.n_all - k, at.n_all)
        return rcopy(gg, gg_in.at[i], gain_s.at[k], gain_r.at[k], sibling)

    def final(r):
        with scope('final_wait'):
            to_x(r).wait_recv()
            dz = z_sum(r, 1) + x_in[r].astype(f32)
        h = hid[pl.ds(pl.multiple_of(r * half, half), half), :].astype(f32)
        inv = lax.rsqrt(jnp.mean(h * h, axis=-1, keepdims=True) + NORM_EPS)
        normed = h * inv
        a = dz * gain[...].astype(f32)[None, :]
        gh[r] = (inv * (a - normed * jnp.mean(a * normed, axis=-1, keepdims=True))).astype(bf16)
        gg[0:1, 0:d] += jnp.sum(dz * normed, axis=0, keepdims=True)
        if r == 1:
            hits = jnp.sum(jnp.sum(hit[...], axis=0, keepdims=True), axis=1, keepdims=True)
            gg[0:1, d:] = jnp.broadcast_to(hits, (1, gg.shape[1] - d))
            at.every(lambda k: tell_gain(k).start())
            gg_in[at.index] = gg[...]
        keep(r).start()
        if r == 1:
            gather_start(1)

    def gather_start(r):
        for cp in gathers(r):
            cp.start()

    def forward(r, jj):
        with scope('fw_wait'):
            arrived(r, jj).wait_recv()
        onward(r, jj).start()

    h_load.wait()
    gg[...] = jnp.zeros(gg.shape, f32)

    def dz_round(r, e):
        lo, hi = r * groups, (r + 1) * groups
        for b in (0, 1):
            for cp in block_loads(lo, b, e):
                cp.start()

        def dz_group(q, _):
            for b in (0, 1):
                with scope('a_wait'):
                    for cp in block_loads(q, b, e):
                        cp.wait()

                    @pl.when(q > lo)
                    def _():
                        for cp in block_saves(q - 1, b, e):
                            cp.wait()
                slot = lax.rem(q, 2)
                if b == 0:
                    @pl.when(q >= 2)
                    def _():
                        to_sib(q - 2).wait_send()
                    with scope('a_dot0'):
                        sib_out[slot] = block_dot(q, b, e).astype(bf16)
                    to_sib(q).start()
                else:
                    @pl.when(q >= 2)
                    def _():
                        to_y(q - 2).wait_send()
                    with scope('a_dot1'):
                        val = block_dot(q, b, e)
                        y_sum[...] = val[0:half]
                        part[lax.rem(q, part.shape[0])] = val[half:]
                    with scope('sib_wait'):
                        to_sib(q).wait_recv()
                    y_out[slot] = (y_sum[...] + sib_in[slot, 0:half].astype(f32)).astype(bf16)
                    part[lax.rem(q, part.shape[0])] += sib_in[slot, half:].astype(f32)
                    to_y(q).start()
                for cp in block_saves(q, b, e):
                    cp.start()

                @pl.when(q + 1 < hi)
                def _():
                    for cp in block_loads(q + 1, b, e):
                        cp.start()

            @pl.when(q == lo)
            def _():
                flush(e - 1, chunk)

            @pl.when(q >= lo + 2)
            def _():
                z_stage(q - 2)
            if r == 0:
                @pl.when(q == hi - 1)
                def _():
                    z_stage(q - 1)
            else:
                @pl.when(q == lo + 2)
                def _():
                    for jj in range(n_z - 1):
                        forward(0, jj)
            return 0

        lax.fori_loop(lo, hi, dz_group, 0)
        for b in (0, 1):
            for cp in block_saves(hi - 1, b, e):
                cp.wait()

    dz_round(0, early[0])
    for b in range(4):
        load_l(early[0] * chunk, chunk, b, b).start()

    def between(c):
        @pl.when(c == early[0])
        def _():
            z_stage(groups - 1)
            x_stage(0)
            if early[1] - early[0] == 1:
                final(0)
                gather_start(0)

        if early[1] - early[0] > 1:
            @pl.when(c == early[0] + 1)
            def _():
                final(0)
                gather_start(0)

    early_chunks(early[0], early[1], 1, between)
    dz_round(1, early[1])
    z_stage(last - 2)

    for b in range(4):
        load_g(early[1] * chunk, chunk, b, b).start()

    quads = n_tok // 4
    nearest = [jj for jj in (2, 0, 1) if jj < n_z - 1]
    steps = [(6 + t, 1, jj) for t, jj in enumerate(nearest)]

    def late_chunk(c, _):
        def quad(i, _):
            for b in range(4):
                k = 4 * i + b
                with scope('b2_wait'):
                    load_g(0, chunk, 0, b).wait()
                with scope('b2_tile'):
                    grad_tile(c * chunk, chunk, k, b, False)
                wrap = k + 4 >= n_tok
                c2, k2 = jnp.where(wrap, c + 1, c), jnp.where(wrap, k + 4 - n_tok, k + 4)

                @pl.when(c2 < sz.full)
                def _():
                    load_g(c2 * chunk, chunk, k2, b).start()

                @pl.when(c2 == sz.full)
                def _():
                    load_g(row_rem, sz.rem, k2, b).start()
                if b == 0:
                    @pl.when(jnp.logical_and(i == 0, c > early[1]))
                    def _():
                        flush(c - 1, chunk)

            for t, r, jj in steps:
                @pl.when((c - early[1]) * quads + i == t)
                def _():
                    forward(r, jj)
            return 0
        lax.fori_loop(0, quads, quad, 0)
        ship(c, chunk)

        @pl.when(c == early[1])
        def _():
            z_stage(last - 1)
            x_stage(1)

        @pl.when(c == early[1] + 1)
        def _():
            final(1)
        return 0

    lax.fori_loop(early[1], sz.full, late_chunk, 0)
    def late_rem(i, _):
        for b in range(4):
            with scope('b2_wait'):
                load_g(row_rem, sz.rem, 0, b).wait()
            with scope('b2_rem'):
                grad_tile(row_rem, sz.rem, 4 * i + b, b, False)

            @pl.when(4 * i + b + 4 < n_tok)
            def _():
                load_g(row_rem, sz.rem, 4 * i + b + 4, b).start()
            if b == 0:
                @pl.when(i == 0)
                def _():
                    flush(sz.full - 1, chunk)
        return 0

    lax.fori_loop(0, n_tok // 4, late_rem, 0)
    ship(sz.full, sz.rem)
    flush(sz.full, sz.rem)
    for t, r, jj in steps:
        if t >= (sz.full - early[1]) * quads:
            forward(r, jj)

    with scope('t_gain'):
        at.every(lambda k: heard_gain(k).wait_recv())
    total = jnp.sum(gg_in[...], axis=0)
    gg_out[0:1, 0:d] = total[0:1, 0:d]
    gg_out[0:1, d:] = (jnp.sum(st[...] * scale[...], axis=1, keepdims=True) - total[0:1, d:]) * (1.0 / LOG2E)
    with scope('t_small'):
        at.every(lambda k: ask(k).wait_send())
        at.every(lambda k: answer(k).wait_send())
        at.every(lambda k: tell_gain(k).wait_send())
        for k in range(1, n):
            for cp in tok_out(k):
                cp.wait_send()
        block_out().wait_send()
        for p in (0, 1):
            h_to_x(p).wait_send()
            for jj in range(n_z - 1):
                h_to_z(jj, p).wait_send()
        for zo in range(n_z):
            h_to_y(zo).wait_send()
        for tp in range(n_tp):
            h_to_core(tp).wait_send()

        def w_sent(c, _):
            for k in range(1, n):
                remote(k, c, c * chunk, chunk).wait_send()
            return 0

        lax.fori_loop(0, sz.full, w_sent, 0)
        for k in range(1, n):
            remote(k, sz.full, row_rem, sz.solid).wait_send()
            when_not_last(lax.rem(me + k, n), lambda: remote(k, sz.full + 1, row_odd, sz.short).wait_send())
        for q in (last - 2, last - 1):
            to_sib(q).wait_send()
            to_y(q).wait_send()
        for q in range(last - n_z, last - 1):
            to_z(q).wait_send()
        to_x(1).wait_send()
    with scope('t_send'):
        def sent(c, _):
            for cp in sends(c, chunk):
                cp.wait_send()
            return 0
        lax.fori_loop(0, sz.full, sent, 0)
        for cp in sends(sz.full, sz.rem):
            cp.wait_send()
    for r in range(ROUNDS):
        with scope(f't_gather{r}'):
            keep(r).wait()
            for cp in gathers(r):
                cp.wait_send()
            for jj in range(n_z - 1):
                onward(r, jj).wait_send()
            for zo in range(n_z):
                rcopy(gh.at[r], home(zo * 2 + 1 - at.y, r), ag_s.at[r, 0], fw_r.at[r, zo], y_peer).wait_recv()
    with scope('t_dw'):
        for k in range(1, n):
            src = lax.rem(me + n - k, n)
            rcopy(dw_hbm.at[pl.ds(0, sz.rows), :], dw_hbm.at[rows_at(src * sz.rows, sz.rows), :], dw_send.at[0, 0], dw_recv.at[k], sibling).wait_recv()


HBM = pl.BlockSpec(memory_space=pl.ANY)
VM = pl.BlockSpec(memory_space=pltpu.VMEM)
DMA = pltpu.SemaphoreType.DMA


def solution(mesh, chunk=CHUNK, tok=TOK, early=EARLY):
    n_fsdp, n_tp = mesh.shape['fsdp'], mesh.shape['tp']
    n_all, n_z = n_fsdp * n_tp, n_tp // 2
    S, V = jax.ShapeDtypeStruct, pltpu.VMEM
    i32 = jnp.int32

    def per_device(hidden, labels, tok_mask, norm_gain, w_rows):
        per_f, d = hidden.shape
        width, vocab_tp = w_rows.shape
        tokens, own = per_f * n_fsdp, per_f // n_tp
        half = own // ROUNDS
        sz = Sizes(vocab_tp, n_fsdp, chunk)
        n_low = sz.full - early[0] + 1

        dw_t, grad_hidden, sums, *_ = pl.pallas_call(
            functools.partial(head_kernel, sz, n_tp, vocab_tp, chunk, tok, early),
            out_shape=(S((n_fsdp * sz.rows, width), bf16), S(hidden.shape, bf16), S((1, d + 128), f32),
                       S((sz.rows, tokens), f32), S((sz.rows, tokens), bf16), S((tokens, d), bf16), S(((sz.full + 1) * chunk, d), bf16)),
            in_specs=[HBM, VM, VM, VM, HBM], out_specs=(HBM, HBM, VM, HBM, HBM, HBM, HBM),
            scratch_shapes=[
                V((tokens, d), bf16), V((sz.rows, d), bf16), *[V((chunk, tok), f32)] * 4, *[V((chunk, tok), bf16)] * 4, *[V((sz.rows, 2 * half), bf16)] * 2,
                V((8, tokens), f32), V((8, tokens), f32), V((1, tokens), f32), V((1, tokens), i32), V((n_fsdp, 1, per_f), i32), V((n_fsdp, 1, per_f), f32),
                V((2, tokens), f32), V((n_all, 2, own), f32), V((1, own), f32), V((1, tokens), f32), V((1, tokens), f32), V((8, min(128, half)), f32), V((own, d), bf16),
                V((chunk, d), f32), V((2, chunk, d), bf16), V((2, 2 * half, d), bf16), V((2, 2 * half, d), bf16), V((half, d), f32),
                V((2, half, d), bf16), V((6, half, d), bf16), V((3, half, d), f32), V((n_z - 1, half, d), bf16), V((ROUNDS, 2, n_z - 1, half, d), bf16), V((2, half, d), f32),
                V((half, d), bf16), V((ROUNDS, half, d), bf16), V((ROUNDS, half, d), bf16), V((1, d + 128), f32), V((n_all, 1, d + 128), f32),
                DMA((sz.full + 2, n_fsdp)), DMA((sz.full + 2, n_fsdp)), DMA((sz.full + 2,)), DMA((per_f // min(256, own),)), DMA((4,)), DMA((4,)), DMA((2, 2)), DMA((2, 2 * n_low)), DMA((2, 2)),
                DMA((n_all,)), DMA((n_all,)), DMA((n_all,)), DMA((n_all,)), DMA((2, n_fsdp)), DMA((2, n_fsdp)), DMA((2,)), DMA((2,)), DMA((2,)),
                DMA((n_z - 1, 2)), DMA((n_z - 1, 2)), DMA((n_z,)), DMA((n_z,)), DMA((n_tp,)), DMA((n_tp,)),
                DMA((1,)), DMA((2,)), DMA((sz.full + 1, 3)), DMA((n_fsdp,)), DMA((2,)), DMA((2,)), DMA((2,)), DMA((2,)), DMA((8,)),
                DMA((n_z - 1,)), DMA((ROUNDS, 2, n_z - 1)), DMA((1,)), DMA((ROUNDS,)),
                DMA((ROUNDS, n_z)), DMA((ROUNDS, n_z)), DMA((ROUNDS, n_z)), DMA((ROUNDS, n_z)), DMA((ROUNDS,)), DMA((n_all,)), DMA((n_all,))],
            compiler_params=pltpu.CompilerParams(vmem_limit_bytes=VMEM_LIMIT, collective_id=0, has_side_effects=True), name='head',
        )(hidden, labels[None, :], tok_mask[None, :], norm_gain, w_rows.T)
        return sums[0, d], grad_hidden, dw_t[:vocab_tp].T, sums[0, :d]

    return jax.shard_map(per_device, mesh=mesh, in_specs=(P('fsdp', None), P('fsdp'), P('fsdp'), P(), P('fsdp', 'tp')), out_specs=(P(), P('fsdp', None), P('fsdp', 'tp'), P()), check_vma=False)
```

```python
import functools

import jax
import jax.numpy as jnp
from jax import lax
from jax.experimental import pallas as pl
from jax.experimental.pallas import tpu as pltpu
from jax.sharding import PartitionSpec as P

NORM_EPS = 1e-6
LOG2E = 1.4426950408889634
NEG = -1e30
CHUNK = 512
TOK = 1024
EARLY = (2, 5)
AHEAD = 5
ROUNDS = 2
VMEM_LIMIT = 67_043_328
MESH = pl.DeviceIdType.MESH
scope = jax.named_scope
f32, bf16 = jnp.float32, jnp.bfloat16


def dot_nt(a, b):
    return lax.dot_general(a, b, (((1,), (1,)), ((), ())), preferred_element_type=f32)


def dot_tn(a, b):
    return lax.dot_general(a, b, (((0,), (0,)), ((), ())), preferred_element_type=f32)


def dot_nn(a, b):
    return lax.dot_general(a, b, (((1,), (0,)), ((), ())), preferred_element_type=f32)


def cols(k, size):
    return pl.ds(pl.multiple_of(k * size, size), size)


def rows_at(row0, rows):
    return pl.ds(pl.multiple_of(row0, 16), rows)


class Sizes:
    def __init__(self, vocab_tp, n_fsdp, chunk):
        self.n = n_fsdp
        self.rows = -(-vocab_tp // (n_fsdp * 16)) * 16
        self.short = n_fsdp * self.rows - vocab_tp
        self.full = self.rows // chunk
        self.rem = self.rows - self.full * chunk
        self.solid = self.rem - self.short
        assert self.rem > self.short and self.rem % 16 == 0 and self.short % 16 == 0


class Place:
    def __init__(self, n_fsdp, n_tp):
        self.n_fsdp, self.n_tp, self.n_all = n_fsdp, n_tp, n_fsdp * n_tp
        self.f, self.tp = lax.axis_index('fsdp'), lax.axis_index('tp')
        self.x, self.c = self.f // 2, lax.rem(self.f, 2)
        self.n_z = n_tp // 2
        self.z, self.y = self.tp // 2, lax.rem(self.tp, 2)
        self.index = self.tp * n_fsdp + self.f

    def other(self, k):
        i = lax.rem(self.index + k, self.n_all)
        return i // self.n_fsdp, lax.rem(i, self.n_fsdp)

    def every(self, fn):
        def go(k, _):
            fn(k)
            return 0
        lax.fori_loop(1, self.n_all, go, 0)


def dev(tp, f):
    return {'tp': tp, 'fsdp': f}


def rcopy(src, dst, ssem, rsem, to):
    return pltpu.make_async_remote_copy(src_ref=src, dst_ref=dst, send_sem=ssem, recv_sem=rsem, device_id=to, device_id_type=MESH)


def enter(at):
    barrier = pltpu.get_barrier_semaphore()

    def tell(k):
        tp, f = at.other(k)
        pl.semaphore_signal(barrier, inc=1, device_id=dev(tp, f), device_id_type=MESH)

    at.every(tell)
    pl.semaphore_wait(barrier, at.n_all - 1)


def head_kernel(sz, n_tp, vocab_tp, chunk, tok, early,
                h_hbm, lab_ref, mask_ref, gain, w_hbm,
                dw_hbm, gh_hbm, gg_out, l_hbm, g_hbm, h_all, ds_hbm,
                z, w, l0, l1, l2, l3, g0, g1, g2, g3, q0, q1, m, s, scale, lab, lab_in, mask_in, st_loc, got, res, st, top_row, hit, hid,
                acc, stage, sib_out, sib_in, y_sum, y_out, y_in, part, z_out, z_in, z_own, x_out, x_in, gh, gg, gg_in,
                w_s, w_r, loc, hsem, lsem, gsem, qsem, bsem, vsem, ssend, srecv, rsend, rrecv, tok_s, tok_r, blk, hx_s, hx_r, hz_s, hz_r, hy_s, hy_r, hc_s, hc_r,
                hid_sem, dw_copy, dw_send, dw_recv, own_sem, sib_s, sib_r, y_s, y_r, zz_s, zz_r, x_s, x_r, ag_s, ag_r, fw_s, fw_r, gh_sem, gain_s, gain_r):
    at = Place(sz.n, n_tp)
    me, n, n_z, width = at.f, sz.n, at.n_z, w_hbm.shape[1]
    per_f, d = h_hbm.shape
    tokens, own = per_f * n, per_f // n_tp
    lbufs, gbufs, qbufs = (l0, l1, l2, l3), (g0, g1, g2, g3), (q0, q1)
    far, sib = 1 - at.x, at.x * 2 + 1 - at.c
    through = far * 2 + at.c
    sibling, y_peer, x_peer = dev(at.tp, sib), dev(at.z * 2 + 1 - at.y, me), dev(at.tp, through)
    row_rem = sz.full * chunk
    row_odd = row_rem + sz.solid

    with scope('enter'):
        enter(at)

    def slab(f, tp):
        return pl.ds(pl.multiple_of((f * n_tp + tp) * own, own), own)

    def block(f):
        return pl.ds(pl.multiple_of(f * per_f, per_f), per_f)

    own2 = own // 2

    def part_of(f, tp, p):
        return pl.ds(pl.multiple_of((f * n_tp + tp) * own + p * own2, own2), own2)

    def h_to_x(p):
        return rcopy(h_hbm.at[pl.ds(pl.multiple_of(at.tp * own + p * own2, own2), own2), :], h_all.at[part_of(me, at.tp, p), :], hx_s.at[p], hx_r.at[p], x_peer)

    def h_from_x(p):
        here = h_all.at[part_of(through, at.tp, p), :]
        return rcopy(here, here, hx_s.at[p], hx_r.at[p], x_peer)

    def block_out():
        return rcopy(h_hbm, h_all.at[block(me), :], blk.at[0], blk.at[1], sibling)

    def block_in():
        return rcopy(h_hbm, h_all.at[block(sib), :], blk.at[0], blk.at[1], sibling)

    def moved(tp, ssem, rsem, to):
        here = h_all.at[slab(through, tp), :]
        return rcopy(here, here, ssem, rsem, to)

    def z_from(jj):
        return lax.rem(at.z + n_z - jj - 1, n_z)

    def h_to_z(jj, p):
        here = h_all.at[part_of(through, at.tp, p), :]
        return rcopy(here, here, hz_s.at[jj, p], hz_r.at[jj, p], dev(lax.rem(at.z + jj + 1, n_z) * 2 + at.y, me))

    def h_from_z(jj, p):
        here = h_all.at[part_of(through, z_from(jj) * 2 + at.y, p), :]
        return rcopy(here, here, hz_s.at[jj, p], hz_r.at[jj, p], sibling)

    def h_to_y(zo):
        return moved(zo * 2 + at.y, hy_s.at[zo], hy_r.at[zo], y_peer)

    def h_from_y(zo):
        return moved(zo * 2 + 1 - at.y, hy_s.at[zo], hy_r.at[zo], y_peer)

    def h_to_core(tp):
        return moved(tp, hc_s.at[tp], hc_r.at[tp], sibling)

    def h_from_core(tp):
        here = h_all.at[slab(far * 2 + 1 - at.c, tp), :]
        return rcopy(here, here, hc_s.at[tp], hc_r.at[tp], sibling)

    def tok_out(k):
        to = dev(at.tp, lax.rem(me + k, n))
        return [rcopy(lab_ref, lab_in.at[me], tok_s.at[0, k], tok_r.at[0, k], to), rcopy(mask_ref, mask_in.at[me], tok_s.at[1, k], tok_r.at[1, k], to)]

    def tok_in(k):
        src = lax.rem(me + n - k, n)
        return [rcopy(lab_ref, lab_in.at[src], tok_s.at[0, k], tok_r.at[0, k], sibling), rcopy(mask_ref, mask_in.at[src], tok_s.at[1, k], tok_r.at[1, k], sibling)]

    for p in (0, 1):
        h_to_x(p).start()
    block_out().start()
    for k in range(1, n):
        for cp in tok_out(k):
            cp.start()
    lab_in[me] = lab_ref[...]
    mask_in[me] = mask_ref[...]

    def remote(k, c, row0, rows):
        dest = lax.rem(me + k, n)
        return rcopy(w_hbm.at[rows_at(dest * sz.rows + row0, rows), :], w.at[rows_at(row0, rows), cols(me, width)], w_s.at[c, k], w_r.at[c, k], dev(at.tp, dest))

    def arrival(k, c, row0, rows):
        src = lax.rem(me + n - k, n)
        return rcopy(w_hbm.at[pl.ds(0, rows), :], w.at[rows_at(row0, rows), cols(src, width)], w_s.at[c, k], w_r.at[c, k], sibling)

    def local(c, row0, rows):
        return pltpu.make_async_copy(w_hbm.at[rows_at(me * sz.rows + row0, rows), :], w.at[rows_at(row0, rows), cols(me, width)], loc.at[c])

    def issue(c):
        local(c, c * chunk, chunk).start()
        for k in range(1, n):
            remote(k, c, c * chunk, chunk).start()

    def when_not_last(dest, fn):
        if sz.short:
            pl.when(dest != n - 1)(fn)

    def issue_rem():
        local(sz.full, row_rem, sz.solid).start()
        when_not_last(me, lambda: local(sz.full + 1, row_odd, sz.short).start())
        for k in range(1, n):
            remote(k, sz.full, row_rem, sz.solid).start()
            when_not_last(lax.rem(me + k, n), lambda: remote(k, sz.full + 1, row_odd, sz.short).start())

    ahead = min(AHEAD, sz.full)
    for c in range(ahead):
        issue(c)
    if sz.short:
        @pl.when(me == n - 1)
        def _():
            w[row_odd:, :] = jnp.zeros((sz.short, d), bf16)

    sub = min(256, own)
    slices, per_own = per_f // sub, own // sub
    lane = min(128, sub)

    def place(t, i):
        near = jnp.where(t == 0, me, sib) * per_f + i * sub
        j = i // per_own
        f = jnp.where(j < n_z, through, far * 2 + 1 - at.c)
        y = jnp.where(t == 2, at.y, 1 - at.y)
        away = (f * n_tp + lax.rem(j, n_z) * 2 + y) * own + lax.rem(i, per_own) * sub
        return pl.multiple_of(jnp.where(t < 2, near, away), sub)

    def norm(t):
        def load(i):
            here = pl.ds(place(t, i), sub)
            return pltpu.make_async_copy(h_hbm.at[cols(i, sub), :] if t == 0 else h_all.at[here, :], z.at[here, :], hsem.at[i])

        def begin(i, _):
            load(i).start()
            return 0

        def one(i, _):
            load(i).wait()
            here = pl.ds(place(t, i), sub)
            h = z[here, :].astype(f32)
            inv = lax.rsqrt(jnp.mean(h * h, axis=-1, keepdims=True) + NORM_EPS)
            z[here, :] = (h * inv * gain[...].astype(f32)[None, :]).astype(bf16)
            return 0

        with scope(f'norm{t}'):
            lax.fori_loop(0, slices, begin, 0)
            lax.fori_loop(0, slices, one, 0)

    def spread_x(p):
        with scope('x_wait'):
            h_from_x(p).wait_recv()
        for jj in (2, 0, 1):
            if jj < n_z - 1:
                h_to_z(jj, p).start()

    norm(0)
    spread_x(0)
    with scope('blk_wait'):
        block_in().wait_recv()
    norm(1)
    spread_x(1)
    h_to_y(at.z).start()
    h_to_core(at.tp).start()
    with scope('tok_wait'):
        for k in range(1, n):
            for cp in tok_in(k):
                cp.wait_recv()
    count = jnp.sum(mask_in[...], axis=(0, 2), keepdims=True)[0]
    for f in range(n):
        here = pl.ds(f * per_f, per_f)
        scale[0:1, here] = mask_in[f] / count
        rel = lab_in[f] - at.tp * vocab_tp
        lab[0:1, here] = jnp.where(jnp.logical_and(rel >= 0, rel < vocab_tp), rel - me * sz.rows, -1)

    def spread_z():
        with scope('z_wait'):
            for jj in range(n_z - 1):
                for p in (0, 1):
                    h_from_z(jj, p).wait_recv()
                h_to_y(z_from(jj)).start()
                h_to_core(z_from(jj) * 2 + at.y).start()

    def spread_y():
        with scope('hy_wait'):
            for k in range(n_z):
                zo = lax.rem(at.z + n_z - k, n_z)
                h_from_y(zo).wait_recv()
                h_to_core(zo * 2 + 1 - at.y).start()

    def far_ready(y):
        with scope('core_wait'):
            for zo in range(n_z):
                h_from_core(zo * 2 + y).wait_recv()

    m[...] = jnp.full(m.shape, NEG, f32)
    s[...] = jnp.zeros(s.shape, f32)
    per_buf = tok // sub
    n_buf = slices // per_buf

    def out_copies(row0, rows, t, b):
        return [pltpu.make_async_copy(lbufs[b * n_buf + i // per_buf].at[pl.ds(0, rows), pl.ds(i % per_buf * sub, sub)],
                                      l_hbm.at[rows_at(row0, rows), pl.ds(place(t, i), sub)], lsem.at[b * n_buf + i // per_buf]) for i in range(slices)]

    def out_done(rows, b):
        for i in range(n_buf):
            pltpu.make_async_copy(lbufs[b * n_buf + i].at[pl.ds(0, rows), :], l_hbm.at[pl.ds(0, rows), pl.ds(0, tok)], lsem.at[b * n_buf + i]).wait()

    def statistics(read, rows, t0):
        group = min(4, rows // 8)
        for c1 in range(0, sub, lane):
            sl = pl.ds(pl.multiple_of(t0 + c1, lane), lane)
            big, tot = m[:, sl], s[:, sl]
            for g in range(0, rows // 8, group):
                piece = [read(r, c1) for r in range(g, min(g + group, rows // 8))]
                new = functools.reduce(jnp.maximum, piece, big)
                tot = tot * jnp.exp2(big - new)
                for x in piece:
                    tot += jnp.exp2(x - new)
                big = new
            m[:, sl], s[:, sl] = big, tot

    def slice_at(b, i):
        return lbufs[b * n_buf + i // per_buf], i % per_buf * sub

    def late_statistics(t, b):
        for i in range(slices - lag, slices):
            buf, i0 = slice_at(b, i)
            statistics(lambda r, c1: buf[8 * r:8 * r + 8, i0 + c1:i0 + c1 + lane], chunk, place(t, i))

    def logits_tile(row0, rows, t, b, masked):
        for i in range(slices):
            t0 = place(t, i)
            logits = dot_nt(w[rows_at(row0, rows), :], z[pl.ds(t0, sub), :]) * LOG2E
            if masked:
                ids = lax.broadcasted_iota(jnp.int32, (rows, sub), 0)
                logits = jnp.where(ids < jnp.where(me == n - 1, sz.solid, sz.rem), logits, NEG)
            buf, i0 = slice_at(b, i)
            buf[0:rows, i0:i0 + sub] = logits
            if masked or i < slices - lag:
                statistics(lambda r, c1: logits[8 * r:8 * r + 8, c1:c1 + lane], rows, t0)

    lag = 2
    for i in range(slices - lag, slices):
        buf, i0 = slice_at(1, i)
        buf[:, i0:i0 + sub] = jnp.full((chunk, sub), NEG, f32)

    n_a = min(3, sz.full)
    n_c = min(3, sz.full - n_a)
    k_b, k_c = 2 * n_a, 3 * n_a
    k_d = k_c + 3 * n_c
    k_e = k_d + n_a + n_c

    def item(k):
        u, v = k - k_c, k - k_e
        c = jnp.where(k < k_b, k // 2, jnp.where(k < k_c, k - k_b, jnp.where(k < k_d, n_a + u // 3, jnp.where(k < k_e, k - k_d, n_a + n_c + v // 4))))
        t = jnp.where(k < k_b, lax.rem(k, 2), jnp.where(k < k_c, 2, jnp.where(k < k_d, lax.rem(u, 3), jnp.where(k < k_e, 3, lax.rem(v, 4)))))
        return c, t

    def work(i2, _):
        for b in (0, 1):
            k = 2 * i2 + b
            c, t = item(k)

            @pl.when(t == 0)
            def _():
                with scope('w_wait'):
                    local(c, c * chunk, chunk).wait()
                    for j in range(1, n):
                        arrival(j, c, c * chunk, chunk).wait_recv()

                @pl.when(c + ahead < sz.full)
                def _():
                    issue(c + ahead)

                @pl.when(c + ahead == sz.full)
                def _():
                    issue_rem()

            @pl.when(k == k_b)
            def _():
                spread_z()
                far_ready(at.y)
                norm(2)

            @pl.when(k == max(k_d - 3, k_c))
            def _():
                spread_y()

            @pl.when(k == k_d)
            def _():
                far_ready(1 - at.y)
                norm(3)

            with scope('l_wait'):
                @pl.when(k >= 2)
                def _():
                    out_done(chunk, b)
            with scope('l_tile'):
                late_statistics(item(jnp.maximum(k - 1, 0))[1], 1 - b)
                logits_tile(c * chunk, chunk, t, b, False)
            for cp in out_copies(c * chunk, chunk, t, b):
                cp.start()
        return 0

    lax.fori_loop(0, sz.full * 2, work, 0)
    late_statistics(item(4 * sz.full - 1)[1], 1)
    with scope('w_wait_rem'):
        local(sz.full, row_rem, sz.solid).wait()
        when_not_last(me, lambda: local(sz.full + 1, row_odd, sz.short).wait())
        for k in range(1, n):
            arrival(k, sz.full, row_rem, sz.solid).wait_recv()
            when_not_last(me, lambda: arrival(k, sz.full + 1, row_odd, sz.short).wait_recv())

    def work_rem(i2, _):
        for b in (0, 1):
            @pl.when(i2 == 0)
            def _():
                out_done(chunk, b)

            @pl.when(i2 > 0)
            def _():
                out_done(sz.rem, b)
            logits_tile(row_rem, sz.rem, 2 * i2 + b, b, True)
            for cp in out_copies(row_rem, sz.rem, 2 * i2 + b, b):
                cp.start()
        return 0

    with scope('l_rem'):
        lax.fori_loop(0, 2, work_rem, 0)

    big = jnp.max(m[...], axis=0, keepdims=True)
    st_loc[0:1, :] = big
    st_loc[1:2, :] = jnp.sum(s[...] * jnp.exp2(m[...] - big), axis=0, keepdims=True)
    mine = slab(at.f, at.tp)

    def ask(k):
        tp, f = at.other(k)
        return rcopy(st_loc.at[:, slab(f, tp)], got.at[k], ssend.at[k], srecv.at[k], dev(tp, f))

    def answer(k):
        tp, f = at.other(k)
        return rcopy(res, st.at[:, mine], rsend.at[k], rrecv.at[k], dev(tp, f))

    def answered(k):
        tp, f = at.other(at.n_all - k)
        return rcopy(res, st.at[:, slab(f, tp)], rsend.at[k], rrecv.at[k], dev(tp, f))

    n_tok = tokens // tok

    def load_l(row0, rows, k, b):
        return pltpu.make_async_copy(l_hbm.at[rows_at(row0, rows), cols(k, tok)], lbufs[b].at[pl.ds(0, rows), :], lsem.at[b])

    def load_g(row0, rows, k, b):
        return pltpu.make_async_copy(g_hbm.at[rows_at(row0, rows), cols(k, tok)], gbufs[b].at[pl.ds(0, rows), :], gsem.at[b])

    def save_g(row0, rows, k, b):
        return pltpu.make_async_copy(gbufs[b].at[pl.ds(0, rows), :], g_hbm.at[rows_at(row0, rows), cols(k, tok)], gsem.at[b])

    at.every(lambda k: ask(k).start())
    got[0] = st_loc[:, mine]
    for b in (0, 1):
        out_done(sz.rem, b)
    for b in range(4):
        load_l(0, chunk, b, b).start()
    h_load = pltpu.make_async_copy(h_hbm.at[pl.ds(pl.multiple_of(at.tp * own, own), own), :], hid, hid_sem.at[0])
    h_load.start()
    acc[...] = jnp.zeros(acc.shape, f32)
    hit[...] = jnp.zeros(hit.shape, f32)
    with scope('ask_wait'):
        at.every(lambda k: ask(k).wait_recv())
    tops = got[:, 0:1, :]
    top = jnp.max(tops, axis=0)
    res[...] = top + jnp.log2(jnp.sum(got[:, 1:2, :] * jnp.exp2(tops - top[None]), axis=0))
    at.every(lambda k: answer(k).start())
    st[:, mine] = res[...]
    with scope('answer_wait'):
        at.every(lambda k: answered(k).wait_recv())
    top_row[...] = st[...] - jnp.log2(scale[...])

    def gradient(x, sl, row0, count=True):
        rows = x.shape[0]
        sc = scale[0:1, sl]
        x3 = x.reshape(rows // 8, 8, x.shape[1])
        p = jnp.exp2(x3 - top_row[0:1, sl][None])
        is_label = lax.broadcasted_iota(jnp.int32, p.shape, 0) * 8 == (lab[0:1, sl] - row0 - lax.broadcasted_iota(jnp.int32, (8, x.shape[1]), 0))[None]
        if count:
            hit[...] += jnp.sum(jnp.where(is_label, x3, 0.0), axis=0) * sc
        return jnp.where(is_label, p - sc[None], p).reshape(x.shape).astype(bf16)

    step = min(256, tok)

    half = own // ROUNDS

    def grad_tile(row0, rows, k, b, fresh, first_round=0):
        total = None
        for c0 in range(0, tok, step):
            if fresh:
                for c1 in range(c0, c0 + step, lane):
                    gbufs[b][0:rows, c1:c1 + lane] = gradient(lbufs[b][0:rows, c1:c1 + lane], pl.ds(pl.multiple_of(k * tok + c1, lane), lane), row0, c1 % own // half >= first_round)
            p = dot_nn(gbufs[b][0:rows, c0:c0 + step], z[pl.ds(pl.multiple_of(k * tok + c0, step), step), :])
            total = p if total is None else total + p
        acc[0:rows, :] += total

    def aside(c, rows):
        slot = lax.rem(c, 2)
        return pltpu.make_async_copy(stage.at[slot, pl.ds(0, rows), :], ds_hbm.at[rows_at(c * chunk, rows), :], dw_copy.at[slot])

    def keep_own(c, rows):
        slot = lax.rem(c, 2)
        return pltpu.make_async_copy(stage.at[slot, pl.ds(0, rows), cols(me, width)], dw_hbm.at[rows_at(me * sz.rows + c * chunk, rows), :], own_sem.at[slot])

    def sends(c, rows):
        out = []
        for i, f in enumerate((far * 2, far * 2 + 1, sib)):
            out.append(rcopy(ds_hbm.at[rows_at(c * chunk, rows), cols(f, width)], dw_hbm.at[rows_at(me * sz.rows + c * chunk, rows), :],
                             dw_send.at[c, i], dw_recv.at[lax.rem(f + n - me, n)], dev(at.tp, f)))
        return out

    def ship(c, rows):
        with scope('ship'):
            stage[lax.rem(c, 2), 0:rows, :] = acc[0:rows, :].astype(bf16)
            acc[...] = jnp.zeros(acc.shape, f32)
        aside(c, rows).start()
        keep_own(c, rows).start()

    def flush(c, rows):
        aside(c, rows).wait()
        keep_own(c, rows).wait()
        for cp in sends(c, rows):
            cp.start()

    def early_chunks(lo, hi, first_round, after):
        def one(c, _):
            def quad(i, _):
                for b in range(4):
                    k = 4 * i + b
                    with scope('b1_wait'):
                        load_l(0, chunk, 0, b).wait()

                        @pl.when(jnp.logical_not(jnp.logical_and(c == lo, i == 0)))
                        def _():
                            save_g(0, chunk, 0, b).wait()
                    with scope('b1_tile'):
                        grad_tile(c * chunk, chunk, k, b, True, first_round)
                    save_g(c * chunk, chunk, k, b).start()
                    wrap = k + 4 >= n_tok
                    c2 = jnp.where(wrap, c + 1, c)

                    @pl.when(c2 < hi)
                    def _():
                        load_l(c2 * chunk, chunk, jnp.where(wrap, k + 4 - n_tok, k + 4), b).start()

                @pl.when(jnp.logical_and(i == 0, c > lo))
                def _():
                    flush(c - 1, chunk)
                return 0
            lax.fori_loop(0, n_tok // 4, quad, 0)
            ship(c, chunk)
            after(c)
            return 0
        lax.fori_loop(lo, hi, one, 0)
        for b in range(4):
            save_g(0, chunk, 0, b).wait()

    early_chunks(0, early[0], 0, lambda c: None)

    groups = 2 * n_z
    last = ROUNDS * groups

    def low(e):
        return [(j, chunk) for j in range(sz.full - e)] + [(sz.full - e, sz.rem)]
    per_l = tok // half

    def group_of(q):
        r, g = q // groups, lax.rem(q, groups)
        xi, jj = g // n_z, lax.rem(g, n_z)
        return r, xi, jj, jnp.where(xi == 0, far, at.x), lax.rem(at.z + jj + 1, n_z)

    def pieces(q, b):
        r, _, _, xb, zb = group_of(q)
        cb = at.c if b == 1 else 1 - at.c
        return [pl.multiple_of((xb * 2 + cb) * per_f + (zb * 2 + yb) * own + r * half, half) for yb in (1 - at.y, at.y)]

    def l_part(b, j, i, rows):
        p = 2 * j + i
        return lbufs[2 * b + p // per_l].at[pl.ds(0, rows), pl.ds(p % per_l * half, half)]

    def block_loads(q, b, e):
        row_low = e * chunk
        out = []
        for i, t0 in enumerate(pieces(q, b)):
            out.append(pltpu.make_async_copy(g_hbm.at[pl.ds(0, row_low), pl.ds(t0, half)], qbufs[b].at[pl.ds(0, row_low), pl.ds(i * half, half)], qsem.at[b, i]))
            for j, rows in low(e):
                out.append(pltpu.make_async_copy(l_hbm.at[pl.ds(row_low + j * chunk, rows), pl.ds(t0, half)], l_part(b, j, i, rows), bsem.at[b, 2 * j + i]))
        return out

    def block_saves(q, b, e):
        row_low = e * chunk
        return [pltpu.make_async_copy(qbufs[b].at[pl.ds(row_low, sz.rows - row_low), pl.ds(i * half, half)],
                                      g_hbm.at[pl.ds(row_low, sz.rows - row_low), pl.ds(t0, half)], vsem.at[b, i]) for i, t0 in enumerate(pieces(q, b))]

    def block_dot(q, b, e):
        row_low = e * chunk
        for i, t0 in enumerate(pieces(q, b)):
            for j, rows in low(e):
                row0 = row_low + j * chunk
                qbufs[b][row0:row0 + rows, i * half:(i + 1) * half] = gradient(l_part(b, j, i, rows)[...], pl.ds(t0, half), row0)
        return dot_tn(qbufs[b][...], w[...])

    def to_sib(q):
        slot = lax.rem(q, 2)
        return rcopy(sib_out.at[slot], sib_in.at[slot], sib_s.at[slot], sib_r.at[slot], sibling)

    def to_y(q):
        slot, land = lax.rem(q, 2), lax.rem(q, y_in.shape[0])
        return rcopy(y_out.at[slot], y_in.at[land], y_s.at[slot], y_r.at[land], y_peer)

    def to_z(q):
        r, xi, jj, _, zb = group_of(q)
        return rcopy(z_out.at[jj], z_in.at[r, xi, jj], zz_s.at[jj], zz_r.at[r, xi, jj], dev(zb * 2 + at.y, me))

    def to_x(r):
        return rcopy(x_out, x_in.at[r], x_s.at[0], x_r.at[r], x_peer)

    def z_stage(q):
        _, xi, jj, _, _ = group_of(q)
        with scope('y_wait'):
            to_y(q).wait_recv()
        val = part[lax.rem(q, part.shape[0])] + y_in[lax.rem(q, y_in.shape[0])].astype(f32)

        @pl.when(jj == n_z - 1)
        def _():
            z_own[xi] = val

        @pl.when(jj < n_z - 1)
        def _():
            @pl.when(q >= n_z)
            def _():
                to_z(q - n_z).wait_send()
            z_out[jj] = val.astype(bf16)
            to_z(q).start()

    def z_sum(r, xi):
        val = z_own[xi]
        for jj in range(n_z - 1):
            rcopy(z_out.at[0], z_in.at[r, xi, jj], zz_s.at[jj], zz_r.at[r, xi, jj], sibling).wait_recv()
            val = val + z_in[r, xi, jj].astype(f32)
        return val

    def x_stage(r):
        @pl.when(r > 0)
        def _():
            to_x(0).wait_send()
        with scope('x_stage'):
            x_out[...] = z_sum(r, 0).astype(bf16)
        to_x(r).start()

    def home(tp, r):
        return gh_hbm.at[pl.ds(pl.multiple_of(tp * own + r * half, half), half), :]

    def gathers(r):
        out = [rcopy(gh.at[r], home(at.tp, r), ag_s.at[r, n_z - 1], fw_r.at[r, at.z], y_peer)]
        for jj in (0, 2, 1):
            if jj >= n_z - 1:
                continue
            to = lax.rem(at.z + jj + 1, n_z)
            out.append(rcopy(gh.at[r], home(at.tp, r), ag_s.at[r, jj], ag_r.at[r, jj], dev(to * 2 + at.y, me)))
        return out

    def keep(r):
        return pltpu.make_async_copy(gh.at[r], home(at.tp, r), gh_sem.at[r])

    def arrived(r, jj):
        return rcopy(gh.at[r], home(z_from(jj) * 2 + at.y, r), ag_s.at[r, jj], ag_r.at[r, jj], sibling)

    def onward(r, jj):
        here = home(z_from(jj) * 2 + at.y, r)
        return rcopy(here, here, fw_s.at[r, jj], fw_r.at[r, z_from(jj)], y_peer)

    def tell_gain(k):
        tp, f = at.other(k)
        return rcopy(gg, gg_in.at[at.index], gain_s.at[k], gain_r.at[k], dev(tp, f))

    def heard_gain(k):
        i = lax.rem(at.index + at.n_all - k, at.n_all)
        return rcopy(gg, gg_in.at[i], gain_s.at[k], gain_r.at[k], sibling)

    def final(r):
        with scope('final_wait'):
            to_x(r).wait_recv()
            dz = z_sum(r, 1) + x_in[r].astype(f32)
        h = hid[pl.ds(pl.multiple_of(r * half, half), half), :].astype(f32)
        inv = lax.rsqrt(jnp.mean(h * h, axis=-1, keepdims=True) + NORM_EPS)
        normed = h * inv
        a = dz * gain[...].astype(f32)[None, :]
        gh[r] = (inv * (a - normed * jnp.mean(a * normed, axis=-1, keepdims=True))).astype(bf16)
        gg[0:1, 0:d] += jnp.sum(dz * normed, axis=0, keepdims=True)
        if r == 1:
            hits = jnp.sum(jnp.sum(hit[...], axis=0, keepdims=True), axis=1, keepdims=True)
            gg[0:1, d:] = jnp.broadcast_to(hits, (1, gg.shape[1] - d))
            at.every(lambda k: tell_gain(k).start())
            gg_in[at.index] = gg[...]
        keep(r).start()
        if r == 1:
            gather_start(1)

    def gather_start(r):
        for cp in gathers(r):
            cp.start()

    def forward(r, jj):
        with scope('fw_wait'):
            arrived(r, jj).wait_recv()
        onward(r, jj).start()

    h_load.wait()
    gg[...] = jnp.zeros(gg.shape, f32)

    def dz_round(r, e):
        lo, hi = r * groups, (r + 1) * groups
        for b in (0, 1):
            for cp in block_loads(lo, b, e):
                cp.start()

        def dz_group(q, _):
            for b in (0, 1):
                with scope('a_wait'):
                    for cp in block_loads(q, b, e):
                        cp.wait()

                    @pl.when(q > lo)
                    def _():
                        for cp in block_saves(q - 1, b, e):
                            cp.wait()
                slot = lax.rem(q, 2)
                if b == 0:
                    @pl.when(q >= 2)
                    def _():
                        to_sib(q - 2).wait_send()
                    with scope('a_dot0'):
                        sib_out[slot] = block_dot(q, b, e).astype(bf16)
                    to_sib(q).start()
                else:
                    @pl.when(q >= 2)
                    def _():
                        to_y(q - 2).wait_send()
                    with scope('a_dot1'):
                        val = block_dot(q, b, e)
                        y_sum[...] = val[0:half]
                        part[lax.rem(q, part.shape[0])] = val[half:]
                    with scope('sib_wait'):
                        to_sib(q).wait_recv()
                    y_out[slot] = (y_sum[...] + sib_in[slot, 0:half].astype(f32)).astype(bf16)
                    part[lax.rem(q, part.shape[0])] += sib_in[slot, half:].astype(f32)
                    to_y(q).start()
                for cp in block_saves(q, b, e):
                    cp.start()

                @pl.when(q + 1 < hi)
                def _():
                    for cp in block_loads(q + 1, b, e):
                        cp.start()

            @pl.when(q == lo)
            def _():
                flush(e - 1, chunk)

            @pl.when(q >= lo + 2)
            def _():
                z_stage(q - 2)
            if r == 0:
                @pl.when(q == hi - 1)
                def _():
                    z_stage(q - 1)
            return 0

        lax.fori_loop(lo, hi, dz_group, 0)
        for b in (0, 1):
            for cp in block_saves(hi - 1, b, e):
                cp.wait()

    dz_round(0, early[0])
    for b in range(4):
        load_l(early[0] * chunk, chunk, b, b).start()

    def between(c):
        @pl.when(c == early[0])
        def _():
            z_stage(groups - 1)
            x_stage(0)
            if early[1] - early[0] == 1:
                final(0)
                gather_start(0)

        if early[1] - early[0] > 1:
            @pl.when(c == early[0] + 1)
            def _():
                final(0)
                gather_start(0)

    early_chunks(early[0], early[1], 1, between)
    dz_round(1, early[1])
    z_stage(last - 2)

    for b in range(4):
        load_g(early[1] * chunk, chunk, b, b).start()

    quads = n_tok // 4
    nearest = [jj for jj in (2, 0, 1) if jj < n_z - 1]
    steps = [(t // 2, 0, jj) for t, jj in enumerate(nearest)] + [(6 + t, 1, jj) for t, jj in enumerate(nearest)]

    def late_chunk(c, _):
        def quad(i, _):
            for b in range(4):
                k = 4 * i + b
                with scope('b2_wait'):
                    load_g(0, chunk, 0, b).wait()
                with scope('b2_tile'):
                    grad_tile(c * chunk, chunk, k, b, False)
                wrap = k + 4 >= n_tok
                c2, k2 = jnp.where(wrap, c + 1, c), jnp.where(wrap, k + 4 - n_tok, k + 4)

                @pl.when(c2 < sz.full)
                def _():
                    load_g(c2 * chunk, chunk, k2, b).start()

                @pl.when(c2 == sz.full)
                def _():
                    load_g(row_rem, sz.rem, k2, b).start()
                if b == 0:
                    @pl.when(jnp.logical_and(i == 0, c > early[1]))
                    def _():
                        flush(c - 1, chunk)

            for t, r, jj in steps:
                @pl.when((c - early[1]) * quads + i == t)
                def _():
                    forward(r, jj)
            return 0
        lax.fori_loop(0, quads, quad, 0)
        ship(c, chunk)

        @pl.when(c == early[1])
        def _():
            z_stage(last - 1)
            x_stage(1)

        @pl.when(c == early[1] + 1)
        def _():
            final(1)
        return 0

    lax.fori_loop(early[1], sz.full, late_chunk, 0)
    def late_rem(i, _):
        for b in range(4):
            with scope('b2_wait'):
                load_g(row_rem, sz.rem, 0, b).wait()
            with scope('b2_rem'):
                grad_tile(row_rem, sz.rem, 4 * i + b, b, False)

            @pl.when(4 * i + b + 4 < n_tok)
            def _():
                load_g(row_rem, sz.rem, 4 * i + b + 4, b).start()
            if b == 0:
                @pl.when(i == 0)
                def _():
                    flush(sz.full - 1, chunk)
        return 0

    lax.fori_loop(0, n_tok // 4, late_rem, 0)
    ship(sz.full, sz.rem)
    flush(sz.full, sz.rem)
    for t, r, jj in steps:
        if t >= (sz.full - early[1]) * quads:
            forward(r, jj)

    with scope('t_gain'):
        at.every(lambda k: heard_gain(k).wait_recv())
    total = jnp.sum(gg_in[...], axis=0)
    gg_out[0:1, 0:d] = total[0:1, 0:d]
    gg_out[0:1, d:] = (jnp.sum(st[...] * scale[...], axis=1, keepdims=True) - total[0:1, d:]) * (1.0 / LOG2E)
    with scope('t_small'):
        at.every(lambda k: ask(k).wait_send())
        at.every(lambda k: answer(k).wait_send())
        at.every(lambda k: tell_gain(k).wait_send())
        for k in range(1, n):
            for cp in tok_out(k):
                cp.wait_send()
        block_out().wait_send()
        for p in (0, 1):
            h_to_x(p).wait_send()
            for jj in range(n_z - 1):
                h_to_z(jj, p).wait_send()
        for zo in range(n_z):
            h_to_y(zo).wait_send()
        for tp in range(n_tp):
            h_to_core(tp).wait_send()

        def w_sent(c, _):
            for k in range(1, n):
                remote(k, c, c * chunk, chunk).wait_send()
            return 0

        lax.fori_loop(0, sz.full, w_sent, 0)
        for k in range(1, n):
            remote(k, sz.full, row_rem, sz.solid).wait_send()
            when_not_last(lax.rem(me + k, n), lambda: remote(k, sz.full + 1, row_odd, sz.short).wait_send())
        for q in (last - 2, last - 1):
            to_sib(q).wait_send()
            to_y(q).wait_send()
        for q in range(last - n_z, last - 1):
            to_z(q).wait_send()
        to_x(1).wait_send()
    with scope('t_send'):
        def sent(c, _):
            for cp in sends(c, chunk):
                cp.wait_send()
            return 0
        lax.fori_loop(0, sz.full, sent, 0)
        for cp in sends(sz.full, sz.rem):
            cp.wait_send()
    for r in range(ROUNDS):
        with scope(f't_gather{r}'):
            keep(r).wait()
            for cp in gathers(r):
                cp.wait_send()
            for jj in range(n_z - 1):
                onward(r, jj).wait_send()
            for zo in range(n_z):
                rcopy(gh.at[r], home(zo * 2 + 1 - at.y, r), ag_s.at[r, 0], fw_r.at[r, zo], y_peer).wait_recv()
    with scope('t_dw'):
        for k in range(1, n):
            src = lax.rem(me + n - k, n)
            rcopy(dw_hbm.at[pl.ds(0, sz.rows), :], dw_hbm.at[rows_at(src * sz.rows, sz.rows), :], dw_send.at[0, 0], dw_recv.at[k], sibling).wait_recv()


HBM = pl.BlockSpec(memory_space=pl.ANY)
VM = pl.BlockSpec(memory_space=pltpu.VMEM)
DMA = pltpu.SemaphoreType.DMA


def solution(mesh, chunk=CHUNK, tok=TOK, early=EARLY):
    n_fsdp, n_tp = mesh.shape['fsdp'], mesh.shape['tp']
    n_all, n_z = n_fsdp * n_tp, n_tp // 2
    S, V = jax.ShapeDtypeStruct, pltpu.VMEM
    i32 = jnp.int32

    def per_device(hidden, labels, tok_mask, norm_gain, w_rows):
        per_f, d = hidden.shape
        width, vocab_tp = w_rows.shape
        tokens, own = per_f * n_fsdp, per_f // n_tp
        half = own // ROUNDS
        sz = Sizes(vocab_tp, n_fsdp, chunk)
        n_low = sz.full - early[0] + 1

        dw_t, grad_hidden, sums, *_ = pl.pallas_call(
            functools.partial(head_kernel, sz, n_tp, vocab_tp, chunk, tok, early),
            out_shape=(S((n_fsdp * sz.rows, width), bf16), S(hidden.shape, bf16), S((1, d + 128), f32),
                       S((sz.rows, tokens), f32), S((sz.rows, tokens), bf16), S((tokens, d), bf16), S(((sz.full + 1) * chunk, d), bf16)),
            in_specs=[HBM, VM, VM, VM, HBM], out_specs=(HBM, HBM, VM, HBM, HBM, HBM, HBM),
            scratch_shapes=[
                V((tokens, d), bf16), V((sz.rows, d), bf16), *[V((chunk, tok), f32)] * 4, *[V((chunk, tok), bf16)] * 4, *[V((sz.rows, 2 * half), bf16)] * 2,
                V((8, tokens), f32), V((8, tokens), f32), V((1, tokens), f32), V((1, tokens), i32), V((n_fsdp, 1, per_f), i32), V((n_fsdp, 1, per_f), f32),
                V((2, tokens), f32), V((n_all, 2, own), f32), V((1, own), f32), V((1, tokens), f32), V((1, tokens), f32), V((8, min(128, half)), f32), V((own, d), bf16),
                V((chunk, d), f32), V((2, chunk, d), bf16), V((2, 2 * half, d), bf16), V((2, 2 * half, d), bf16), V((half, d), f32),
                V((2, half, d), bf16), V((6, half, d), bf16), V((3, half, d), f32), V((n_z - 1, half, d), bf16), V((ROUNDS, 2, n_z - 1, half, d), bf16), V((2, half, d), f32),
                V((half, d), bf16), V((ROUNDS, half, d), bf16), V((ROUNDS, half, d), bf16), V((1, d + 128), f32), V((n_all, 1, d + 128), f32),
                DMA((sz.full + 2, n_fsdp)), DMA((sz.full + 2, n_fsdp)), DMA((sz.full + 2,)), DMA((per_f // min(256, own),)), DMA((4,)), DMA((4,)), DMA((2, 2)), DMA((2, 2 * n_low)), DMA((2, 2)),
                DMA((n_all,)), DMA((n_all,)), DMA((n_all,)), DMA((n_all,)), DMA((2, n_fsdp)), DMA((2, n_fsdp)), DMA((2,)), DMA((2,)), DMA((2,)),
                DMA((n_z - 1, 2)), DMA((n_z - 1, 2)), DMA((n_z,)), DMA((n_z,)), DMA((n_tp,)), DMA((n_tp,)),
                DMA((1,)), DMA((2,)), DMA((sz.full + 1, 3)), DMA((n_fsdp,)), DMA((2,)), DMA((2,)), DMA((2,)), DMA((2,)), DMA((8,)),
                DMA((n_z - 1,)), DMA((ROUNDS, 2, n_z - 1)), DMA((1,)), DMA((ROUNDS,)),
                DMA((ROUNDS, n_z)), DMA((ROUNDS, n_z)), DMA((ROUNDS, n_z)), DMA((ROUNDS, n_z)), DMA((ROUNDS,)), DMA((n_all,)), DMA((n_all,))],
            compiler_params=pltpu.CompilerParams(vmem_limit_bytes=VMEM_LIMIT, collective_id=0, has_side_effects=True), name='head',
        )(hidden, labels[None, :], tok_mask[None, :], norm_gain, w_rows.T)
        return sums[0, d], grad_hidden, dw_t[:vocab_tp].T, sums[0, :d]

    return jax.shard_map(per_device, mesh=mesh, in_specs=(P('fsdp', None), P('fsdp'), P('fsdp'), P(), P('fsdp', 'tp')), out_specs=(P(), P('fsdp', None), P('fsdp', 'tp'), P()), check_vma=False)
```

```python
import functools

import jax
import jax.numpy as jnp
from jax import lax
from jax.experimental import pallas as pl
from jax.experimental.pallas import tpu as pltpu
from jax.sharding import PartitionSpec as P

NORM_EPS = 1e-6
LOG2E = 1.4426950408889634
NEG = -1e30
CHUNK = 512
TOK = 1024
EARLY = (3, 5)
AHEAD = 5
ROUNDS = 2
VMEM_LIMIT = 67_043_328
MESH = pl.DeviceIdType.MESH
scope = jax.named_scope
f32, bf16 = jnp.float32, jnp.bfloat16


def dot_nt(a, b):
    return lax.dot_general(a, b, (((1,), (1,)), ((), ())), preferred_element_type=f32)


def dot_tn(a, b):
    return lax.dot_general(a, b, (((0,), (0,)), ((), ())), preferred_element_type=f32)


def dot_nn(a, b):
    return lax.dot_general(a, b, (((1,), (0,)), ((), ())), preferred_element_type=f32)


def cols(k, size):
    return pl.ds(pl.multiple_of(k * size, size), size)


def rows_at(row0, rows):
    return pl.ds(pl.multiple_of(row0, 16), rows)


class Sizes:
    def __init__(self, vocab_tp, n_fsdp, chunk):
        self.n = n_fsdp
        self.rows = -(-vocab_tp // (n_fsdp * 16)) * 16
        self.short = n_fsdp * self.rows - vocab_tp
        self.full = self.rows // chunk
        self.rem = self.rows - self.full * chunk
        self.solid = self.rem - self.short
        assert self.rem > self.short and self.rem % 16 == 0 and self.short % 16 == 0


class Place:
    def __init__(self, n_fsdp, n_tp):
        self.n_fsdp, self.n_tp, self.n_all = n_fsdp, n_tp, n_fsdp * n_tp
        self.f, self.tp = lax.axis_index('fsdp'), lax.axis_index('tp')
        self.x, self.c = self.f // 2, lax.rem(self.f, 2)
        self.n_z = n_tp // 2
        self.z, self.y = self.tp // 2, lax.rem(self.tp, 2)
        self.index = self.tp * n_fsdp + self.f

    def other(self, k):
        i = lax.rem(self.index + k, self.n_all)
        return i // self.n_fsdp, lax.rem(i, self.n_fsdp)

    def every(self, fn):
        def go(k, _):
            fn(k)
            return 0
        lax.fori_loop(1, self.n_all, go, 0)


def dev(tp, f):
    return {'tp': tp, 'fsdp': f}


def rcopy(src, dst, ssem, rsem, to):
    return pltpu.make_async_remote_copy(src_ref=src, dst_ref=dst, send_sem=ssem, recv_sem=rsem, device_id=to, device_id_type=MESH)


def enter(at):
    barrier = pltpu.get_barrier_semaphore()

    def tell(k):
        tp, f = at.other(k)
        pl.semaphore_signal(barrier, inc=1, device_id=dev(tp, f), device_id_type=MESH)

    at.every(tell)
    pl.semaphore_wait(barrier, at.n_all - 1)


def head_kernel(sz, n_tp, vocab_tp, chunk, tok, early,
                h_hbm, lab_ref, mask_ref, gain, w_hbm,
                dw_hbm, gh_hbm, gg_out, l_hbm, g_hbm, h_all, ds_hbm,
                z, w, l0, l1, l2, l3, g0, g1, g2, g3, q0, q1, m, s, scale, lab, lab_in, mask_in, st_loc, got, res, st, top_row, hit, hid,
                acc, stage, sib_out, sib_in, y_sum, y_out, y_in, part, z_out, z_in, z_own, x_out, x_in, gh, gg, gg_in,
                w_s, w_r, loc, hsem, lsem, gsem, qsem, bsem, vsem, ssend, srecv, rsend, rrecv, tok_s, tok_r, blk, hx_s, hx_r, hz_s, hz_r, hy_s, hy_r, hc_s, hc_r,
                hid_sem, dw_copy, dw_send, dw_recv, own_sem, sib_s, sib_r, y_s, y_r, zz_s, zz_r, x_s, x_r, ag_s, ag_r, fw_s, fw_r, gh_sem, gain_s, gain_r):
    at = Place(sz.n, n_tp)
    me, n, n_z, width = at.f, sz.n, at.n_z, w_hbm.shape[1]
    per_f, d = h_hbm.shape
    tokens, own = per_f * n, per_f // n_tp
    lbufs, gbufs, qbufs = (l0, l1, l2, l3), (g0, g1, g2, g3), (q0, q1)
    far, sib = 1 - at.x, at.x * 2 + 1 - at.c
    through = far * 2 + at.c
    sibling, y_peer, x_peer = dev(at.tp, sib), dev(at.z * 2 + 1 - at.y, me), dev(at.tp, through)
    row_rem = sz.full * chunk
    row_odd = row_rem + sz.solid

    with scope('enter'):
        enter(at)

    def slab(f, tp):
        return pl.ds(pl.multiple_of((f * n_tp + tp) * own, own), own)

    def block(f):
        return pl.ds(pl.multiple_of(f * per_f, per_f), per_f)

    own2 = own // 2

    def part_of(f, tp, p):
        return pl.ds(pl.multiple_of((f * n_tp + tp) * own + p * own2, own2), own2)

    def h_to_x(p):
        return rcopy(h_hbm.at[pl.ds(pl.multiple_of(at.tp * own + p * own2, own2), own2), :], h_all.at[part_of(me, at.tp, p), :], hx_s.at[p], hx_r.at[p], x_peer)

    def h_from_x(p):
        here = h_all.at[part_of(through, at.tp, p), :]
        return rcopy(here, here, hx_s.at[p], hx_r.at[p], x_peer)

    def block_out():
        return rcopy(h_hbm, h_all.at[block(me), :], blk.at[0], blk.at[1], sibling)

    def block_in():
        return rcopy(h_hbm, h_all.at[block(sib), :], blk.at[0], blk.at[1], sibling)

    def moved(tp, ssem, rsem, to):
        here = h_all.at[slab(through, tp), :]
        return rcopy(here, here, ssem, rsem, to)

    def z_from(jj):
        return lax.rem(at.z + n_z - jj - 1, n_z)

    def h_to_z(jj, p):
        here = h_all.at[part_of(through, at.tp, p), :]
        return rcopy(here, here, hz_s.at[jj, p], hz_r.at[jj, p], dev(lax.rem(at.z + jj + 1, n_z) * 2 + at.y, me))

    def h_from_z(jj, p):
        here = h_all.at[part_of(through, z_from(jj) * 2 + at.y, p), :]
        return rcopy(here, here, hz_s.at[jj, p], hz_r.at[jj, p], sibling)

    def h_to_y(zo):
        return moved(zo * 2 + at.y, hy_s.at[zo], hy_r.at[zo], y_peer)

    def h_from_y(zo):
        return moved(zo * 2 + 1 - at.y, hy_s.at[zo], hy_r.at[zo], y_peer)

    def h_to_core(tp):
        return moved(tp, hc_s.at[tp], hc_r.at[tp], sibling)

    def h_from_core(tp):
        here = h_all.at[slab(far * 2 + 1 - at.c, tp), :]
        return rcopy(here, here, hc_s.at[tp], hc_r.at[tp], sibling)

    def tok_out(k):
        to = dev(at.tp, lax.rem(me + k, n))
        return [rcopy(lab_ref, lab_in.at[me], tok_s.at[0, k], tok_r.at[0, k], to), rcopy(mask_ref, mask_in.at[me], tok_s.at[1, k], tok_r.at[1, k], to)]

    def tok_in(k):
        src = lax.rem(me + n - k, n)
        return [rcopy(lab_ref, lab_in.at[src], tok_s.at[0, k], tok_r.at[0, k], sibling), rcopy(mask_ref, mask_in.at[src], tok_s.at[1, k], tok_r.at[1, k], sibling)]

    for p in (0, 1):
        h_to_x(p).start()
    block_out().start()
    for k in range(1, n):
        for cp in tok_out(k):
            cp.start()
    lab_in[me] = lab_ref[...]
    mask_in[me] = mask_ref[...]

    def remote(k, c, row0, rows):
        dest = lax.rem(me + k, n)
        return rcopy(w_hbm.at[rows_at(dest * sz.rows + row0, rows), :], w.at[rows_at(row0, rows), cols(me, width)], w_s.at[c, k], w_r.at[c, k], dev(at.tp, dest))

    def arrival(k, c, row0, rows):
        src = lax.rem(me + n - k, n)
        return rcopy(w_hbm.at[pl.ds(0, rows), :], w.at[rows_at(row0, rows), cols(src, width)], w_s.at[c, k], w_r.at[c, k], sibling)

    def local(c, row0, rows):
        return pltpu.make_async_copy(w_hbm.at[rows_at(me * sz.rows + row0, rows), :], w.at[rows_at(row0, rows), cols(me, width)], loc.at[c])

    def issue(c):
        local(c, c * chunk, chunk).start()
        for k in range(1, n):
            remote(k, c, c * chunk, chunk).start()

    def when_not_last(dest, fn):
        if sz.short:
            pl.when(dest != n - 1)(fn)

    def issue_rem():
        local(sz.full, row_rem, sz.solid).start()
        when_not_last(me, lambda: local(sz.full + 1, row_odd, sz.short).start())
        for k in range(1, n):
            remote(k, sz.full, row_rem, sz.solid).start()
            when_not_last(lax.rem(me + k, n), lambda: remote(k, sz.full + 1, row_odd, sz.short).start())

    ahead = min(AHEAD, sz.full)
    for c in range(ahead):
        issue(c)
    if sz.short:
        @pl.when(me == n - 1)
        def _():
            w[row_odd:, :] = jnp.zeros((sz.short, d), bf16)

    sub = min(256, own)
    slices, per_own = per_f // sub, own // sub
    lane = min(128, sub)

    def place(t, i):
        near = jnp.where(t == 0, me, sib) * per_f + i * sub
        j = i // per_own
        f = jnp.where(j < n_z, through, far * 2 + 1 - at.c)
        y = jnp.where(t == 2, at.y, 1 - at.y)
        away = (f * n_tp + lax.rem(j, n_z) * 2 + y) * own + lax.rem(i, per_own) * sub
        return pl.multiple_of(jnp.where(t < 2, near, away), sub)

    def norm(t):
        def load(i):
            here = pl.ds(place(t, i), sub)
            return pltpu.make_async_copy(h_hbm.at[cols(i, sub), :] if t == 0 else h_all.at[here, :], z.at[here, :], hsem.at[i])

        def begin(i, _):
            load(i).start()
            return 0

        def one(i, _):
            load(i).wait()
            here = pl.ds(place(t, i), sub)
            h = z[here, :].astype(f32)
            inv = lax.rsqrt(jnp.mean(h * h, axis=-1, keepdims=True) + NORM_EPS)
            z[here, :] = (h * inv * gain[...].astype(f32)[None, :]).astype(bf16)
            return 0

        with scope(f'norm{t}'):
            lax.fori_loop(0, slices, begin, 0)
            lax.fori_loop(0, slices, one, 0)

    def spread_x(p):
        with scope('x_wait'):
            h_from_x(p).wait_recv()
        for jj in (2, 0, 1):
            if jj < n_z - 1:
                h_to_z(jj, p).start()

    norm(0)
    spread_x(0)
    with scope('blk_wait'):
        block_in().wait_recv()
    norm(1)
    spread_x(1)
    h_to_y(at.z).start()
    h_to_core(at.tp).start()
    with scope('tok_wait'):
        for k in range(1, n):
            for cp in tok_in(k):
                cp.wait_recv()
    count = jnp.sum(mask_in[...], axis=(0, 2), keepdims=True)[0]
    for f in range(n):
        here = pl.ds(f * per_f, per_f)
        scale[0:1, here] = mask_in[f] / count
        rel = lab_in[f] - at.tp * vocab_tp
        lab[0:1, here] = jnp.where(jnp.logical_and(rel >= 0, rel < vocab_tp), rel - me * sz.rows, -1)

    def spread_z():
        with scope('z_wait'):
            for jj in range(n_z - 1):
                for p in (0, 1):
                    h_from_z(jj, p).wait_recv()
                h_to_y(z_from(jj)).start()
                h_to_core(z_from(jj) * 2 + at.y).start()

    def spread_y():
        with scope('hy_wait'):
            for k in range(n_z):
                zo = lax.rem(at.z + n_z - k, n_z)
                h_from_y(zo).wait_recv()
                h_to_core(zo * 2 + 1 - at.y).start()

    def far_ready(y):
        with scope('core_wait'):
            for zo in range(n_z):
                h_from_core(zo * 2 + y).wait_recv()

    m[...] = jnp.full(m.shape, NEG, f32)
    s[...] = jnp.zeros(s.shape, f32)
    per_buf = tok // sub
    n_buf = slices // per_buf

    def out_copies(row0, rows, t, b):
        return [pltpu.make_async_copy(lbufs[b * n_buf + i // per_buf].at[pl.ds(0, rows), pl.ds(i % per_buf * sub, sub)],
                                      l_hbm.at[rows_at(row0, rows), pl.ds(place(t, i), sub)], lsem.at[b * n_buf + i // per_buf]) for i in range(slices)]

    def out_done(rows, b):
        for i in range(n_buf):
            pltpu.make_async_copy(lbufs[b * n_buf + i].at[pl.ds(0, rows), :], l_hbm.at[pl.ds(0, rows), pl.ds(0, tok)], lsem.at[b * n_buf + i]).wait()

    def statistics(read, rows, t0):
        group = min(4, rows // 8)
        for c1 in range(0, sub, lane):
            sl = pl.ds(pl.multiple_of(t0 + c1, lane), lane)
            big, tot = m[:, sl], s[:, sl]
            for g in range(0, rows // 8, group):
                piece = [read(r, c1) for r in range(g, min(g + group, rows // 8))]
                new = functools.reduce(jnp.maximum, piece, big)
                tot = tot * jnp.exp2(big - new)
                for x in piece:
                    tot += jnp.exp2(x - new)
                big = new
            m[:, sl], s[:, sl] = big, tot

    def slice_at(b, i):
        return lbufs[b * n_buf + i // per_buf], i % per_buf * sub

    def late_statistics(t, b):
        for i in range(slices - lag, slices):
            buf, i0 = slice_at(b, i)
            statistics(lambda r, c1: buf[8 * r:8 * r + 8, i0 + c1:i0 + c1 + lane], chunk, place(t, i))

    def logits_tile(row0, rows, t, b, masked):
        for i in range(slices):
            t0 = place(t, i)
            logits = dot_nt(w[rows_at(row0, rows), :], z[pl.ds(t0, sub), :]) * LOG2E
            if masked:
                ids = lax.broadcasted_iota(jnp.int32, (rows, sub), 0)
                logits = jnp.where(ids < jnp.where(me == n - 1, sz.solid, sz.rem), logits, NEG)
            buf, i0 = slice_at(b, i)
            buf[0:rows, i0:i0 + sub] = logits
            if masked or i < slices - lag:
                statistics(lambda r, c1: logits[8 * r:8 * r + 8, c1:c1 + lane], rows, t0)

    lag = 2
    for i in range(slices - lag, slices):
        buf, i0 = slice_at(1, i)
        buf[:, i0:i0 + sub] = jnp.full((chunk, sub), NEG, f32)

    n_a = min(3, sz.full)
    n_c = min(3, sz.full - n_a)
    k_b, k_c = 2 * n_a, 3 * n_a
    k_d = k_c + 3 * n_c
    k_e = k_d + n_a + n_c

    def item(k):
        u, v = k - k_c, k - k_e
        c = jnp.where(k < k_b, k // 2, jnp.where(k < k_c, k - k_b, jnp.where(k < k_d, n_a + u // 3, jnp.where(k < k_e, k - k_d, n_a + n_c + v // 4))))
        t = jnp.where(k < k_b, lax.rem(k, 2), jnp.where(k < k_c, 2, jnp.where(k < k_d, lax.rem(u, 3), jnp.where(k < k_e, 3, lax.rem(v, 4)))))
        return c, t

    def work(i2, _):
        for b in (0, 1):
            k = 2 * i2 + b
            c, t = item(k)

            @pl.when(t == 0)
            def _():
                with scope('w_wait'):
                    local(c, c * chunk, chunk).wait()
                    for j in range(1, n):
                        arrival(j, c, c * chunk, chunk).wait_recv()

                @pl.when(c + ahead < sz.full)
                def _():
                    issue(c + ahead)

                @pl.when(c + ahead == sz.full)
                def _():
                    issue_rem()

            @pl.when(k == k_b)
            def _():
                spread_z()
                far_ready(at.y)
                norm(2)

            @pl.when(k == max(k_d - 3, k_c))
            def _():
                spread_y()

            @pl.when(k == k_d)
            def _():
                far_ready(1 - at.y)
                norm(3)

            with scope('l_wait'):
                @pl.when(k >= 2)
                def _():
                    out_done(chunk, b)
            with scope('l_tile'):
                late_statistics(item(jnp.maximum(k - 1, 0))[1], 1 - b)
                logits_tile(c * chunk, chunk, t, b, False)
            for cp in out_copies(c * chunk, chunk, t, b):
                cp.start()
        return 0

    lax.fori_loop(0, sz.full * 2, work, 0)
    late_statistics(item(4 * sz.full - 1)[1], 1)
    with scope('w_wait_rem'):
        local(sz.full, row_rem, sz.solid).wait()
        when_not_last(me, lambda: local(sz.full + 1, row_odd, sz.short).wait())
        for k in range(1, n):
            arrival(k, sz.full, row_rem, sz.solid).wait_recv()
            when_not_last(me, lambda: arrival(k, sz.full + 1, row_odd, sz.short).wait_recv())

    def work_rem(i2, _):
        for b in (0, 1):
            @pl.when(i2 == 0)
            def _():
                out_done(chunk, b)

            @pl.when(i2 > 0)
            def _():
                out_done(sz.rem, b)
            logits_tile(row_rem, sz.rem, 2 * i2 + b, b, True)
            for cp in out_copies(row_rem, sz.rem, 2 * i2 + b, b):
                cp.start()
        return 0

    with scope('l_rem'):
        lax.fori_loop(0, 2, work_rem, 0)

    big = jnp.max(m[...], axis=0, keepdims=True)
    st_loc[0:1, :] = big
    st_loc[1:2, :] = jnp.sum(s[...] * jnp.exp2(m[...] - big), axis=0, keepdims=True)
    mine = slab(at.f, at.tp)

    def ask(k):
        tp, f = at.other(k)
        return rcopy(st_loc.at[:, slab(f, tp)], got.at[k], ssend.at[k], srecv.at[k], dev(tp, f))

    def answer(k):
        tp, f = at.other(k)
        return rcopy(res, st.at[:, mine], rsend.at[k], rrecv.at[k], dev(tp, f))

    def answered(k):
        tp, f = at.other(at.n_all - k)
        return rcopy(res, st.at[:, slab(f, tp)], rsend.at[k], rrecv.at[k], dev(tp, f))

    n_tok = tokens // tok

    def load_l(row0, rows, k, b):
        return pltpu.make_async_copy(l_hbm.at[rows_at(row0, rows), cols(k, tok)], lbufs[b].at[pl.ds(0, rows), :], lsem.at[b])

    def load_g(row0, rows, k, b):
        return pltpu.make_async_copy(g_hbm.at[rows_at(row0, rows), cols(k, tok)], gbufs[b].at[pl.ds(0, rows), :], gsem.at[b])

    def save_g(row0, rows, k, b):
        return pltpu.make_async_copy(gbufs[b].at[pl.ds(0, rows), :], g_hbm.at[rows_at(row0, rows), cols(k, tok)], gsem.at[b])

    at.every(lambda k: ask(k).start())
    got[0] = st_loc[:, mine]
    for b in (0, 1):
        out_done(sz.rem, b)
    for b in range(4):
        load_l(0, chunk, b, b).start()
    h_load = pltpu.make_async_copy(h_hbm.at[pl.ds(pl.multiple_of(at.tp * own, own), own), :], hid, hid_sem.at[0])
    h_load.start()
    acc[...] = jnp.zeros(acc.shape, f32)
    hit[...] = jnp.zeros(hit.shape, f32)
    with scope('ask_wait'):
        at.every(lambda k: ask(k).wait_recv())
    tops = got[:, 0:1, :]
    top = jnp.max(tops, axis=0)
    res[...] = top + jnp.log2(jnp.sum(got[:, 1:2, :] * jnp.exp2(tops - top[None]), axis=0))
    at.every(lambda k: answer(k).start())
    st[:, mine] = res[...]
    with scope('answer_wait'):
        at.every(lambda k: answered(k).wait_recv())
    top_row[...] = st[...] - jnp.log2(scale[...])

    def gradient(x, sl, row0, count=True):
        rows = x.shape[0]
        sc = scale[0:1, sl]
        x3 = x.reshape(rows // 8, 8, x.shape[1])
        p = jnp.exp2(x3 - top_row[0:1, sl][None])
        is_label = lax.broadcasted_iota(jnp.int32, p.shape, 0) * 8 == (lab[0:1, sl] - row0 - lax.broadcasted_iota(jnp.int32, (8, x.shape[1]), 0))[None]
        if count:
            hit[...] += jnp.sum(jnp.where(is_label, x3, 0.0), axis=0) * sc
        return jnp.where(is_label, p - sc[None], p).reshape(x.shape).astype(bf16)

    step = min(256, tok)

    half = own // ROUNDS

    def grad_tile(row0, rows, k, b, fresh, first_round=0):
        total = None
        for c0 in range(0, tok, step):
            if fresh:
                for c1 in range(c0, c0 + step, lane):
                    gbufs[b][0:rows, c1:c1 + lane] = gradient(lbufs[b][0:rows, c1:c1 + lane], pl.ds(pl.multiple_of(k * tok + c1, lane), lane), row0, c1 % own // half >= first_round)
            p = dot_nn(gbufs[b][0:rows, c0:c0 + step], z[pl.ds(pl.multiple_of(k * tok + c0, step), step), :])
            total = p if total is None else total + p
        acc[0:rows, :] += total

    def aside(c, rows):
        slot = lax.rem(c, 2)
        return pltpu.make_async_copy(stage.at[slot, pl.ds(0, rows), :], ds_hbm.at[rows_at(c * chunk, rows), :], dw_copy.at[slot])

    def keep_own(c, rows):
        slot = lax.rem(c, 2)
        return pltpu.make_async_copy(stage.at[slot, pl.ds(0, rows), cols(me, width)], dw_hbm.at[rows_at(me * sz.rows + c * chunk, rows), :], own_sem.at[slot])

    def sends(c, rows):
        out = []
        for i, f in enumerate((far * 2, far * 2 + 1, sib)):
            out.append(rcopy(ds_hbm.at[rows_at(c * chunk, rows), cols(f, width)], dw_hbm.at[rows_at(me * sz.rows + c * chunk, rows), :],
                             dw_send.at[c, i], dw_recv.at[lax.rem(f + n - me, n)], dev(at.tp, f)))
        return out

    def ship(c, rows):
        with scope('ship'):
            stage[lax.rem(c, 2), 0:rows, :] = acc[0:rows, :].astype(bf16)
            acc[...] = jnp.zeros(acc.shape, f32)
        aside(c, rows).start()
        keep_own(c, rows).start()

    def flush(c, rows):
        aside(c, rows).wait()
        keep_own(c, rows).wait()
        for cp in sends(c, rows):
            cp.start()

    def early_chunks(lo, hi, first_round, after):
        def one(c, _):
            def quad(i, _):
                for b in range(4):
                    k = 4 * i + b
                    with scope('b1_wait'):
                        load_l(0, chunk, 0, b).wait()

                        @pl.when(jnp.logical_not(jnp.logical_and(c == lo, i == 0)))
                        def _():
                            save_g(0, chunk, 0, b).wait()
                    with scope('b1_tile'):
                        grad_tile(c * chunk, chunk, k, b, True, first_round)
                    save_g(c * chunk, chunk, k, b).start()
                    wrap = k + 4 >= n_tok
                    c2 = jnp.where(wrap, c + 1, c)

                    @pl.when(c2 < hi)
                    def _():
                        load_l(c2 * chunk, chunk, jnp.where(wrap, k + 4 - n_tok, k + 4), b).start()

                @pl.when(jnp.logical_and(i == 0, c > lo))
                def _():
                    flush(c - 1, chunk)
                return 0
            lax.fori_loop(0, n_tok // 4, quad, 0)
            ship(c, chunk)
            after(c)
            return 0
        lax.fori_loop(lo, hi, one, 0)
        for b in range(4):
            save_g(0, chunk, 0, b).wait()

    early_chunks(0, early[0], 0, lambda c: None)

    groups = 2 * n_z
    last = ROUNDS * groups

    def low(e):
        return [(j, chunk) for j in range(sz.full - e)] + [(sz.full - e, sz.rem)]
    per_l = tok // half

    def group_of(q):
        r, g = q // groups, lax.rem(q, groups)
        xi, jj = g // n_z, lax.rem(g, n_z)
        return r, xi, jj, jnp.where(xi == 0, far, at.x), lax.rem(at.z + jj + 1, n_z)

    def pieces(q, b):
        r, _, _, xb, zb = group_of(q)
        cb = at.c if b == 1 else 1 - at.c
        return [pl.multiple_of((xb * 2 + cb) * per_f + (zb * 2 + yb) * own + r * half, half) for yb in (1 - at.y, at.y)]

    def l_part(b, j, i, rows):
        p = 2 * j + i
        return lbufs[2 * b + p // per_l].at[pl.ds(0, rows), pl.ds(p % per_l * half, half)]

    def block_loads(q, b, e):
        row_low = e * chunk
        out = []
        for i, t0 in enumerate(pieces(q, b)):
            out.append(pltpu.make_async_copy(g_hbm.at[pl.ds(0, row_low), pl.ds(t0, half)], qbufs[b].at[pl.ds(0, row_low), pl.ds(i * half, half)], qsem.at[b, i]))
            for j, rows in low(e):
                out.append(pltpu.make_async_copy(l_hbm.at[pl.ds(row_low + j * chunk, rows), pl.ds(t0, half)], l_part(b, j, i, rows), bsem.at[b, 2 * j + i]))
        return out

    def block_saves(q, b, e):
        row_low = e * chunk
        return [pltpu.make_async_copy(qbufs[b].at[pl.ds(row_low, sz.rows - row_low), pl.ds(i * half, half)],
                                      g_hbm.at[pl.ds(row_low, sz.rows - row_low), pl.ds(t0, half)], vsem.at[b, i]) for i, t0 in enumerate(pieces(q, b))]

    def block_dot(q, b, e):
        row_low = e * chunk
        for i, t0 in enumerate(pieces(q, b)):
            for j, rows in low(e):
                row0 = row_low + j * chunk
                qbufs[b][row0:row0 + rows, i * half:(i + 1) * half] = gradient(l_part(b, j, i, rows)[...], pl.ds(t0, half), row0)
        return dot_tn(qbufs[b][...], w[...])

    def to_sib(q):
        slot = lax.rem(q, 2)
        return rcopy(sib_out.at[slot], sib_in.at[slot], sib_s.at[slot], sib_r.at[slot], sibling)

    def to_y(q):
        slot, land = lax.rem(q, 2), lax.rem(q, y_in.shape[0])
        return rcopy(y_out.at[slot], y_in.at[land], y_s.at[slot], y_r.at[land], y_peer)

    def to_z(q):
        r, xi, jj, _, zb = group_of(q)
        return rcopy(z_out.at[jj], z_in.at[r, xi, jj], zz_s.at[jj], zz_r.at[r, xi, jj], dev(zb * 2 + at.y, me))

    def to_x(r):
        return rcopy(x_out, x_in.at[r], x_s.at[0], x_r.at[r], x_peer)

    def z_stage(q):
        _, xi, jj, _, _ = group_of(q)
        with scope('y_wait'):
            to_y(q).wait_recv()
        val = part[lax.rem(q, part.shape[0])] + y_in[lax.rem(q, y_in.shape[0])].astype(f32)

        @pl.when(jj == n_z - 1)
        def _():
            z_own[xi] = val

        @pl.when(jj < n_z - 1)
        def _():
            @pl.when(q >= n_z)
            def _():
                to_z(q - n_z).wait_send()
            z_out[jj] = val.astype(bf16)
            to_z(q).start()

    def z_sum(r, xi):
        val = z_own[xi]
        for jj in range(n_z - 1):
            rcopy(z_out.at[0], z_in.at[r, xi, jj], zz_s.at[jj], zz_r.at[r, xi, jj], sibling).wait_recv()
            val = val + z_in[r, xi, jj].astype(f32)
        return val

    def x_stage(r):
        @pl.when(r > 0)
        def _():
            to_x(0).wait_send()
        with scope('x_stage'):
            x_out[...] = z_sum(r, 0).astype(bf16)
        to_x(r).start()

    def home(tp, r):
        return gh_hbm.at[pl.ds(pl.multiple_of(tp * own + r * half, half), half), :]

    def gathers(r):
        out = [rcopy(gh.at[r], home(at.tp, r), ag_s.at[r, n_z - 1], fw_r.at[r, at.z], y_peer)]
        for jj in (0, 2, 1):
            if jj >= n_z - 1:
                continue
            to = lax.rem(at.z + jj + 1, n_z)
            out.append(rcopy(gh.at[r], home(at.tp, r), ag_s.at[r, jj], ag_r.at[r, jj], dev(to * 2 + at.y, me)))
        return out

    def keep(r):
        return pltpu.make_async_copy(gh.at[r], home(at.tp, r), gh_sem.at[r])

    def arrived(r, jj):
        return rcopy(gh.at[r], home(z_from(jj) * 2 + at.y, r), ag_s.at[r, jj], ag_r.at[r, jj], sibling)

    def onward(r, jj):
        here = home(z_from(jj) * 2 + at.y, r)
        return rcopy(here, here, fw_s.at[r, jj], fw_r.at[r, z_from(jj)], y_peer)

    def tell_gain(k):
        tp, f = at.other(k)
        return rcopy(gg, gg_in.at[at.index], gain_s.at[k], gain_r.at[k], dev(tp, f))

    def heard_gain(k):
        i = lax.rem(at.index + at.n_all - k, at.n_all)
        return rcopy(gg, gg_in.at[i], gain_s.at[k], gain_r.at[k], sibling)

    def final(r):
        with scope('final_wait'):
            to_x(r).wait_recv()
            dz = z_sum(r, 1) + x_in[r].astype(f32)
        h = hid[pl.ds(pl.multiple_of(r * half, half), half), :].astype(f32)
        inv = lax.rsqrt(jnp.mean(h * h, axis=-1, keepdims=True) + NORM_EPS)
        normed = h * inv
        a = dz * gain[...].astype(f32)[None, :]
        gh[r] = (inv * (a - normed * jnp.mean(a * normed, axis=-1, keepdims=True))).astype(bf16)
        gg[0:1, 0:d] += jnp.sum(dz * normed, axis=0, keepdims=True)
        if r == 1:
            hits = jnp.sum(jnp.sum(hit[...], axis=0, keepdims=True), axis=1, keepdims=True)
            gg[0:1, d:] = jnp.broadcast_to(hits, (1, gg.shape[1] - d))
            at.every(lambda k: tell_gain(k).start())
            gg_in[at.index] = gg[...]
        keep(r).start()
        if r == 1:
            gather_start(1)

    def gather_start(r):
        for cp in gathers(r):
            cp.start()

    def forward(r, jj):
        with scope('fw_wait'):
            arrived(r, jj).wait_recv()
        onward(r, jj).start()

    h_load.wait()
    gg[...] = jnp.zeros(gg.shape, f32)

    def dz_round(r, e):
        lo, hi = r * groups, (r + 1) * groups
        for b in (0, 1):
            for cp in block_loads(lo, b, e):
                cp.start()

        def dz_group(q, _):
            for b in (0, 1):
                with scope('a_wait'):
                    for cp in block_loads(q, b, e):
                        cp.wait()

                    @pl.when(q > lo)
                    def _():
                        for cp in block_saves(q - 1, b, e):
                            cp.wait()
                slot = lax.rem(q, 2)
                if b == 0:
                    @pl.when(q >= 2)
                    def _():
                        to_sib(q - 2).wait_send()
                    with scope('a_dot0'):
                        sib_out[slot] = block_dot(q, b, e).astype(bf16)
                    to_sib(q).start()
                else:
                    @pl.when(q >= 2)
                    def _():
                        to_y(q - 2).wait_send()
                    with scope('a_dot1'):
                        val = block_dot(q, b, e)
                        y_sum[...] = val[0:half]
                        part[lax.rem(q, part.shape[0])] = val[half:]
                    with scope('sib_wait'):
                        to_sib(q).wait_recv()
                    y_out[slot] = (y_sum[...] + sib_in[slot, 0:half].astype(f32)).astype(bf16)
                    part[lax.rem(q, part.shape[0])] += sib_in[slot, half:].astype(f32)
                    to_y(q).start()
                for cp in block_saves(q, b, e):
                    cp.start()

                @pl.when(q + 1 < hi)
                def _():
                    for cp in block_loads(q + 1, b, e):
                        cp.start()

            @pl.when(q == lo)
            def _():
                flush(e - 1, chunk)

            @pl.when(q >= lo + 2)
            def _():
                z_stage(q - 2)
            if r == 0:
                @pl.when(q == hi - 1)
                def _():
                    z_stage(q - 1)
            return 0

        lax.fori_loop(lo, hi, dz_group, 0)
        for b in (0, 1):
            for cp in block_saves(hi - 1, b, e):
                cp.wait()

    dz_round(0, early[0])
    for b in range(4):
        load_l(early[0] * chunk, chunk, b, b).start()

    def between(c):
        @pl.when(c == early[0])
        def _():
            z_stage(groups - 1)
            x_stage(0)
            if early[1] - early[0] == 1:
                final(0)
                gather_start(0)

        if early[1] - early[0] > 1:
            @pl.when(c == early[0] + 1)
            def _():
                final(0)
                gather_start(0)

    early_chunks(early[0], early[1], 1, between)
    dz_round(1, early[1])
    z_stage(last - 2)

    for b in range(4):
        load_g(early[1] * chunk, chunk, b, b).start()

    quads = n_tok // 4
    nearest = [jj for jj in (2, 0, 1) if jj < n_z - 1]
    steps = [(t // 2, 0, jj) for t, jj in enumerate(nearest)] + [(6 + t, 1, jj) for t, jj in enumerate(nearest)]

    def late_chunk(c, _):
        def quad(i, _):
            for b in range(4):
                k = 4 * i + b
                with scope('b2_wait'):
                    load_g(0, chunk, 0, b).wait()
                with scope('b2_tile'):
                    grad_tile(c * chunk, chunk, k, b, False)
                wrap = k + 4 >= n_tok
                c2, k2 = jnp.where(wrap, c + 1, c), jnp.where(wrap, k + 4 - n_tok, k + 4)

                @pl.when(c2 < sz.full)
                def _():
                    load_g(c2 * chunk, chunk, k2, b).start()

                @pl.when(c2 == sz.full)
                def _():
                    load_g(row_rem, sz.rem, k2, b).start()
                if b == 0:
                    @pl.when(jnp.logical_and(i == 0, c > early[1]))
                    def _():
                        flush(c - 1, chunk)

            for t, r, jj in steps:
                @pl.when((c - early[1]) * quads + i == t)
                def _():
                    forward(r, jj)
            return 0
        lax.fori_loop(0, quads, quad, 0)
        ship(c, chunk)

        @pl.when(c == early[1])
        def _():
            z_stage(last - 1)
            x_stage(1)

        @pl.when(c == early[1] + 1)
        def _():
            final(1)
        return 0

    lax.fori_loop(early[1], sz.full, late_chunk, 0)
    def late_rem(i, _):
        for b in range(4):
            with scope('b2_wait'):
                load_g(row_rem, sz.rem, 0, b).wait()
            with scope('b2_rem'):
                grad_tile(row_rem, sz.rem, 4 * i + b, b, False)

            @pl.when(4 * i + b + 4 < n_tok)
            def _():
                load_g(row_rem, sz.rem, 4 * i + b + 4, b).start()
            if b == 0:
                @pl.when(i == 0)
                def _():
                    flush(sz.full - 1, chunk)
        return 0

    lax.fori_loop(0, n_tok // 4, late_rem, 0)
    ship(sz.full, sz.rem)
    flush(sz.full, sz.rem)
    for t, r, jj in steps:
        if t >= (sz.full - early[1]) * quads:
            forward(r, jj)

    with scope('t_gain'):
        at.every(lambda k: heard_gain(k).wait_recv())
    total = jnp.sum(gg_in[...], axis=0)
    gg_out[0:1, 0:d] = total[0:1, 0:d]
    gg_out[0:1, d:] = (jnp.sum(st[...] * scale[...], axis=1, keepdims=True) - total[0:1, d:]) * (1.0 / LOG2E)
    with scope('t_small'):
        at.every(lambda k: ask(k).wait_send())
        at.every(lambda k: answer(k).wait_send())
        at.every(lambda k: tell_gain(k).wait_send())
        for k in range(1, n):
            for cp in tok_out(k):
                cp.wait_send()
        block_out().wait_send()
        for p in (0, 1):
            h_to_x(p).wait_send()
            for jj in range(n_z - 1):
                h_to_z(jj, p).wait_send()
        for zo in range(n_z):
            h_to_y(zo).wait_send()
        for tp in range(n_tp):
            h_to_core(tp).wait_send()

        def w_sent(c, _):
            for k in range(1, n):
                remote(k, c, c * chunk, chunk).wait_send()
            return 0

        lax.fori_loop(0, sz.full, w_sent, 0)
        for k in range(1, n):
            remote(k, sz.full, row_rem, sz.solid).wait_send()
            when_not_last(lax.rem(me + k, n), lambda: remote(k, sz.full + 1, row_odd, sz.short).wait_send())
        for q in (last - 2, last - 1):
            to_sib(q).wait_send()
            to_y(q).wait_send()
        for q in range(last - n_z, last - 1):
            to_z(q).wait_send()
        to_x(1).wait_send()
    with scope('t_send'):
        def sent(c, _):
            for cp in sends(c, chunk):
                cp.wait_send()
            return 0
        lax.fori_loop(0, sz.full, sent, 0)
        for cp in sends(sz.full, sz.rem):
            cp.wait_send()
    for r in range(ROUNDS):
        with scope(f't_gather{r}'):
            keep(r).wait()
            for cp in gathers(r):
                cp.wait_send()
            for jj in range(n_z - 1):
                onward(r, jj).wait_send()
            for zo in range(n_z):
                rcopy(gh.at[r], home(zo * 2 + 1 - at.y, r), ag_s.at[r, 0], fw_r.at[r, zo], y_peer).wait_recv()
    with scope('t_dw'):
        for k in range(1, n):
            src = lax.rem(me + n - k, n)
            rcopy(dw_hbm.at[pl.ds(0, sz.rows), :], dw_hbm.at[rows_at(src * sz.rows, sz.rows), :], dw_send.at[0, 0], dw_recv.at[k], sibling).wait_recv()


HBM = pl.BlockSpec(memory_space=pl.ANY)
VM = pl.BlockSpec(memory_space=pltpu.VMEM)
DMA = pltpu.SemaphoreType.DMA


def solution(mesh, chunk=CHUNK, tok=TOK, early=EARLY):
    n_fsdp, n_tp = mesh.shape['fsdp'], mesh.shape['tp']
    n_all, n_z = n_fsdp * n_tp, n_tp // 2
    S, V = jax.ShapeDtypeStruct, pltpu.VMEM
    i32 = jnp.int32

    def per_device(hidden, labels, tok_mask, norm_gain, w_rows):
        per_f, d = hidden.shape
        width, vocab_tp = w_rows.shape
        tokens, own = per_f * n_fsdp, per_f // n_tp
        half = own // ROUNDS
        sz = Sizes(vocab_tp, n_fsdp, chunk)
        n_low = sz.full - early[0] + 1

        dw_t, grad_hidden, sums, *_ = pl.pallas_call(
            functools.partial(head_kernel, sz, n_tp, vocab_tp, chunk, tok, early),
            out_shape=(S((n_fsdp * sz.rows, width), bf16), S(hidden.shape, bf16), S((1, d + 128), f32),
                       S((sz.rows, tokens), f32), S((sz.rows, tokens), bf16), S((tokens, d), bf16), S(((sz.full + 1) * chunk, d), bf16)),
            in_specs=[HBM, VM, VM, VM, HBM], out_specs=(HBM, HBM, VM, HBM, HBM, HBM, HBM),
            scratch_shapes=[
                V((tokens, d), bf16), V((sz.rows, d), bf16), *[V((chunk, tok), f32)] * 4, *[V((chunk, tok), bf16)] * 4, *[V((sz.rows, 2 * half), bf16)] * 2,
                V((8, tokens), f32), V((8, tokens), f32), V((1, tokens), f32), V((1, tokens), i32), V((n_fsdp, 1, per_f), i32), V((n_fsdp, 1, per_f), f32),
                V((2, tokens), f32), V((n_all, 2, own), f32), V((1, own), f32), V((1, tokens), f32), V((1, tokens), f32), V((8, min(128, half)), f32), V((own, d), bf16),
                V((chunk, d), f32), V((2, chunk, d), bf16), V((2, 2 * half, d), bf16), V((2, 2 * half, d), bf16), V((half, d), f32),
                V((2, half, d), bf16), V((6, half, d), bf16), V((3, half, d), f32), V((n_z - 1, half, d), bf16), V((ROUNDS, 2, n_z - 1, half, d), bf16), V((2, half, d), f32),
                V((half, d), bf16), V((ROUNDS, half, d), bf16), V((ROUNDS, half, d), bf16), V((1, d + 128), f32), V((n_all, 1, d + 128), f32),
                DMA((sz.full + 2, n_fsdp)), DMA((sz.full + 2, n_fsdp)), DMA((sz.full + 2,)), DMA((per_f // min(256, own),)), DMA((4,)), DMA((4,)), DMA((2, 2)), DMA((2, 2 * n_low)), DMA((2, 2)),
                DMA((n_all,)), DMA((n_all,)), DMA((n_all,)), DMA((n_all,)), DMA((2, n_fsdp)), DMA((2, n_fsdp)), DMA((2,)), DMA((2,)), DMA((2,)),
                DMA((n_z - 1, 2)), DMA((n_z - 1, 2)), DMA((n_z,)), DMA((n_z,)), DMA((n_tp,)), DMA((n_tp,)),
                DMA((1,)), DMA((2,)), DMA((sz.full + 1, 3)), DMA((n_fsdp,)), DMA((2,)), DMA((2,)), DMA((2,)), DMA((2,)), DMA((8,)),
                DMA((n_z - 1,)), DMA((ROUNDS, 2, n_z - 1)), DMA((1,)), DMA((ROUNDS,)),
                DMA((ROUNDS, n_z)), DMA((ROUNDS, n_z)), DMA((ROUNDS, n_z)), DMA((ROUNDS, n_z)), DMA((ROUNDS,)), DMA((n_all,)), DMA((n_all,))],
            compiler_params=pltpu.CompilerParams(vmem_limit_bytes=VMEM_LIMIT, collective_id=0, has_side_effects=True), name='head',
        )(hidden, labels[None, :], tok_mask[None, :], norm_gain, w_rows.T)
        return sums[0, d], grad_hidden, dw_t[:vocab_tp].T, sums[0, :d]

    return jax.shard_map(per_device, mesh=mesh, in_specs=(P('fsdp', None), P('fsdp'), P('fsdp'), P(), P('fsdp', 'tp')), out_specs=(P(), P('fsdp', None), P('fsdp', 'tp'), P()), check_vma=False)
```
